32 devices in a mesh: inst: 1 (over z), qy: 4 (over y), qx: 8 (over x, core).
Axes of the slice: x: 4, y: 4, z: 1, core: 2. Of those that a mesh axis runs over, the one named last changes fastest.
The devices are a block of a 4x4x8 slice.
Arguments:
- cost_diag: float32 [2097152], P(('inst', 'qy', 'qx'))
- gamma_angles: float32 [8], replicated
- beta_angles: float32 [8], replicated
Outputs:
- output 1: float32 [1], P('inst')
- output 2: float32 [16], P('inst')
- output 3: float32 [2, 2097152], P(None, ('inst', 'qy', 'qx'))
All inputs are finite; a program needn't handle non-finite values.
Results may differ from the reference program's by a relative error of at most 0.001.
Values sent between devices are 32-bit elements.
A program may use at most 768 MiB of HBM per device.

```python
import math
import jax
import jax.numpy as jnp
from jax import lax

STATE_LEN = 2097152
LAYERS = 8
DEGREE = 3
NUM_QUBITS = int(math.log2(STATE_LEN))
NUM_EDGES = DEGREE * NUM_QUBITS // 2


def setup_inputs(seed: int = 0, part: int = 0) -> dict:
    base_key = jax.random.key(seed)
    part_key = jax.random.fold_in(base_key, part)
    key_heads, key_offsets, key_weights = jax.random.split(part_key, 3)
    ring_heads = jnp.arange(NUM_QUBITS, dtype=jnp.int32)
    extra_heads = jax.random.randint(key_heads, (NUM_EDGES - NUM_QUBITS,), 0, NUM_QUBITS, dtype=jnp.int32)
    edge_heads = jnp.concatenate([ring_heads, extra_heads])
    offsets = jax.random.randint(key_offsets, (NUM_EDGES,), 1, NUM_QUBITS, dtype=jnp.int32)
    edge_tails = (edge_heads + offsets) % NUM_QUBITS
    weights = jax.random.uniform(key_weights, (NUM_EDGES,), jnp.float32, 0.5, 1.5)
    positions = jnp.arange(STATE_LEN, dtype=jnp.int32)

    def add_edge(cost_sum, edge_data):
        edge_head, edge_tail, weight = edge_data
        parity = jnp.bitwise_and(jnp.bitwise_xor(jnp.right_shift(positions, edge_head), jnp.right_shift(positions, edge_tail)), 1)
        return cost_sum + weight * (1.0 - 2.0 * parity.astype(jnp.float32)), None

    cost_sum = lax.scan(add_edge, jnp.zeros((STATE_LEN,), jnp.float32), (edge_heads, edge_tails, weights))[0]
    cost_diag = cost_sum / jnp.sqrt(jnp.sum(weights * weights))
    angle_key = jax.random.key(seed + 17)
    key_gamma, key_beta = jax.random.split(angle_key)
    gamma_angles = jax.random.uniform(key_gamma, (LAYERS,), jnp.float32, 0.2, 0.8)
    beta_angles = jax.random.uniform(key_beta, (LAYERS,), jnp.float32, 0.4, 1.4)
    return {"cost_diag": cost_diag, "gamma_angles": gamma_angles, "beta_angles": beta_angles}


def turn_vec(state_vec):
    return jnp.stack([state_vec[1], -state_vec[0]])


def phase_turn(state_vec, cost_diag, angle, sign_flip):
    phase_angle = angle * cost_diag
    cos_phase = jnp.cos(phase_angle)
    sin_phase = sign_flip * jnp.sin(phase_angle)
    return jnp.stack([cos_phase * state_vec[0] + sin_phase * state_vec[1], cos_phase * state_vec[1] - sin_phase * state_vec[0]])


def mix_qubit(state_vec, half_block, cos_half, sin_half):
    split_view = state_vec.reshape(state_vec.shape[:-1] + (state_vec.shape[-1] // (2 * half_block), 2, half_block))
    partner = jnp.flip(split_view, axis=-2)
    return (cos_half * split_view + sin_half * turn_vec(partner)).reshape(state_vec.shape)


def unmix_qubit(both_vecs, half_block, cos_half, sin_half):
    split_view = both_vecs.reshape(both_vecs.shape[:-1] + (both_vecs.shape[-1] // (2 * half_block), 2, half_block))
    partner = jnp.flip(split_view, axis=-2)
    beta_term = jnp.sum(split_view[0, 1] * partner[1, 0] - split_view[1, 1] * partner[0, 0], axis=(-3, -2, -1))
    return (cos_half * split_view - sin_half * turn_vec(partner)).reshape(both_vecs.shape), beta_term


def reference(cost_diag, gamma_angles, beta_angles):
    amplitude = STATE_LEN ** -0.5
    start_state = jnp.stack([jnp.full((STATE_LEN,), amplitude, jnp.float32), jnp.zeros((STATE_LEN,), jnp.float32)])

    def forward_layer(state_vec, layer_angles):
        layer_gamma, layer_beta = layer_angles
        state_vec = phase_turn(state_vec, cost_diag, layer_gamma, 1.0)
        cos_half = jnp.cos(0.5 * layer_beta)
        sin_half = jnp.sin(0.5 * layer_beta)
        for qubit_num in range(NUM_QUBITS):
            state_vec = mix_qubit(state_vec, 2 ** qubit_num, cos_half, sin_half)
        return state_vec, None

    final_psi = lax.scan(forward_layer, start_state, (gamma_angles, beta_angles))[0]
    energy = jnp.sum(cost_diag * (final_psi[0] ** 2 + final_psi[1] ** 2))
    start_pair = jnp.stack([final_psi, cost_diag * final_psi], axis=1)

    def backward_layer(both_vecs, layer_angles):
        layer_gamma, layer_beta = layer_angles
        cos_half = jnp.cos(0.5 * layer_beta)
        sin_half = jnp.sin(0.5 * layer_beta)
        beta_sum = jnp.zeros((), jnp.float32)
        for qubit_num in range(NUM_QUBITS):
            both_vecs, beta_term = unmix_qubit(both_vecs, 2 ** qubit_num, cos_half, sin_half)
            beta_sum = beta_sum + beta_term
        gamma_sum = 2.0 * jnp.sum(cost_diag * (both_vecs[0, 1] * both_vecs[1, 0] - both_vecs[1, 1] * both_vecs[0, 0]))
        both_vecs = phase_turn(both_vecs, cost_diag, layer_gamma, -1.0)
        return both_vecs, (gamma_sum, beta_sum)

    layer_grads = lax.scan(backward_layer, start_pair, (gamma_angles, beta_angles), reverse=True)[1]
    angle_grad = jnp.concatenate([layer_grads[0], layer_grads[1]])
    final_state = final_psi * STATE_LEN ** 0.5
    return (energy.reshape(1), angle_grad, final_state)
```

```python
import functools
import math

import jax
import jax.numpy as jnp
from jax import lax
from jax.experimental import pallas as pl
from jax.experimental.pallas import tpu as pltpu
from jax.sharding import PartitionSpec as P

LANES = 128
MESH_ID = pl.DeviceIdType.MESH


def mix_pair(blocks, tan_half, stride):
    out = list(blocks)
    for low in range(len(blocks)):
        if low & stride:
            continue
        high = low | stride
        (re0, im0), (re1, im1) = blocks[low], blocks[high]
        out[low] = (re0 + tan_half * im1, im0 - tan_half * re1)
        out[high] = (re1 + tan_half * im0, im1 - tan_half * re0)
    return out


def mix_all(blocks, tan_half):
    stride = 1
    while stride < len(blocks):
        blocks = mix_pair(blocks, tan_half, stride)
        stride *= 2
    return blocks


def partner_sums(blocks):
    out = []
    for place in range(len(blocks)):
        stride, re, im = 1, None, None
        while stride < len(blocks):
            pre, pim = blocks[place ^ stride]
            re, im = (pre, pim) if re is None else (re + pre, im + pim)
            stride *= 2
        out.append((re, im))
    return out


def inner_partners(tiles, per_block, apply):
    lane = lax.broadcasted_iota(jnp.int32, (1, 8, LANES), 2)
    sub = lax.broadcasted_iota(jnp.int32, (1, 8, LANES), 1)

    def rolled(x, ids, dist, axis, size):
        if 2 * dist == size:
            return pltpu.roll(x, dist, axis)
        upper = (ids // dist) % 2 > 0
        return jnp.where(upper, pltpu.roll(x, dist, axis), pltpu.roll(x, size - dist, axis))

    for bit in range(7):
        tiles = apply(tiles, lambda x, d=2 ** bit: rolled(x, lane, d, 2, LANES))
    for bit in range(3):
        tiles = apply(tiles, lambda x, d=2 ** bit: rolled(x, sub, d, 1, 8))
    stride = 1
    while stride < per_block:
        def swapped(x, d=stride):
            return jnp.concatenate([x[(i ^ d):(i ^ d) + 1] for i in range(x.shape[0])], axis=0)
        tiles = apply(tiles, swapped)
        stride *= 2
    return tiles


def kernel(ny, nx, num_layers, num_qubits, amp, cost, gamma, beta, final, totals,
           cost_b, tabs, post, pre, recv, send, work, lam, lam_pre, qbuf, angle, acc, part, gath,
           send_sem, recv_sem, cost_send, cost_recv, sum_send, sum_recv):
    nb = ny * nx
    chips = nx // 2
    rows = cost.shape[1]
    tiles = rows // 8
    my_y = lax.axis_index("qy")
    my_x = lax.axis_index("qx")
    my_chip, my_core = my_x // 2, my_x % 2
    me = my_y * nx + my_x

    def peer(dy, dx, dc):
        y = (my_y + dy) % ny
        x = ((my_chip + dx) % chips) * 2 + (my_core + dc) % 2
        return y, x, y * nx + x

    dy_order = sorted(range(ny), key=lambda d: -min(d, ny - d))
    dx_order = sorted(range(chips), key=lambda d: -min(d, chips - d))
    offsets = [(dy, dx, dc) for dy in dy_order for dx in dx_order for dc in (1, 0)]

    barrier = pltpu.get_barrier_semaphore()
    for dy, dx, dc in offsets:
        if dy or dx or dc:
            y, x, _ = peer(dy, dx, dc)
            pl.semaphore_signal(barrier, inc=1, device_id={"qy": y, "qx": x}, device_id_type=MESH_ID)

    for layer in range(num_layers):
        half = jnp.full((8, LANES), 0.5 * beta[layer], jnp.float32)
        cos_half, sin_half = jnp.cos(half), jnp.sin(half)
        scale, power, left = None, cos_half, num_qubits
        while left:
            if left % 2:
                scale = power if scale is None else scale * power
            power, left = power * power, left // 2
        angle[layer, 0] = sin_half / cos_half
        angle[layer, 1] = scale

    def angle_of(layer, kind):
        tile = angle[layer, kind]
        return jnp.concatenate([tile] * tiles, axis=0) if tiles > 1 else tile

    def make_table(layer, source):
        g = gamma[layer]

        def body(j, _):
            theta = g * source[j]
            tabs[layer, 0, j] = jnp.cos(theta)
            tabs[layer, 1, j] = jnp.sin(theta)
            return 0

        lax.fori_loop(0, nb, body, 0)

    def turn(block, layer, j, sign):
        re, im = block
        c, s = tabs[layer, 0, j], sign * tabs[layer, 1, j]
        return c * re + s * im, c * im - s * re

    def low_bits(src, dst, tan_half, y):
        blocks = [(src[y * nx + x, 0], src[y * nx + x, 1]) for x in range(nx)]
        for x, (re, im) in enumerate(mix_all(blocks, tan_half)):
            dst[y * nx + x, 0] = re
            dst[y * nx + x, 1] = im

    def start_send(par, dy, dx, dc):
        y, x, dest = peer(dy, dx, dc)
        if not (dy or dx or dc):
            pltpu.make_async_copy(send.at[par, me], recv.at[par, me], recv_sem.at[par, me]).start()
            return
        pltpu.make_async_remote_copy(
            src_ref=send.at[par, dest], dst_ref=recv.at[par, me],
            send_sem=send_sem.at[par], recv_sem=recv_sem.at[par, me],
            device_id={"qy": y, "qx": x}, device_id_type=MESH_ID).start()

    def wait_sends(par):
        view = send.at[par, pl.ds(0, nb - 1)]
        pltpu.make_async_copy(view, view, send_sem.at[par]).wait()

    def low_bits_and_send(par, tan_half):
        for dy in dy_order:
            y = (my_y + dy) % ny
            low_bits(work, send.at[par], tan_half, y)
            for dx in dx_order:
                for dc in (1, 0):
                    start_send(par, dy, dx, dc)

    groups = (nb + 3) // 4

    def receive(par, tan_half):
        tile = tan_half[:8].reshape(1, 8, LANES)

        def body(i, _):
            slots = []
            for k in range(nb // groups):
                n = i * (nb // groups) + k
                dy = (n // nx + ny // 2) % ny
                dx = ((n % nx) // 2 + chips // 2) % chips
                _, _, slot = peer(dy, dx, n % 2)
                view = recv.at[par, slot]
                pltpu.make_async_copy(view, view, recv_sem.at[par, slot]).wait()
                slots.append(slot)
            re = jnp.concatenate([recv[par, s, 0].reshape(tiles, 8, LANES) for s in slots], axis=0)
            im = jnp.concatenate([recv[par, s, 1].reshape(tiles, 8, LANES) for s in slots], axis=0)
            re, im = inner_partners((re, im), tiles, lambda t, f: (t[0] + tile * f(t[1]), t[1] - tile * f(t[0])))
            for k, s in enumerate(slots):
                recv[par, s, 0] = re[k * tiles:(k + 1) * tiles].reshape(rows, LANES)
                recv[par, s, 1] = im[k * tiles:(k + 1) * tiles].reshape(rows, LANES)
            return 0

        lax.fori_loop(0, groups, body, 0)

    def all_low_bits(par, tan_half):
        def body(y, _):
            low_bits(recv.at[par], work, tan_half, y)
            return 0
        lax.fori_loop(0, ny, body, 0)

    def column(x):
        return [y * nx + x for y in range(ny)]

    def load(ref, places):
        return [(ref[j, 0], ref[j, 1]) for j in places]

    def store(ref, places, blocks):
        for j, (re, im) in zip(places, blocks):
            ref[j, 0] = re
            ref[j, 1] = im

    def for_columns(body):
        lax.fori_loop(0, nx, lambda x, _: (body(column(x)), 0)[1], 0)

    def scaled(blocks, scale):
        return [(scale * re, scale * im) for re, im in blocks]

    make_table(0, cost)
    tan0 = angle_of(0, 0)

    def first(places):
        flat = jnp.full((rows, LANES), amp, jnp.float32)
        blocks = [(flat, jnp.zeros_like(flat)) for _ in places]
        blocks = [turn(b, 0, j, 1.0) for b, j in zip(blocks, places)]
        store(pre.at[0], places, blocks)
        store(work, places, mix_all(blocks, tan0))

    for_columns(first)
    for place in range(acc.shape[0]):
        acc[place] = jnp.zeros((8, LANES), jnp.float32)

    pl.semaphore_wait(barrier, nb - 1)

    for dy, dx, dc in offsets:
        y, x, dest = peer(dy, dx, dc)
        if dy or dx or dc:
            pltpu.make_async_remote_copy(
                src_ref=cost.at[dest], dst_ref=cost_b.at[me], send_sem=cost_send, recv_sem=cost_recv.at[me],
                device_id={"qy": y, "qx": x}, device_id_type=MESH_ID).start()
        else:
            pltpu.make_async_copy(cost.at[me], cost_b.at[me], cost_recv.at[me]).start()
    low_bits_and_send(0, tan0)

    def cost_wait(j, _):
        pltpu.make_async_copy(cost_b.at[j], cost_b.at[j], cost_recv.at[j]).wait()
        return 0

    lax.fori_loop(0, nb, cost_wait, 0)

    def forward(layer, _):
        par = layer % 2

        @pl.when(par == 0)
        def _():
            make_table(layer + 1, cost_b)

        @pl.when(par == 1)
        def _():
            make_table(layer + 1, cost)

        tan_half, scale = angle_of(layer, 0), angle_of(layer, 1)
        tan_next = angle_of(layer + 1, 0)
        receive(par, tan_half)
        all_low_bits(par, tan_half)

        def middle(places):
            blocks = scaled(mix_all(load(work, places), tan_half), scale)
            store(post.at[layer], places, blocks)
            blocks = [turn(b, layer + 1, j, 1.0) for b, j in zip(blocks, places)]
            store(pre.at[layer + 1], places, blocks)
            store(work, places, mix_all(blocks, tan_next))

        for_columns(middle)

        @pl.when(layer > 0)
        def _():
            wait_sends(1 - par)

        low_bits_and_send(1 - par, tan_next)
        return 0

    lax.fori_loop(0, num_layers - 1, forward, 0)

    last = num_layers - 1
    par = last % 2
    tan_half, scale = angle_of(last, 0), angle_of(last, 1)
    receive(par, tan_half)
    all_low_bits(par, tan_half)
    root = jnp.float32(1.0 / amp)

    def turn_point(places):
        blocks = scaled(mix_all(load(work, places), tan_half), scale)
        store(post.at[last], places, blocks)
        turned = []
        energy = acc[0]
        for j, (re, im) in zip(places, blocks):
            c = cost[j]
            final[0, j] = root * re
            final[1, j] = root * im
            turned.append((c * re, c * im))
            energy += (c * (re * re + im * im)).reshape(tiles, 8, LANES).sum(axis=0)
        acc[0] = energy
        store(lam, places, turned)
        store(work, places, mix_all(turned, -tan_half))

    for_columns(turn_point)
    wait_sends(1 - par)
    low_bits_and_send(1 - par, -tan_half)

    def im_dot(left, right):
        return (left[0] * right[1] - left[1] * right[0]).reshape(tiles, 8, LANES).sum(axis=0)

    def block_sums(src):
        def low(y, _):
            places = [y * nx + x for x in range(nx)]
            store(qbuf, places, partner_sums(load(src, places)))
            return 0

        lax.fori_loop(0, ny, low, 0)

        def high(places):
            sums = partner_sums(load(src, places))
            store(qbuf, places, [(a + c, b + d) for (a, b), (c, d) in zip(sums, load(qbuf, places))])

        for_columns(high)

    def inner_sums(src):
        def body(j, _):
            x = (src[j, 0].reshape(tiles, 8, LANES), src[j, 1].reshape(tiles, 8, LANES))
            total = (qbuf[j, 0].reshape(tiles, 8, LANES), qbuf[j, 1].reshape(tiles, 8, LANES))
            parts = []
            inner_partners(x, tiles, lambda t, f: (parts.append((f(t[0]), f(t[1]))), t)[1])
            for re, im in parts:
                total = (total[0] + re, total[1] + im)
            qbuf[j, 0] = total[0].reshape(rows, LANES)
            qbuf[j, 1] = total[1].reshape(rows, LANES)
            return 0

        lax.fori_loop(0, nb, body, 0)

    def dot_with_sums(left):
        def body(j, total):
            return total + im_dot((left[j, 0], left[j, 1]), (qbuf[j, 0], qbuf[j, 1]))
        return lax.fori_loop(0, nb, body, jnp.zeros((8, LANES), jnp.float32))

    def backward(step, _):
        layer = last - step
        par = layer % 2
        back = 1 - par
        block_sums(post.at[layer])
        beta_part = dot_with_sums(lam)
        block_sums(pre.at[layer])
        inner_sums(pre.at[layer])

        tan_half, scale = -angle_of(layer, 0), angle_of(layer, 1)
        receive(back, tan_half)
        all_low_bits(back, tan_half)

        before = lax.max(layer - 1, 0)
        tan_next = -angle_of(before, 0)

        def middle(places):
            blocks = scaled(mix_all(load(work, places), tan_half), scale)
            store(lam_pre, places, blocks)
            blocks = [turn(b, layer, j, -1.0) for b, j in zip(blocks, places)]
            store(lam, places, blocks)
            store(work, places, mix_all(blocks, tan_next))

        for_columns(middle)
        wait_sends(par)

        @pl.when(layer > 0)
        def _():
            low_bits_and_send(par, tan_next)

        beta_part += dot_with_sums(lam_pre)

        def gamma_body(j, total):
            prod = lam_pre[j, 0] * pre[layer, j, 1] - lam_pre[j, 1] * pre[layer, j, 0]
            prod = prod * jnp.where(par == 0, cost[j], cost_b[j])
            return total + prod.reshape(tiles, 8, LANES).sum(axis=0)

        gamma_part = lax.fori_loop(0, nb, gamma_body, jnp.zeros((8, LANES), jnp.float32))
        acc[1 + layer] = 2.0 * gamma_part
        acc[1 + num_layers + layer] = beta_part
        return 0

    lax.fori_loop(0, num_layers, backward, 0)
    wait_sends((last + 1) % 2 if num_layers == 1 else 1)

    lane = lax.broadcasted_iota(jnp.int32, (1, LANES), 1)
    row = jnp.zeros((1, LANES), jnp.float32)
    for place in range(acc.shape[0]):
        value = jnp.sum(jnp.sum(acc[place], axis=0, keepdims=True), axis=1, keepdims=True)
        row = jnp.where(lane == place, value, row)
    part[...] = row
    for dy, dx, dc in offsets:
        y, x, dest = peer(dy, dx, dc)
        if dy or dx or dc:
            pltpu.make_async_remote_copy(
                src_ref=part, dst_ref=gath.at[me], send_sem=sum_send, recv_sem=sum_recv.at[me],
                device_id={"qy": y, "qx": x}, device_id_type=MESH_ID).start()
        else:
            pltpu.make_async_copy(part, gath.at[me], sum_recv.at[me]).start()

    def sum_wait(j, _):
        pltpu.make_async_copy(part, gath.at[j], sum_recv.at[j]).wait()
        return 0

    lax.fori_loop(0, nb, sum_wait, 0)
    totals[...] = lax.fori_loop(0, nb, lambda j, t: t + gath[j], jnp.zeros((1, LANES), jnp.float32))
    view = gath.at[pl.ds(0, nb - 1)]
    pltpu.make_async_copy(view, view, sum_send).wait()
    view = cost_b.at[pl.ds(0, nb - 1)]
    pltpu.make_async_copy(view, view, cost_send).wait()


def solution(mesh):
    ny, nx = mesh.shape["qy"], mesh.shape["qx"]
    nb = ny * nx

    def local_run(cost_local, gamma_angles, beta_angles):
        chunk = cost_local.shape[0]
        num_layers = gamma_angles.shape[0]
        rows = chunk // (nb * LANES)
        num_qubits = int(math.log2(chunk * nb))
        amp = (chunk * nb) ** -0.5
        vmem, smem = pltpu.VMEM, pltpu.SMEM
        state = (nb, 2, rows, LANES)
        f32 = jnp.float32
        final, totals = pl.pallas_call(
            functools.partial(kernel, ny, nx, num_layers, num_qubits, amp),
            out_shape=(jax.ShapeDtypeStruct((2, nb, rows, LANES), f32), jax.ShapeDtypeStruct((1, LANES), f32)),
            in_specs=[pl.BlockSpec(memory_space=vmem), pl.BlockSpec(memory_space=smem), pl.BlockSpec(memory_space=smem)],
            out_specs=(pl.BlockSpec(memory_space=vmem), pl.BlockSpec(memory_space=vmem)),
            scratch_shapes=[
                vmem((nb, rows, LANES), f32),
                vmem((num_layers, 2, nb, rows, LANES), f32),
                vmem((num_layers,) + state, f32),
                vmem((num_layers,) + state, f32),
                vmem((2,) + state, f32),
                vmem((2,) + state, f32),
                vmem(state, f32),
                vmem(state, f32),
                vmem(state, f32),
                vmem(state, f32),
                vmem((num_layers, 2, 8, LANES), f32),
                vmem((1 + 2 * num_layers, 8, LANES), f32),
                vmem((1, LANES), f32),
                vmem((nb, 1, LANES), f32),
                pltpu.SemaphoreType.DMA((2,)),
                pltpu.SemaphoreType.DMA((2, nb)),
                pltpu.SemaphoreType.DMA,
                pltpu.SemaphoreType.DMA((nb,)),
                pltpu.SemaphoreType.DMA,
                pltpu.SemaphoreType.DMA((nb,)),
            ],
            compiler_params=pltpu.CompilerParams(
                collective_id=0, has_side_effects=True, vmem_limit_bytes=48 * 1024 * 1024),
            name="qaoa",
        )(cost_local.reshape(nb, rows, LANES), gamma_angles, beta_angles)
        energy = totals[0, :1]
        grad = totals[0, 1:1 + 2 * num_layers]
        return energy, grad, final.reshape(2, chunk)

    state_spec = P(("inst", "qy", "qx"))
    return jax.shard_map(
        local_run, mesh=mesh, in_specs=(state_spec, P(), P()),
        out_specs=(P("inst"), P("inst"), P(None, ("inst", "qy", "qx"))), check_vma=False)
```

```python
import functools
import math

import jax
import jax.numpy as jnp
from jax import lax
from jax.experimental import pallas as pl
from jax.experimental.pallas import tpu as pltpu
from jax.sharding import PartitionSpec as P

LANES = 128
MESH_ID = pl.DeviceIdType.MESH


def mix_pair(blocks, tan_half, stride):
    out = list(blocks)
    for low in range(len(blocks)):
        if low & stride:
            continue
        high = low | stride
        (re0, im0), (re1, im1) = blocks[low], blocks[high]
        out[low] = (re0 + tan_half * im1, im0 - tan_half * re1)
        out[high] = (re1 + tan_half * im0, im1 - tan_half * re0)
    return out


def mix_all(blocks, tan_half):
    stride = 1
    while stride < len(blocks):
        blocks = mix_pair(blocks, tan_half, stride)
        stride *= 2
    return blocks


def partner_sums(blocks):
    out = []
    for place in range(len(blocks)):
        stride, re, im = 1, None, None
        while stride < len(blocks):
            pre, pim = blocks[place ^ stride]
            re, im = (pre, pim) if re is None else (re + pre, im + pim)
            stride *= 2
        out.append((re, im))
    return out


def sublane_partner(x, ids, dist):
    return jnp.take_along_axis(x, ids ^ dist, axis=0, mode="promise_in_bounds")


def rows_of(tiles):
    return jnp.concatenate(tiles, axis=0)


def matmul(x, w):
    return jnp.dot(x, w, precision=lax.Precision.HIGHEST, preferred_element_type=jnp.float32)


def kernel(ny, nx, num_layers, num_qubits, amp, cost, gamma, beta, final, totals,
           cost_b, tabs, post, pre, recv, send, work, lam, lam_pre, qbuf, angle, lane_mix, lane_sum, acc, part, gath,
           send_sem, recv_sem, cost_send, cost_recv, sum_send, sum_recv):
    nb = ny * nx
    chips = nx // 2
    rows = cost.shape[1]
    tiles = rows // 8
    my_y = lax.axis_index("qy")
    my_x = lax.axis_index("qx")
    my_chip, my_core = my_x // 2, my_x % 2
    me = my_y * nx + my_x

    def peer(dy, dx, dc):
        y = (my_y + dy) % ny
        x = ((my_chip + dx) % chips) * 2 + (my_core + dc) % 2
        return y, x, y * nx + x

    dy_order = sorted(range(ny), key=lambda d: -min(d, ny - d))
    dx_order = sorted(range(chips), key=lambda d: -min(d, chips - d))
    offsets = [(dy, dx, dc) for dy in dy_order for dx in dx_order for dc in (1, 0)]

    barrier = pltpu.get_barrier_semaphore()
    for dy, dx, dc in offsets:
        if dy or dx or dc:
            y, x, _ = peer(dy, dx, dc)
            pl.semaphore_signal(barrier, inc=1, device_id={"qy": y, "qx": x}, device_id_type=MESH_ID)

    flips = lax.broadcasted_iota(jnp.int32, (LANES, LANES), 0) ^ lax.broadcasted_iota(jnp.int32, (LANES, LANES), 1)
    weight = sum((flips >> bit) & 1 for bit in range(7))
    ones = jnp.where(weight == 1, 1.0, 0.0).astype(jnp.float32)
    lane_sum[:LANES, :LANES] = ones
    lane_sum[LANES:, LANES:] = ones
    lane_sum[:LANES, LANES:] = jnp.zeros_like(ones)
    lane_sum[LANES:, :LANES] = jnp.zeros_like(ones)
    for layer in range(num_layers):
        half = jnp.full((8, LANES), 0.5 * beta[layer], jnp.float32)
        cos_half, sin_half = jnp.cos(half), jnp.sin(half)
        scale, power, left = None, cos_half, num_qubits - 7
        while left:
            if left % 2:
                scale = power if scale is None else scale * power
            power, left = power * power, left // 2
        angle[layer, 0] = sin_half / cos_half
        angle[layer, 1] = scale
        coefs = []
        for k in range(8):
            c = cos_half[:1]
            s = sin_half[:1]
            coef = None
            for factor in [c] * (7 - k) + [s] * k:
                coef = factor if coef is None else coef * factor
            coefs.append(coef)
        even, odd = jnp.zeros((LANES, LANES), jnp.float32), jnp.zeros((LANES, LANES), jnp.float32)
        for k in range(8):
            value = coefs[k] if (k // 2) % 2 == 0 else -coefs[k]
            if k % 2 == 0:
                even = jnp.where(weight == k, value, even)
            else:
                odd = jnp.where(weight == k, value, odd)
        lane_mix[layer, :LANES, :LANES] = even
        lane_mix[layer, LANES:, LANES:] = even
        lane_mix[layer, LANES:, :LANES] = odd
        lane_mix[layer, :LANES, LANES:] = -odd

    def angle_of(layer, kind):
        tile = angle[layer, kind]
        return jnp.concatenate([tile] * tiles, axis=0) if tiles > 1 else tile

    def make_table(layer, source):
        g = gamma[layer]

        def body(j, _):
            theta = g * source[j]
            tabs[layer, 0, j] = jnp.cos(theta)
            tabs[layer, 1, j] = jnp.sin(theta)
            return 0

        lax.fori_loop(0, nb, body, 0)

    def turn(block, layer, j, sign):
        re, im = block
        c, s = tabs[layer, 0, j], sign * tabs[layer, 1, j]
        return c * re + s * im, c * im - s * re

    def low_bits(src, dst, tan_half, y):
        blocks = [(src[y * nx + x, 0], src[y * nx + x, 1]) for x in range(nx)]
        for x, (re, im) in enumerate(mix_all(blocks, tan_half)):
            dst[y * nx + x, 0] = re
            dst[y * nx + x, 1] = im

    def start_send(par, dy, dx, dc):
        y, x, dest = peer(dy, dx, dc)
        if not (dy or dx or dc):
            pltpu.make_async_copy(send.at[par, me], recv.at[par, me], recv_sem.at[par, me]).start()
            return
        pltpu.make_async_remote_copy(
            src_ref=send.at[par, dest], dst_ref=recv.at[par, me],
            send_sem=send_sem.at[par], recv_sem=recv_sem.at[par, me],
            device_id={"qy": y, "qx": x}, device_id_type=MESH_ID).start()

    def wait_sends(par):
        view = send.at[par, pl.ds(0, nb - 1)]
        pltpu.make_async_copy(view, view, send_sem.at[par]).wait()

    def low_bits_and_send(par, tan_half):
        for dy in dy_order:
            y = (my_y + dy) % ny
            low_bits(work, send.at[par], tan_half, y)
            for dx in dx_order:
                for dc in (1, 0):
                    start_send(par, dy, dx, dc)

    sub = lax.broadcasted_iota(jnp.int32, (8, LANES), 0)

    def load_row(ref, y):
        return [(ref[y * nx + x, 0, 8 * i:8 * i + 8], ref[y * nx + x, 1, 8 * i:8 * i + 8])
                for x in range(nx) for i in range(tiles)]

    def receive(par, layer, tan_half, back):
        tan_tile = tan_half[:8]

        def body(i, _):
            y = (my_y + i + ny // 2) % ny
            for dx in range(chips):
                for dc in range(2):
                    slot = y * nx + ((my_chip + chips // 2 + dx) % chips) * 2 + (my_core + dc) % 2
                    view = recv.at[par, slot]
                    pltpu.make_async_copy(view, view, recv_sem.at[par, slot]).wait()
            row = load_row(recv.at[par], y)
            for dist in (1, 2, 4):
                row = [(re + tan_tile * sublane_partner(im, sub, dist), im - tan_tile * sublane_partner(re, sub, dist))
                       for re, im in row]
            row = mix_all(row, tan_tile)
            re, im = rows_of([t[0] for t in row]), rows_of([t[1] for t in row])
            mixed = matmul(jnp.concatenate([im, re] if back else [re, im], axis=1), lane_mix[layer])
            first, second = mixed[:, :LANES], mixed[:, LANES:]
            re, im = (second, first) if back else (first, second)
            for x in range(nx):
                work[y * nx + x, 0] = re[x * rows:(x + 1) * rows]
                work[y * nx + x, 1] = im[x * rows:(x + 1) * rows]
            return 0

        lax.fori_loop(0, ny, body, 0)

    def column(x):
        return [y * nx + x for y in range(ny)]

    def load(ref, places):
        return [(ref[j, 0], ref[j, 1]) for j in places]

    def store(ref, places, blocks):
        for j, (re, im) in zip(places, blocks):
            ref[j, 0] = re
            ref[j, 1] = im

    def for_columns(body):
        lax.fori_loop(0, nx, lambda x, _: (body(column(x)), 0)[1], 0)

    def scaled(blocks, scale):
        return [(scale * re, scale * im) for re, im in blocks]

    make_table(0, cost)
    tan0 = angle_of(0, 0)

    def first(places):
        flat = jnp.full((rows, LANES), amp, jnp.float32)
        blocks = [(flat, jnp.zeros_like(flat)) for _ in places]
        blocks = [turn(b, 0, j, 1.0) for b, j in zip(blocks, places)]
        store(pre.at[0], places, blocks)
        store(work, places, mix_all(blocks, tan0))

    for_columns(first)
    for place in range(acc.shape[0]):
        acc[place] = jnp.zeros((8, LANES), jnp.float32)

    pl.semaphore_wait(barrier, nb - 1)

    for dy, dx, dc in offsets:
        y, x, dest = peer(dy, dx, dc)
        if dy or dx or dc:
            pltpu.make_async_remote_copy(
                src_ref=cost.at[dest], dst_ref=cost_b.at[me], send_sem=cost_send, recv_sem=cost_recv.at[me],
                device_id={"qy": y, "qx": x}, device_id_type=MESH_ID).start()
        else:
            pltpu.make_async_copy(cost.at[me], cost_b.at[me], cost_recv.at[me]).start()
    low_bits_and_send(0, tan0)

    def cost_wait(j, _):
        pltpu.make_async_copy(cost_b.at[j], cost_b.at[j], cost_recv.at[j]).wait()
        return 0

    lax.fori_loop(0, nb, cost_wait, 0)

    def forward(layer, _):
        par = layer % 2

        @pl.when(par == 0)
        def _():
            make_table(layer + 1, cost_b)

        @pl.when(par == 1)
        def _():
            make_table(layer + 1, cost)

        tan_half, scale = angle_of(layer, 0), angle_of(layer, 1)
        tan_next = angle_of(layer + 1, 0)
        receive(par, layer, tan_half, False)

        def middle(places):
            blocks = scaled(mix_all(load(work, places), tan_half), scale)
            store(post.at[layer], places, blocks)
            blocks = [turn(b, layer + 1, j, 1.0) for b, j in zip(blocks, places)]
            store(pre.at[layer + 1], places, blocks)
            store(work, places, mix_all(blocks, tan_next))

        for_columns(middle)

        @pl.when(layer > 0)
        def _():
            wait_sends(1 - par)

        low_bits_and_send(1 - par, tan_next)
        return 0

    lax.fori_loop(0, num_layers - 1, forward, 0)

    last = num_layers - 1
    par = last % 2
    tan_half, scale = angle_of(last, 0), angle_of(last, 1)
    receive(par, last, tan_half, False)
    root = jnp.float32(1.0 / amp)

    def turn_point(places):
        blocks = scaled(mix_all(load(work, places), tan_half), scale)
        store(post.at[last], places, blocks)
        turned = []
        energy = acc[0]
        for j, (re, im) in zip(places, blocks):
            c = cost[j]
            final[0, j] = root * re
            final[1, j] = root * im
            turned.append((c * re, c * im))
            energy += (c * (re * re + im * im)).reshape(tiles, 8, LANES).sum(axis=0)
        acc[0] = energy
        store(lam, places, turned)
        store(work, places, mix_all(turned, -tan_half))

    for_columns(turn_point)
    wait_sends(1 - par)
    low_bits_and_send(1 - par, -tan_half)

    def im_dot(left, right):
        return (left[0] * right[1] - left[1] * right[0]).reshape(tiles, 8, LANES).sum(axis=0)

    def block_sums(src, inner):
        def low(y, _):
            row = load_row(src, y)
            if inner:
                re, im = rows_of([t[0] for t in row]), rows_of([t[1] for t in row])
                lanes = matmul(jnp.concatenate([re, im], axis=1), lane_sum[...])
                total = partner_sums(row)
                for n, (re, im) in enumerate(row):
                    sre, sim = total[n]
                    for dist in (1, 2, 4):
                        sre += sublane_partner(re, sub, dist)
                        sim += sublane_partner(im, sub, dist)
                    place, top = y * nx + n // tiles, 8 * (n % tiles)
                    qbuf[place, 0, top:top + 8] = sre + lanes[8 * n:8 * n + 8, :LANES]
                    qbuf[place, 1, top:top + 8] = sim + lanes[8 * n:8 * n + 8, LANES:]
            else:
                places = [y * nx + x for x in range(nx)]
                store(qbuf, places, partner_sums(load(src, places)))
            return 0

        lax.fori_loop(0, ny, low, 0)

        def high(places):
            sums = partner_sums(load(src, places))
            store(qbuf, places, [(a + c, b + d) for (a, b), (c, d) in zip(sums, load(qbuf, places))])

        for_columns(high)

    def dot_with_sums(left):
        def body(j, total):
            return total + im_dot((left[j, 0], left[j, 1]), (qbuf[j, 0], qbuf[j, 1]))
        return lax.fori_loop(0, nb, body, jnp.zeros((8, LANES), jnp.float32))

    def backward(step, _):
        layer = last - step
        par = layer % 2
        back = 1 - par
        block_sums(post.at[layer], False)
        beta_part = dot_with_sums(lam)
        block_sums(pre.at[layer], True)

        tan_half, scale = -angle_of(layer, 0), angle_of(layer, 1)
        receive(back, layer, tan_half, True)

        before = lax.max(layer - 1, 0)
        tan_next = -angle_of(before, 0)

        def middle(places):
            blocks = scaled(mix_all(load(work, places), tan_half), scale)
            store(lam_pre, places, blocks)
            blocks = [turn(b, layer, j, -1.0) for b, j in zip(blocks, places)]
            store(lam, places, blocks)
            store(work, places, mix_all(blocks, tan_next))

        for_columns(middle)
        wait_sends(par)

        @pl.when(layer > 0)
        def _():
            low_bits_and_send(par, tan_next)

        beta_part += dot_with_sums(lam_pre)

        def gamma_body(j, total):
            prod = lam_pre[j, 0] * pre[layer, j, 1] - lam_pre[j, 1] * pre[layer, j, 0]
            prod = prod * jnp.where(par == 0, cost[j], cost_b[j])
            return total + prod.reshape(tiles, 8, LANES).sum(axis=0)

        gamma_part = lax.fori_loop(0, nb, gamma_body, jnp.zeros((8, LANES), jnp.float32))
        acc[1 + layer] = 2.0 * gamma_part
        acc[1 + num_layers + layer] = beta_part
        return 0

    lax.fori_loop(0, num_layers, backward, 0)
    wait_sends((last + 1) % 2 if num_layers == 1 else 1)

    lane = lax.broadcasted_iota(jnp.int32, (1, LANES), 1)
    row = jnp.zeros((1, LANES), jnp.float32)
    for place in range(acc.shape[0]):
        value = jnp.sum(jnp.sum(acc[place], axis=0, keepdims=True), axis=1, keepdims=True)
        row = jnp.where(lane == place, value, row)
    part[...] = row
    for dy, dx, dc in offsets:
        y, x, dest = peer(dy, dx, dc)
        if dy or dx or dc:
            pltpu.make_async_remote_copy(
                src_ref=part, dst_ref=gath.at[me], send_sem=sum_send, recv_sem=sum_recv.at[me],
                device_id={"qy": y, "qx": x}, device_id_type=MESH_ID).start()
        else:
            pltpu.make_async_copy(part, gath.at[me], sum_recv.at[me]).start()

    def sum_wait(j, _):
        pltpu.make_async_copy(part, gath.at[j], sum_recv.at[j]).wait()
        return 0

    lax.fori_loop(0, nb, sum_wait, 0)
    totals[...] = lax.fori_loop(0, nb, lambda j, t: t + gath[j], jnp.zeros((1, LANES), jnp.float32))
    view = gath.at[pl.ds(0, nb - 1)]
    pltpu.make_async_copy(view, view, sum_send).wait()
    view = cost_b.at[pl.ds(0, nb - 1)]
    pltpu.make_async_copy(view, view, cost_send).wait()


def solution(mesh):
    ny, nx = mesh.shape["qy"], mesh.shape["qx"]
    nb = ny * nx

    def local_run(cost_local, gamma_angles, beta_angles):
        chunk = cost_local.shape[0]
        num_layers = gamma_angles.shape[0]
        rows = chunk // (nb * LANES)
        num_qubits = int(math.log2(chunk * nb))
        amp = (chunk * nb) ** -0.5
        vmem, smem = pltpu.VMEM, pltpu.SMEM
        state = (nb, 2, rows, LANES)
        f32 = jnp.float32
        final, totals = pl.pallas_call(
            functools.partial(kernel, ny, nx, num_layers, num_qubits, amp),
            out_shape=(jax.ShapeDtypeStruct((2, nb, rows, LANES), f32), jax.ShapeDtypeStruct((1, LANES), f32)),
            in_specs=[pl.BlockSpec(memory_space=vmem), pl.BlockSpec(memory_space=smem), pl.BlockSpec(memory_space=smem)],
            out_specs=(pl.BlockSpec(memory_space=vmem), pl.BlockSpec(memory_space=vmem)),
            scratch_shapes=[
                vmem((nb, rows, LANES), f32),
                vmem((num_layers, 2, nb, rows, LANES), f32),
                vmem((num_layers,) + state, f32),
                vmem((num_layers,) + state, f32),
                vmem((2,) + state, f32),
                vmem((2,) + state, f32),
                vmem(state, f32),
                vmem(state, f32),
                vmem(state, f32),
                vmem(state, f32),
                vmem((num_layers, 2, 8, LANES), f32),
                vmem((num_layers, 2 * LANES, 2 * LANES), f32),
                vmem((2 * LANES, 2 * LANES), f32),
                vmem((1 + 2 * num_layers, 8, LANES), f32),
                vmem((1, LANES), f32),
                vmem((nb, 1, LANES), f32),
                pltpu.SemaphoreType.DMA((2,)),
                pltpu.SemaphoreType.DMA((2, nb)),
                pltpu.SemaphoreType.DMA,
                pltpu.SemaphoreType.DMA((nb,)),
                pltpu.SemaphoreType.DMA,
                pltpu.SemaphoreType.DMA((nb,)),
            ],
            compiler_params=pltpu.CompilerParams(
                collective_id=0, has_side_effects=True, vmem_limit_bytes=48 * 1024 * 1024),
            name="qaoa",
        )(cost_local.reshape(nb, rows, LANES), gamma_angles, beta_angles)
        energy = totals[0, :1]
        grad = totals[0, 1:1 + 2 * num_layers]
        return energy, grad, final.reshape(2, chunk)

    state_spec = P(("inst", "qy", "qx"))
    return jax.shard_map(
        local_run, mesh=mesh, in_specs=(state_spec, P(), P()),
        out_specs=(P("inst"), P("inst"), P(None, ("inst", "qy", "qx"))), check_vma=False)
```

```python
import functools
import math

import jax
import jax.numpy as jnp
from jax import lax
from jax.experimental import pallas as pl
from jax.experimental.pallas import tpu as pltpu
from jax.sharding import PartitionSpec as P

LANES = 128
MESH_ID = pl.DeviceIdType.MESH


def mix_pair(blocks, tan_half, stride):
    out = list(blocks)
    for low in range(len(blocks)):
        if low & stride:
            continue
        high = low | stride
        (re0, im0), (re1, im1) = blocks[low], blocks[high]
        out[low] = (re0 + tan_half * im1, im0 - tan_half * re1)
        out[high] = (re1 + tan_half * im0, im1 - tan_half * re0)
    return out


def mix_all(blocks, tan_half):
    stride = 1
    while stride < len(blocks):
        blocks = mix_pair(blocks, tan_half, stride)
        stride *= 2
    return blocks


def partner_sums(blocks):
    out = []
    for place in range(len(blocks)):
        stride, re, im = 1, None, None
        while stride < len(blocks):
            pre, pim = blocks[place ^ stride]
            re, im = (pre, pim) if re is None else (re + pre, im + pim)
            stride *= 2
        out.append((re, im))
    return out


def sublane_partner(x, ids, dist):
    return jnp.take_along_axis(x, ids ^ dist, axis=1, mode="promise_in_bounds")


def swapped(x, stride):
    pairs = x.reshape((x.shape[0] // (2 * stride), 2, stride) + x.shape[1:])
    return jnp.concatenate([pairs[:, 1:], pairs[:, :1]], axis=1).reshape(x.shape)


def mix_leading(re, im, tan_half, size):
    stride = 1
    while stride < size:
        re, im = re + tan_half * swapped(im, stride), im - tan_half * swapped(re, stride)
        stride *= 2
    return re, im


def matmul(x, w):
    return jnp.dot(x, w, precision=lax.Precision.HIGHEST, preferred_element_type=jnp.float32)


def kernel(ny, nx, num_layers, num_qubits, amp, cost, gamma, beta, final, totals,
           cost_b, tabs, kept, recv, send, work, qbuf, angle, lane_mix, lane_sum, acc, part, gath,
           send_sem, recv_sem, cost_send, cost_recv, sum_send, sum_recv):
    nb = ny * nx
    chips = nx // 2
    last = num_layers - 1
    my_y = lax.axis_index("qy")
    my_x = lax.axis_index("qx")
    my_chip, my_core = my_x // 2, my_x % 2
    me = my_y * nx + my_x

    def peer(dy, dx, dc):
        y = (my_y + dy) % ny
        x = ((my_chip + dx) % chips) * 2 + (my_core + dc) % 2
        return y, x, y * nx + x

    dy_order = sorted(range(ny), key=lambda d: -min(d, ny - d))
    dx_order = sorted(range(chips), key=lambda d: -min(d, chips - d))
    offsets = [(dy, dx, dc) for dy in dy_order for dx in dx_order for dc in (1, 0) if dy or dx or dc]

    barrier = pltpu.get_barrier_semaphore()
    for dy, dx, dc in offsets:
        y, x, _ = peer(dy, dx, dc)
        pl.semaphore_signal(barrier, inc=1, device_id={"qy": y, "qx": x}, device_id_type=MESH_ID)

    def make_angle(layer):
        half = jnp.full((8, LANES), 0.5 * beta[layer], jnp.float32)
        cos_half, sin_half = jnp.cos(half), jnp.sin(half)
        scale, power, left = None, cos_half, num_qubits - 7
        while left:
            if left % 2:
                scale = power if scale is None else scale * power
            power, left = power * power, left // 2
        angle[layer, 0] = sin_half / cos_half
        angle[layer, 1] = scale
        return cos_half[:1], sin_half[:1]

    def make_lanes():
        flips = lax.broadcasted_iota(jnp.int32, (LANES, LANES), 0) ^ lax.broadcasted_iota(jnp.int32, (LANES, LANES), 1)
        weight = sum((flips >> bit) & 1 for bit in range(7))
        ones = jnp.where(weight == 1, 1.0, 0.0).astype(jnp.float32)
        lane_sum[:LANES, :LANES] = ones
        lane_sum[LANES:, LANES:] = ones
        lane_sum[:LANES, LANES:] = jnp.zeros_like(ones)
        lane_sum[LANES:, :LANES] = jnp.zeros_like(ones)
        for layer in range(num_layers):
            c, s = make_angle(layer)
            coefs = []
            for k in range(8):
                coef = None
                for factor in [c] * (7 - k) + [s] * k:
                    coef = factor if coef is None else coef * factor
                coefs.append(coef if (k // 2) % 2 == 0 else -coef)
            even, odd = jnp.zeros((LANES, LANES), jnp.float32), jnp.zeros((LANES, LANES), jnp.float32)
            for k in range(8):
                if k % 2 == 0:
                    even = jnp.where(weight == k, coefs[k], even)
                else:
                    odd = jnp.where(weight == k, coefs[k], odd)
            lane_mix[layer, :LANES, :LANES] = even
            lane_mix[layer, LANES:, LANES:] = even
            lane_mix[layer, LANES:, :LANES] = odd
            lane_mix[layer, :LANES, LANES:] = -odd

    def make_table(layer, source):
        g = gamma[layer]

        def body(j, _):
            for h in range(2):
                theta = g * source[j, h]
                tabs[layer, 0, h, j] = jnp.cos(theta)
                tabs[layer, 1, h, j] = jnp.sin(theta)
            return 0

        lax.fori_loop(0, nb, body, 0)

    def load(ref, places):
        return [(ref[h, j, 0], ref[h, j, 1]) for h, j in places]

    def store(ref, places, blocks):
        for (h, j), (re, im) in zip(places, blocks):
            ref[h, j, 0] = re
            ref[h, j, 1] = im

    def turn(blocks, layer, places):
        out = []
        for (re, im), (h, j) in zip(blocks, places):
            c, s = tabs[layer, 0, h, j], tabs[layer, 1, h, j]
            out.append((c * re + s * im, c * im - s * re))
        return out

    def scaled(blocks, scale):
        return [(scale * re, scale * im) for re, im in blocks]

    def column(x, halves):
        return [(h, y * nx + x) for y in range(ny) for h in halves]

    def for_columns(halves, body):
        lax.fori_loop(0, nx, lambda x, _: (body(column(x, halves)), 0)[1], 0)

    def load_row(ref, h, y):
        return ref[h, pl.ds(y * nx, nx), 0], ref[h, pl.ds(y * nx, nx), 1]

    def store_row(ref, h, y, row):
        for c in range(2):
            ref[h, pl.ds(y * nx, nx), c] = row[c]

    def send_half(par, h, tan_half):
        for dy in dy_order:
            y = (my_y + dy) % ny
            re, im = load_row(work, h, y)
            store_row(send.at[par], h, y, mix_leading(re, im, tan_half, nx))
            for dx in dx_order:
                for dc in (1, 0):
                    if dy or dx or dc:
                        _, x, dest = peer(dy, dx, dc)
                        pltpu.make_async_remote_copy(
                            src_ref=send.at[par, h, dest], dst_ref=recv.at[par, h, me],
                            send_sem=send_sem.at[par, h], recv_sem=recv_sem.at[par, h, me],
                            device_id={"qy": y, "qx": x}, device_id_type=MESH_ID).start()
        for c in range(2):
            recv[par, h, me, c] = send[par, h, me, c]

    def wait_sends(par, h):
        view = send.at[par, h, pl.ds(0, nb - 1)]
        pltpu.make_async_copy(view, view, send_sem.at[par, h]).wait()

    sub = lax.broadcasted_iota(jnp.int32, (nx, 8, LANES), 1)
    source_order = [(ny - dy) % ny for dy in dy_order]
    waves = [source_order[i:i + 2] for i in range(0, ny, 2)]

    def receive(par, h, layer, tan_half):
        for wave in waves:
            rows = []
            for dy in wave:
                y = (my_y + dy) % ny
                for dx in dx_order:
                    for dc in (1, 0):
                        if dy or dx or dc:
                            slot = peer(dy, dx, dc)[2]
                            view = recv.at[par, h, slot]
                            pltpu.make_async_copy(view, view, recv_sem.at[par, h, slot]).wait()
                re, im = load_row(recv.at[par], h, y)
                for dist in (1, 2, 4):
                    re, im = (re + tan_half * sublane_partner(im, sub, dist),
                              im - tan_half * sublane_partner(re, sub, dist))
                re, im = mix_leading(re, im, tan_half, nx)
                rows.append(jnp.concatenate([re.reshape(nx * 8, LANES), im.reshape(nx * 8, LANES)], axis=1))
            mixed = matmul(jnp.concatenate(rows, axis=0), lane_mix[layer])
            for k, dy in enumerate(wave):
                part_rows = mixed[k * nx * 8:(k + 1) * nx * 8]
                store_row(work, h, (my_y + dy) % ny, (part_rows[:, :LANES].reshape(nx, 8, LANES),
                                                      part_rows[:, LANES:].reshape(nx, 8, LANES)))

    def per_half(body):
        lax.fori_loop(0, 2, lambda h, _: (body(h), 0)[1], 0)

    make_angle(0)
    make_table(0, cost)
    tan0 = angle[0, 0]

    def first(places):
        flat = jnp.full((8, LANES), amp, jnp.float32)
        blocks = turn([(flat, jnp.zeros_like(flat)) for _ in places], 0, places)
        store(kept.at[num_layers], places, blocks)
        store(work, places, mix_all(blocks, tan0))

    for_columns((0, 1), first)
    for place in range(acc.shape[0]):
        acc[place] = jnp.zeros((8, LANES), jnp.float32)

    pl.semaphore_wait(barrier, nb - 1)

    for dy, dx, dc in offsets:
        y, x, dest = peer(dy, dx, dc)
        pltpu.make_async_remote_copy(
            src_ref=cost.at[dest], dst_ref=cost_b.at[me], send_sem=cost_send, recv_sem=cost_recv.at[me],
            device_id={"qy": y, "qx": x}, device_id_type=MESH_ID).start()
    for h in range(2):
        cost_b[me, h] = cost[me, h]
    per_half(lambda h: send_half(0, h, tan0))
    make_lanes()
    for dy, dx, dc in offsets:
        slot = peer(dy, dx, dc)[2]
        pltpu.make_async_copy(cost_b.at[slot], cost_b.at[slot], cost_recv.at[slot]).wait()
    make_table(1, cost_b)

    before_at, lam_pre, lam = num_layers, 2 * num_layers, 2 * num_layers + 1
    root = jnp.float32(1.0 / amp)
    zero = jnp.zeros((8, LANES), jnp.float32)
    pairs = num_layers // 2

    def plan(step):
        back = step // num_layers
        done = step + back * (2 * num_layers - 1 - 2 * step)
        return back, done, done + 1 - back, (done + 1 - 2 * back + num_layers) % num_layers

    def middle(step):
        back, done, turned, following = plan(step)
        tan_half, scale, tan_next = angle[done, 0], angle[done, 1], angle[following, 0]
        first_at = done + back * (lam_pre - done)
        second_at = before_at + turned + back * (lam - before_at - turned)

        def body(places):
            blocks = scaled(mix_all(load(work, places), tan_half), scale)
            store(kept.at[first_at], places, blocks)
            blocks = turn(blocks, turned, places)
            store(kept.at[second_at], places, blocks)
            store(work, places, mix_all(blocks, tan_next))

        return body

    def turn_point(places):
        tan_half, scale = angle[last, 0], angle[last, 1]
        blocks = scaled(mix_all(load(work, places), tan_half), scale)
        store(kept.at[last], places, blocks)
        conj = []
        energy = acc[0]
        for (h, j), (re, im) in zip(places, blocks):
            c = cost[j, h]
            final[0, j, h] = root * re
            final[1, j, h] = root * im
            conj.append((c * re, -(c * im)))
            energy += c * (re * re + im * im)
        acc[0] = energy
        store(kept.at[lam], places, conj)
        store(work, places, mix_all(conj, tan_half))

    def im_dot(conj, right):
        return conj[0] * right[1] + conj[1] * right[0]

    def sums_of(re, im, size):
        total_re, total_im, stride = swapped(re, 1), swapped(im, 1), 2
        while stride < size:
            total_re, total_im, stride = total_re + swapped(re, stride), total_im + swapped(im, stride), 2 * stride
        return total_re, total_im

    def high_sums(at):
        def body(x, _):
            for h in range(2):
                places = column(x, (h,))
                sums = partner_sums(load(kept.at[at], places))
                store(qbuf, places, [(a + c, b + d) for (a, b), (c, d) in zip(sums, load(qbuf, places))])
            return 0

        lax.fori_loop(0, nx, body, 0)

    def prepare(layer):
        def low(n, _):
            h, y = n // ny, n % ny
            re, im = load_row(kept.at[layer], h, y)
            store_row(qbuf, h, y, sums_of(re, im, nx))
            return 0

        lax.fori_loop(0, 2 * ny, low, 0)
        high_sums(layer)

        def body(j, total):
            for h in range(2):
                total += im_dot((kept[lam, h, j, 0], kept[lam, h, j, 1]), (qbuf[h, j, 0], qbuf[h, j, 1]))
            return total

        acc[1 + num_layers + layer] = lax.fori_loop(0, nb, body, zero)
        at = before_at + layer

        def inner(y, _):
            rows = [load_row(kept.at[at], h, y) for h in range(2)]
            x = jnp.concatenate([jnp.concatenate([re.reshape(nx * 8, LANES), im.reshape(nx * 8, LANES)], axis=1)
                                 for re, im in rows], axis=0)
            lanes = matmul(x, lane_sum[...])
            for h in range(2):
                sre, sim = sums_of(*rows[h], nx)
                (re, im), (ore, oim) = rows[h], rows[1 - h]
                for dist in (1, 2, 4):
                    sre += sublane_partner(re, sub, dist)
                    sim += sublane_partner(im, sub, dist)
                mine = lanes[h * nx * 8:(h + 1) * nx * 8]
                store_row(qbuf, h, y, (sre + ore + mine[:, :LANES].reshape(nx, 8, LANES),
                                       sim + oim + mine[:, LANES:].reshape(nx, 8, LANES)))
            return 0

        lax.fori_loop(0, ny, inner, 0)
        high_sums(at)

    def collect(layer, source):
        at = before_at + layer

        def body(j, sums):
            gamma_sum, beta_sum = sums
            for h in range(2):
                left = (kept[lam_pre, h, j, 0], kept[lam_pre, h, j, 1])
                gamma_sum += source[j, h] * im_dot(left, (kept[at, h, j, 0], kept[at, h, j, 1]))
                beta_sum += im_dot(left, (qbuf[h, j, 0], qbuf[h, j, 1]))
            return gamma_sum, beta_sum

        gamma_sum, beta_sum = lax.fori_loop(0, nb, body, (zero, zero))
        acc[1 + layer] = 2.0 * gamma_sum
        acc[1 + num_layers + layer] += beta_sum

    def last_sums(x, sums):
        gamma_sum, beta_sum = sums
        places = column(x, (0, 1))
        blocks = scaled(mix_all(load(work, places), angle[0, 0]), angle[0, 1])
        for (h, j), left, right, q in zip(places, blocks, load(kept.at[before_at], places), load(qbuf, places)):
            gamma_sum += cost[j, h] * im_dot(left, right)
            beta_sum += im_dot(left, q)
        return gamma_sum, beta_sum

    def two_gaps(k, _):
        step = 2 * k
        _, done, _, following = plan(step)
        tan_half, tan_next = angle[done, 0], angle[following, 0]

        def half(h):
            receive(0, h, done, tan_half)
            for_columns((h,), middle(step))

            @pl.when(k > 0)
            def _():
                wait_sends(1, h)

            send_half(1, h, tan_next)

        per_half(half)

        @pl.when(k < pairs - 1)
        def _():
            make_table(step + 2, cost)

        @pl.when(k >= pairs)
        def _():
            collect(done, cost_b)
            prepare(following)

        step = 2 * k + 1
        _, done, _, following = plan(step)
        tan_half = angle[done, 0]
        per_half(lambda h: receive(1, h, done, tan_half))

        @pl.when(k % pairs < pairs - 1)
        def _():
            for_columns((0, 1), middle(step))

        @pl.when(k == pairs - 1)
        def _():
            for_columns((0, 1), turn_point)

        @pl.when(k < 2 * pairs - 1)
        def _():
            tan_next = angle[following - (k // (pairs - 1)) * (1 - k // pairs) * (following - last), 0]

            def half_joint(h):
                wait_sends(0, h)
                send_half(0, h, tan_next)

            per_half(half_joint)

        @pl.when(k < pairs - 1)
        def _():
            make_table(step + 2, cost_b)

        @pl.when((k >= pairs) & (k < 2 * pairs - 1))
        def _():
            collect(done, cost)

        @pl.when((k >= pairs - 1) & (k < 2 * pairs - 1))
        def _():
            prepare(2 * num_layers - 3 - 2 * k)

        return 0

    lax.fori_loop(0, 2 * pairs, two_gaps, 0)
    gamma_sum, beta_sum = lax.fori_loop(0, nx, last_sums, (zero, zero))
    acc[1] = 2.0 * gamma_sum
    acc[1 + num_layers] += beta_sum

    lane = lax.broadcasted_iota(jnp.int32, (1, LANES), 1)
    row = jnp.zeros((1, LANES), jnp.float32)
    for place in range(acc.shape[0]):
        value = jnp.sum(jnp.sum(acc[place], axis=0, keepdims=True), axis=1, keepdims=True)
        row = jnp.where(lane == place, value, row)
    part[...] = row
    for dy, dx, dc in offsets:
        y, x, dest = peer(dy, dx, dc)
        pltpu.make_async_remote_copy(
            src_ref=part, dst_ref=gath.at[me], send_sem=sum_send, recv_sem=sum_recv.at[me],
            device_id={"qy": y, "qx": x}, device_id_type=MESH_ID).start()
    gath[me] = row
    for par in range(2):
        for h in range(2):
            wait_sends(par, h)
    view = cost_b.at[pl.ds(0, nb - 1)]
    pltpu.make_async_copy(view, view, cost_send).wait()
    for dy, dx, dc in offsets:
        slot = peer(dy, dx, dc)[2]
        pltpu.make_async_copy(part, gath.at[slot], sum_recv.at[slot]).wait()
    total = gath[0]
    for j in range(1, nb):
        total += gath[j]
    totals[...] = total
    view = gath.at[pl.ds(0, nb - 1)]
    pltpu.make_async_copy(view, view, sum_send).wait()


def solution(mesh):
    ny, nx = mesh.shape["qy"], mesh.shape["qx"]
    nb = ny * nx

    def local_run(cost_local, gamma_angles, beta_angles):
        chunk = cost_local.shape[0]
        num_layers = gamma_angles.shape[0]
        assert chunk == nb * 16 * LANES and num_layers % 2 == 0
        num_qubits = int(math.log2(chunk * nb))
        amp = (chunk * nb) ** -0.5
        vmem, smem, dma = pltpu.VMEM, pltpu.SMEM, pltpu.SemaphoreType.DMA
        f32 = jnp.float32
        state = (2, nb, 2, 8, LANES)
        final, totals = pl.pallas_call(
            functools.partial(kernel, ny, nx, num_layers, num_qubits, amp),
            out_shape=(jax.ShapeDtypeStruct((2, nb, 2, 8, LANES), f32), jax.ShapeDtypeStruct((1, LANES), f32)),
            in_specs=[pl.BlockSpec(memory_space=vmem), pl.BlockSpec(memory_space=smem), pl.BlockSpec(memory_space=smem)],
            out_specs=(pl.BlockSpec(memory_space=vmem), pl.BlockSpec(memory_space=vmem)),
            scratch_shapes=[
                vmem((nb, 2, 8, LANES), f32),
                vmem((num_layers, 2, 2, nb, 8, LANES), f32),
                vmem((2 * num_layers + 2,) + state, f32),
                vmem((2,) + state, f32),
                vmem((2,) + state, f32),
                vmem(state, f32),
                vmem(state, f32),
                vmem((num_layers, 2, 8, LANES), f32),
                vmem((num_layers, 2 * LANES, 2 * LANES), f32),
                vmem((2 * LANES, 2 * LANES), f32),
                vmem((1 + 2 * num_layers, 8, LANES), f32),
                vmem((1, LANES), f32),
                vmem((nb, 1, LANES), f32),
                dma((2, 2)),
                dma((2, 2, nb)),
                dma,
                dma((nb,)),
                dma,
                dma((nb,)),
            ],
            compiler_params=pltpu.CompilerParams(
                collective_id=0, has_side_effects=True, vmem_limit_bytes=48 * 1024 * 1024),
            name="qaoa",
        )(cost_local.reshape(nb, 2, 8, LANES), gamma_angles, beta_angles)
        energy = totals[0, :1]
        grad = totals[0, 1:1 + 2 * num_layers]
        return energy, grad, final.reshape(2, chunk)

    state_spec = P(("inst", "qy", "qx"))
    return jax.shard_map(
        local_run, mesh=mesh, in_specs=(state_spec, P(), P()),
        out_specs=(P("inst"), P("inst"), P(None, ("inst", "qy", "qx"))), check_vma=False)
```

```python
import functools
import math

import jax
import jax.numpy as jnp
from jax import lax
from jax.experimental import pallas as pl
from jax.experimental.pallas import tpu as pltpu
from jax.sharding import PartitionSpec as P

LANES = 128
MESH_ID = pl.DeviceIdType.MESH


def mix_pair(blocks, tan_half, stride):
    out = list(blocks)
    for low in range(len(blocks)):
        if low & stride:
            continue
        high = low | stride
        (re0, im0), (re1, im1) = blocks[low], blocks[high]
        out[low] = (re0 + tan_half * im1, im0 - tan_half * re1)
        out[high] = (re1 + tan_half * im0, im1 - tan_half * re0)
    return out


def mix_all(blocks, tan_half):
    stride = 1
    while stride < len(blocks):
        blocks = mix_pair(blocks, tan_half, stride)
        stride *= 2
    return blocks


def partner_sums(blocks):
    out = []
    for place in range(len(blocks)):
        stride, re, im = 1, None, None
        while stride < len(blocks):
            pre, pim = blocks[place ^ stride]
            re, im = (pre, pim) if re is None else (re + pre, im + pim)
            stride *= 2
        out.append((re, im))
    return out


def sublane_partner(x, ids, dist):
    return jnp.take_along_axis(x, ids ^ dist, axis=1, mode="promise_in_bounds")


def swapped(x, stride):
    pairs = x.reshape((x.shape[0] // (2 * stride), 2, stride) + x.shape[1:])
    return jnp.concatenate([pairs[:, 1:], pairs[:, :1]], axis=1).reshape(x.shape)


def mix_leading(re, im, tan_half, size):
    stride = 1
    while stride < size:
        re, im = re + tan_half * swapped(im, stride), im - tan_half * swapped(re, stride)
        stride *= 2
    return re, im


def matmul(x, w):
    return jnp.dot(x, w, precision=lax.Precision.HIGHEST, preferred_element_type=jnp.float32)


def kernel(ny, nx, num_layers, num_qubits, amp, cost_in, gamma_in, beta_in, final, totals,
           cost, gamma, beta, cost_b, tabs, kept, recv, send, work, qbuf, angle, lane_mix, lane_sum, acc, part, gath,
           load_sem, send_sem, recv_sem, cost_send, cost_recv, sum_send, sum_recv):
    nb = ny * nx
    chips = nx // 2
    last = num_layers - 1
    my_y = lax.axis_index("qy")
    my_x = lax.axis_index("qx")
    my_chip, my_core = my_x // 2, my_x % 2
    me = my_y * nx + my_x

    def peer(dy, dx, dc):
        y = (my_y + dy) % ny
        x = ((my_chip + dx) % chips) * 2 + (my_core + dc) % 2
        return y, x, y * nx + x

    dy_order = sorted(range(ny), key=lambda d: -min(d, ny - d))
    dx_order = sorted(range(chips), key=lambda d: -min(d, chips - d))
    offsets = [(dy, dx, dc) for dy in dy_order for dx in dx_order for dc in (1, 0) if dy or dx or dc]

    inputs = [pltpu.make_async_copy(src, dst, load_sem.at[n])
              for n, (src, dst) in enumerate([(gamma_in, gamma), (beta_in, beta), (cost_in, cost)])]
    for copy in inputs:
        copy.start()
    barrier = pltpu.get_barrier_semaphore()
    for dy, dx, dc in offsets:
        y, x, _ = peer(dy, dx, dc)
        pl.semaphore_signal(barrier, inc=1, device_id={"qy": y, "qx": x}, device_id_type=MESH_ID)

    def make_angle(layer):
        half = jnp.full((8, LANES), 0.5 * beta[layer], jnp.float32)
        cos_half, sin_half = jnp.cos(half), jnp.sin(half)
        scale, power, left = None, cos_half, num_qubits - 7
        while left:
            if left % 2:
                scale = power if scale is None else scale * power
            power, left = power * power, left // 2
        angle[layer, 0] = sin_half / cos_half
        angle[layer, 1] = scale
        return cos_half[:1], sin_half[:1]

    def make_lanes():
        flips = lax.broadcasted_iota(jnp.int32, (LANES, LANES), 0) ^ lax.broadcasted_iota(jnp.int32, (LANES, LANES), 1)
        weight = sum((flips >> bit) & 1 for bit in range(7))
        ones = jnp.where(weight == 1, 1.0, 0.0).astype(jnp.float32)
        lane_sum[:LANES, :LANES] = ones
        lane_sum[LANES:, LANES:] = ones
        lane_sum[:LANES, LANES:] = jnp.zeros_like(ones)
        lane_sum[LANES:, :LANES] = jnp.zeros_like(ones)
        for layer in range(num_layers):
            c, s = make_angle(layer)
            coefs = []
            for k in range(8):
                coef = None
                for factor in [c] * (7 - k) + [s] * k:
                    coef = factor if coef is None else coef * factor
                coefs.append(coef if (k // 2) % 2 == 0 else -coef)
            even, odd = jnp.zeros((LANES, LANES), jnp.float32), jnp.zeros((LANES, LANES), jnp.float32)
            for k in range(8):
                if k % 2 == 0:
                    even = jnp.where(weight == k, coefs[k], even)
                else:
                    odd = jnp.where(weight == k, coefs[k], odd)
            lane_mix[layer, :LANES, :LANES] = even
            lane_mix[layer, LANES:, LANES:] = even
            lane_mix[layer, LANES:, :LANES] = odd
            lane_mix[layer, :LANES, LANES:] = -odd

    def make_table(layer, source):
        g = gamma[layer]

        def body(j, _):
            for h in range(2):
                theta = g * source[j, h]
                tabs[layer, 0, h, j] = jnp.cos(theta)
                tabs[layer, 1, h, j] = jnp.sin(theta)
            return 0

        lax.fori_loop(0, nb, body, 0)

    def load(ref, places):
        return [(ref[h, j, 0], ref[h, j, 1]) for h, j in places]

    def store(ref, places, blocks):
        for (h, j), (re, im) in zip(places, blocks):
            ref[h, j, 0] = re
            ref[h, j, 1] = im

    def turn(blocks, layer, places):
        out = []
        for (re, im), (h, j) in zip(blocks, places):
            c, s = tabs[layer, 0, h, j], tabs[layer, 1, h, j]
            out.append((c * re + s * im, c * im - s * re))
        return out

    def scaled(blocks, scale):
        return [(scale * re, scale * im) for re, im in blocks]

    def column(x, halves):
        return [(h, y * nx + x) for y in range(ny) for h in halves]

    def for_columns(halves, body):
        lax.fori_loop(0, nx, lambda x, _: (body(column(x, halves)), 0)[1], 0)

    def load_row(ref, h, y):
        return ref[h, pl.ds(y * nx, nx), 0], ref[h, pl.ds(y * nx, nx), 1]

    def store_row(ref, h, y, row):
        for c in range(2):
            ref[h, pl.ds(y * nx, nx), c] = row[c]

    waves = [dy_order[:1]] + [dy_order[i:i + 2] for i in range(1, ny, 2)]

    def mix_lanes(rows, layer):
        x = jnp.concatenate([jnp.concatenate([re.reshape(nx * 8, LANES), im.reshape(nx * 8, LANES)], axis=1)
                             for re, im in rows], axis=0)
        x = matmul(x, lane_mix[layer])
        parts = [x[n * nx * 8:(n + 1) * nx * 8] for n in range(len(rows))]
        return [(p[:, :LANES].reshape(nx, 8, LANES), p[:, LANES:].reshape(nx, 8, LANES)) for p in parts]

    def send_half(par, h, layer, tan_half):
        rows = {dy: mix_leading(*load_row(work, h, (my_y + dy) % ny), tan_half, nx) for dy in dy_order}

        def leave(wave, dy):
            y = (my_y + dy) % ny
            store_row(send.at[par], h, y, rows[dy])
            for dx in dx_order:
                for dc in (1, 0):
                    if dy or dx or dc:
                        _, x, dest = peer(dy, dx, dc)
                        pltpu.make_async_remote_copy(
                            src_ref=send.at[par, h, dest], dst_ref=recv.at[par, h, me],
                            send_sem=send_sem.at[par, h], recv_sem=recv_sem.at[par, h, wave],
                            device_id={"qy": y, "qx": x}, device_id_type=MESH_ID).start()

        leave(0, dy_order[0])
        rest = dy_order[1:]
        rows.update(zip(rest, mix_lanes([rows[dy] for dy in rest], layer)))
        for n, wave in enumerate(waves[1:]):
            for dy in wave:
                leave(n + 1, dy)
        for c in range(2):
            recv[par, h, me, c] = send[par, h, me, c]

    def wait_sends(par, h):
        view = send.at[par, h, pl.ds(0, nb - 1)]
        pltpu.make_async_copy(view, view, send_sem.at[par, h]).wait()

    sub = lax.broadcasted_iota(jnp.int32, (nx, 8, LANES), 1)

    def receive(par, h, layer, tan_half):
        for n, wave in enumerate(waves):
            count = len(wave) * nx - (1 if 0 in wave else 0)
            view = recv.at[par, h, pl.ds(0, count)]
            pltpu.make_async_copy(view, view, recv_sem.at[par, h, n]).wait()
            for dy in wave:
                y = (my_y + ny - dy) % ny
                re, im = load_row(recv.at[par], h, y)
                for dist in (1, 2, 4):
                    re, im = (re + tan_half * sublane_partner(im, sub, dist),
                              im - tan_half * sublane_partner(re, sub, dist))
                re, im = mix_leading(re, im, tan_half, nx)
                if n == 0:
                    re, im = mix_lanes([(re, im)], layer)[0]
                store_row(work, h, y, (re, im))

    def per_half(body):
        lax.fori_loop(0, 2, lambda h, _: (body(h), 0)[1], 0)

    for copy in inputs:
        copy.wait()
    make_lanes()
    make_table(0, cost)
    tan0 = angle[0, 0]

    def first(places):
        flat = jnp.full((8, LANES), amp, jnp.float32)
        blocks = turn([(flat, jnp.zeros_like(flat)) for _ in places], 0, places)
        store(kept.at[num_layers], places, blocks)
        store(work, places, mix_all(blocks, tan0))

    for_columns((0, 1), first)
    for place in range(acc.shape[0]):
        acc[place] = jnp.zeros((8, LANES), jnp.float32)

    pl.semaphore_wait(barrier, nb - 1)

    for dy, dx, dc in offsets:
        y, x, dest = peer(dy, dx, dc)
        pltpu.make_async_remote_copy(
            src_ref=cost.at[dest], dst_ref=cost_b.at[me], send_sem=cost_send, recv_sem=cost_recv,
            device_id={"qy": y, "qx": x}, device_id_type=MESH_ID).start()
    for h in range(2):
        cost_b[me, h] = cost[me, h]
    per_half(lambda h: send_half(0, h, 0, tan0))
    view = cost_b.at[pl.ds(0, nb - 1)]
    pltpu.make_async_copy(view, view, cost_recv).wait()
    make_table(1, cost_b)

    before_at, lam_pre, lam = num_layers, 2 * num_layers, 2 * num_layers + 1
    root = jnp.float32(1.0 / amp)
    zero = jnp.zeros((8, LANES), jnp.float32)
    pairs = num_layers // 2

    def plan(step):
        back = step // num_layers
        done = step + back * (2 * num_layers - 1 - 2 * step)
        return back, done, done + 1 - back, (done + 1 - 2 * back + num_layers) % num_layers

    def middle(step):
        back, done, turned, following = plan(step)
        tan_half, scale, tan_next = angle[done, 0], angle[done, 1], angle[following, 0]
        first_at = done + back * (lam_pre - done)
        second_at = before_at + turned + back * (lam - before_at - turned)

        def body(places):
            blocks = scaled(mix_all(load(work, places), tan_half), scale)
            store(kept.at[first_at], places, blocks)
            blocks = turn(blocks, turned, places)
            store(kept.at[second_at], places, blocks)
            store(work, places, mix_all(blocks, tan_next))

        return body

    def turn_point(places):
        tan_half, scale = angle[last, 0], angle[last, 1]
        blocks = scaled(mix_all(load(work, places), tan_half), scale)
        store(kept.at[last], places, blocks)
        conj = []
        energy = acc[0]
        for (h, j), (re, im) in zip(places, blocks):
            c = cost[j, h]
            conj.append((c * re, -(c * im)))
            energy += c * (re * re + im * im)
        acc[0] = energy
        store(kept.at[lam], places, conj)
        store(work, places, mix_all(conj, tan_half))

    def im_dot(conj, right):
        return conj[0] * right[1] + conj[1] * right[0]

    def sums_of(re, im, size):
        total_re, total_im, stride = swapped(re, 1), swapped(im, 1), 2
        while stride < size:
            total_re, total_im, stride = total_re + swapped(re, stride), total_im + swapped(im, stride), 2 * stride
        return total_re, total_im

    def high_sums(at):
        def body(x, _):
            for h in range(2):
                places = column(x, (h,))
                sums = partner_sums(load(kept.at[at], places))
                store(qbuf, places, [(a + c, b + d) for (a, b), (c, d) in zip(sums, load(qbuf, places))])
            return 0

        lax.fori_loop(0, nx, body, 0)

    def prepare(layer):
        def low(n, _):
            h, y = n // ny, n % ny
            re, im = load_row(kept.at[layer], h, y)
            store_row(qbuf, h, y, sums_of(re, im, nx))
            return 0

        lax.fori_loop(0, 2 * ny, low, 0)
        high_sums(layer)

        def body(j, total):
            for h in range(2):
                total += im_dot((kept[lam, h, j, 0], kept[lam, h, j, 1]), (qbuf[h, j, 0], qbuf[h, j, 1]))
            return total

        acc[1 + num_layers + layer] = lax.fori_loop(0, nb, body, zero)
        at = before_at + layer

        def inner(y, _):
            rows = [load_row(kept.at[at], h, y) for h in range(2)]
            x = jnp.concatenate([jnp.concatenate([re.reshape(nx * 8, LANES), im.reshape(nx * 8, LANES)], axis=1)
                                 for re, im in rows], axis=0)
            lanes = matmul(x, lane_sum[...])
            for h in range(2):
                sre, sim = sums_of(*rows[h], nx)
                (re, im), (ore, oim) = rows[h], rows[1 - h]
                for dist in (1, 2, 4):
                    sre += sublane_partner(re, sub, dist)
                    sim += sublane_partner(im, sub, dist)
                mine = lanes[h * nx * 8:(h + 1) * nx * 8]
                store_row(qbuf, h, y, (sre + ore + mine[:, :LANES].reshape(nx, 8, LANES),
                                       sim + oim + mine[:, LANES:].reshape(nx, 8, LANES)))
            return 0

        lax.fori_loop(0, ny, inner, 0)
        high_sums(at)

    def collect(layer, source):
        at = before_at + layer

        def body(j, sums):
            gamma_sum, beta_sum = sums
            for h in range(2):
                left = (kept[lam_pre, h, j, 0], kept[lam_pre, h, j, 1])
                gamma_sum += source[j, h] * im_dot(left, (kept[at, h, j, 0], kept[at, h, j, 1]))
                beta_sum += im_dot(left, (qbuf[h, j, 0], qbuf[h, j, 1]))
            return gamma_sum, beta_sum

        gamma_sum, beta_sum = lax.fori_loop(0, nb, body, (zero, zero))
        acc[1 + layer] = 2.0 * gamma_sum
        acc[1 + num_layers + layer] += beta_sum

    def last_sums(x, sums):
        gamma_sum, beta_sum = sums
        places = column(x, (0, 1))
        blocks = scaled(mix_all(load(work, places), angle[0, 0]), angle[0, 1])
        for (h, j), left, right, q in zip(places, blocks, load(kept.at[before_at], places), load(qbuf, places)):
            gamma_sum += cost[j, h] * im_dot(left, right)
            beta_sum += im_dot(left, q)
        return gamma_sum, beta_sum

    def two_gaps(k, _):
        step = 2 * k
        _, done, _, following = plan(step)
        tan_half, tan_next = angle[done, 0], angle[following, 0]

        def half(h):
            receive(0, h, done, tan_half)
            for_columns((h,), middle(step))

            @pl.when(k > 0)
            def _():
                wait_sends(1, h)

            send_half(1, h, following, tan_next)

        per_half(half)

        @pl.when(k < pairs - 1)
        def _():
            make_table(step + 2, cost)

        @pl.when(k >= pairs)
        def _():
            collect(done, cost_b)
            prepare(following)

        step = 2 * k + 1
        _, done, _, following = plan(step)
        tan_half = angle[done, 0]
        per_half(lambda h: receive(1, h, done, tan_half))

        @pl.when(k % pairs < pairs - 1)
        def _():
            for_columns((0, 1), middle(step))

        @pl.when(k == pairs - 1)
        def _():
            for_columns((0, 1), turn_point)

        @pl.when(k < 2 * pairs - 1)
        def _():
            into = following - (k // (pairs - 1)) * (1 - k // pairs) * (following - last)
            tan_next = angle[into, 0]

            def half_joint(h):
                wait_sends(0, h)
                send_half(0, h, into, tan_next)

            per_half(half_joint)

        @pl.when(k < pairs - 1)
        def _():
            make_table(step + 2, cost_b)

        @pl.when(k == pairs - 1)
        def _():
            def write(j, _):
                for h in range(2):
                    for c in range(2):
                        final[c, j, h] = root * kept[last, h, j, c]
                return 0

            lax.fori_loop(0, nb, write, 0)

        @pl.when((k >= pairs) & (k < 2 * pairs - 1))
        def _():
            collect(done, cost)

        @pl.when((k >= pairs - 1) & (k < 2 * pairs - 1))
        def _():
            prepare(2 * num_layers - 3 - 2 * k)

        return 0

    lax.fori_loop(0, 2 * pairs, two_gaps, 0)
    gamma_sum, beta_sum = lax.fori_loop(0, nx, last_sums, (zero, zero))
    acc[1] = 2.0 * gamma_sum
    acc[1 + num_layers] += beta_sum

    lane = lax.broadcasted_iota(jnp.int32, (1, LANES), 1)
    row = jnp.zeros((1, LANES), jnp.float32)
    for place in range(acc.shape[0]):
        value = jnp.sum(jnp.sum(acc[place], axis=0, keepdims=True), axis=1, keepdims=True)
        row = jnp.where(lane == place, value, row)
    part[...] = row
    for dy, dx, dc in offsets:
        y, x, dest = peer(dy, dx, dc)
        pltpu.make_async_remote_copy(
            src_ref=part, dst_ref=gath.at[me], send_sem=sum_send, recv_sem=sum_recv,
            device_id={"qy": y, "qx": x}, device_id_type=MESH_ID).start()
    gath[me] = row
    for par in range(2):
        for h in range(2):
            wait_sends(par, h)
    view = cost_b.at[pl.ds(0, nb - 1)]
    pltpu.make_async_copy(view, view, cost_send).wait()
    view = gath.at[pl.ds(0, nb - 1)]
    pltpu.make_async_copy(view, view, sum_recv).wait()
    total = gath[0]
    for j in range(1, nb):
        total += gath[j]
    totals[...] = total
    view = gath.at[pl.ds(0, nb - 1)]
    pltpu.make_async_copy(view, view, sum_send).wait()


def solution(mesh):
    ny, nx = mesh.shape["qy"], mesh.shape["qx"]
    nb = ny * nx

    def local_run(cost_local, gamma_angles, beta_angles):
        chunk = cost_local.shape[0]
        num_layers = gamma_angles.shape[0]
        assert chunk == nb * 16 * LANES and num_layers % 2 == 0
        num_qubits = int(math.log2(chunk * nb))
        amp = (chunk * nb) ** -0.5
        vmem, smem, dma = pltpu.VMEM, pltpu.SMEM, pltpu.SemaphoreType.DMA
        f32 = jnp.float32
        state = (2, nb, 2, 8, LANES)
        final, totals = pl.pallas_call(
            functools.partial(kernel, ny, nx, num_layers, num_qubits, amp),
            out_shape=(jax.ShapeDtypeStruct((2, nb, 2, 8, LANES), f32), jax.ShapeDtypeStruct((1, LANES), f32)),
            in_specs=[pl.BlockSpec(memory_space=pl.ANY)] * 3,
            out_specs=(pl.BlockSpec(memory_space=vmem), pl.BlockSpec(memory_space=vmem)),
            scratch_shapes=[
                vmem((nb, 2, 8, LANES), f32),
                smem((num_layers,), f32),
                smem((num_layers,), f32),
                vmem((nb, 2, 8, LANES), f32),
                vmem((num_layers, 2, 2, nb, 8, LANES), f32),
                vmem((2 * num_layers + 2,) + state, f32),
                vmem((2,) + state, f32),
                vmem((2,) + state, f32),
                vmem(state, f32),
                vmem(state, f32),
                vmem((num_layers, 2, 8, LANES), f32),
                vmem((num_layers, 2 * LANES, 2 * LANES), f32),
                vmem((2 * LANES, 2 * LANES), f32),
                vmem((1 + 2 * num_layers, 8, LANES), f32),
                vmem((1, LANES), f32),
                vmem((nb, 1, LANES), f32),
                dma((3,)),
                dma((2, 2)),
                dma((2, 2, 1 + ny // 2)),
                dma,
                dma,
                dma,
                dma,
            ],
            compiler_params=pltpu.CompilerParams(
                collective_id=0, has_side_effects=True, vmem_limit_bytes=48 * 1024 * 1024),
            name="qaoa",
        )(cost_local.reshape(nb, 2, 8, LANES), gamma_angles, beta_angles)
        energy = totals[0, :1]
        grad = totals[0, 1:1 + 2 * num_layers]
        return energy, grad, final.reshape(2, chunk)

    state_spec = P(("inst", "qy", "qx"))
    return jax.shard_map(
        local_run, mesh=mesh, in_specs=(state_spec, P(), P()),
        out_specs=(P("inst"), P("inst"), P(None, ("inst", "qy", "qx"))), check_vma=False)
```

```python
import functools
import math

import jax
import jax.numpy as jnp
from jax import lax
from jax.experimental import pallas as pl
from jax.experimental.pallas import tpu as pltpu
from jax.sharding import PartitionSpec as P

LANES = 128
MESH_ID = pl.DeviceIdType.MESH


def mix_pair(blocks, tan_half, stride):
    out = list(blocks)
    for low in range(len(blocks)):
        if low & stride:
            continue
        high = low | stride
        (re0, im0), (re1, im1) = blocks[low], blocks[high]
        out[low] = (re0 + tan_half * im1, im0 - tan_half * re1)
        out[high] = (re1 + tan_half * im0, im1 - tan_half * re0)
    return out


def mix_all(blocks, tan_half):
    stride = 1
    while stride < len(blocks):
        blocks = mix_pair(blocks, tan_half, stride)
        stride *= 2
    return blocks


def partner_sums(blocks):
    out = []
    for place in range(len(blocks)):
        stride, re, im = 1, None, None
        while stride < len(blocks):
            pre, pim = blocks[place ^ stride]
            re, im = (pre, pim) if re is None else (re + pre, im + pim)
            stride *= 2
        out.append((re, im))
    return out


def sublane_partner(x, ids, dist):
    return jnp.take_along_axis(x, ids ^ dist, axis=1, mode="promise_in_bounds")


def swapped(x, stride):
    pairs = x.reshape((x.shape[0] // (2 * stride), 2, stride) + x.shape[1:])
    return jnp.concatenate([pairs[:, 1:], pairs[:, :1]], axis=1).reshape(x.shape)


def mix_leading(re, im, tan_half, size):
    stride = 1
    while stride < size:
        re, im = re + tan_half * swapped(im, stride), im - tan_half * swapped(re, stride)
        stride *= 2
    return re, im


def matmul(x, w):
    return jnp.dot(x, w, precision=lax.Precision.HIGHEST, preferred_element_type=jnp.float32)


def kernel(ny, nx, num_layers, num_qubits, amp, cost_in, gamma_in, beta_in, final, totals,
           cost, gamma, beta, cost_b, tabs, kept, recv, send, work, side, qbuf, angle, lane_mix, lane_sum, acc, part, gath,
           load_sem, send_sem, recv_sem, cost_send, cost_recv, sum_send, sum_recv):
    nb = ny * nx
    chips = nx // 2
    last = num_layers - 1
    my_y = lax.axis_index("qy")
    my_x = lax.axis_index("qx")
    my_chip, my_core = my_x // 2, my_x % 2
    me = my_y * nx + my_x

    def peer(dy, dx, dc):
        y = (my_y + dy) % ny
        x = ((my_chip + dx) % chips) * 2 + (my_core + dc) % 2
        return y, x, y * nx + x

    dy_order = sorted(range(ny), key=lambda d: -min(d, ny - d))
    dx_order = sorted(range(chips), key=lambda d: -min(d, chips - d))
    offsets = [(dy, dx, dc) for dy in dy_order for dx in dx_order for dc in (1, 0) if dy or dx or dc]

    inputs = [pltpu.make_async_copy(src, dst, load_sem.at[n])
              for n, (src, dst) in enumerate([(gamma_in, gamma), (beta_in, beta), (cost_in, cost)])]
    for copy in inputs:
        copy.start()
    barrier = pltpu.get_barrier_semaphore()
    for dy, dx, dc in offsets:
        y, x, _ = peer(dy, dx, dc)
        pl.semaphore_signal(barrier, inc=1, device_id={"qy": y, "qx": x}, device_id_type=MESH_ID)

    def make_angle(layer):
        half = jnp.full((8, LANES), 0.5 * beta[layer], jnp.float32)
        cos_half, sin_half = jnp.cos(half), jnp.sin(half)
        scale, power, left = None, cos_half, num_qubits - 7
        while left:
            if left % 2:
                scale = power if scale is None else scale * power
            power, left = power * power, left // 2
        angle[layer, 0] = sin_half / cos_half
        angle[layer, 1] = scale
        return cos_half[:1], sin_half[:1]

    def make_lanes():
        flips = lax.broadcasted_iota(jnp.int32, (LANES, LANES), 0) ^ lax.broadcasted_iota(jnp.int32, (LANES, LANES), 1)
        weight = sum((flips >> bit) & 1 for bit in range(7))
        ones = jnp.where(weight == 1, 1.0, 0.0).astype(jnp.float32)
        lane_sum[:LANES, :LANES] = ones
        lane_sum[LANES:, LANES:] = ones
        lane_sum[:LANES, LANES:] = jnp.zeros_like(ones)
        lane_sum[LANES:, :LANES] = jnp.zeros_like(ones)
        for layer in range(num_layers):
            c, s = make_angle(layer)
            coefs = []
            for k in range(8):
                coef = None
                for factor in [c] * (7 - k) + [s] * k:
                    coef = factor if coef is None else coef * factor
                coefs.append(coef if (k // 2) % 2 == 0 else -coef)
            even, odd = jnp.zeros((LANES, LANES), jnp.float32), jnp.zeros((LANES, LANES), jnp.float32)
            for k in range(8):
                if k % 2 == 0:
                    even = jnp.where(weight == k, coefs[k], even)
                else:
                    odd = jnp.where(weight == k, coefs[k], odd)
            lane_mix[layer, :LANES, :LANES] = even
            lane_mix[layer, LANES:, LANES:] = even
            lane_mix[layer, LANES:, :LANES] = odd
            lane_mix[layer, :LANES, LANES:] = -odd

    def make_table(layer, source):
        g = gamma[layer]

        def body(j, _):
            for h in range(2):
                theta = g * source[j, h]
                tabs[layer, 0, h, j] = jnp.cos(theta)
                tabs[layer, 1, h, j] = jnp.sin(theta)
            return 0

        lax.fori_loop(0, nb, body, 0)

    def load(ref, places):
        return [(ref[h, j, 0], ref[h, j, 1]) for h, j in places]

    def store(ref, places, blocks):
        for (h, j), (re, im) in zip(places, blocks):
            ref[h, j, 0] = re
            ref[h, j, 1] = im

    def turn(blocks, layer, places):
        out = []
        for (re, im), (h, j) in zip(blocks, places):
            c, s = tabs[layer, 0, h, j], tabs[layer, 1, h, j]
            out.append((c * re + s * im, c * im - s * re))
        return out

    def scaled(blocks, scale):
        return [(scale * re, scale * im) for re, im in blocks]

    def column(x, halves):
        return [(h, y * nx + x) for y in range(ny) for h in halves]

    def for_columns(halves, body):
        lax.fori_loop(0, nx, lambda x, _: (body(column(x, halves)), 0)[1], 0)

    def load_row(ref, h, y):
        return ref[h, pl.ds(y * nx, nx), 0], ref[h, pl.ds(y * nx, nx), 1]

    def store_row(ref, h, y, row):
        for c in range(2):
            ref[h, pl.ds(y * nx, nx), c] = row[c]

    waves = [dy_order[:1]] + [dy_order[i:i + 2] for i in range(1, ny, 2)]

    def mix_lanes(rows, layer):
        x = jnp.concatenate([jnp.concatenate([re.reshape(nx * 8, LANES), im.reshape(nx * 8, LANES)], axis=1)
                             for re, im in rows], axis=0)
        x = matmul(x, lane_mix[layer])
        parts = [x[n * nx * 8:(n + 1) * nx * 8] for n in range(len(rows))]
        return [(p[:, :LANES].reshape(nx, 8, LANES), p[:, LANES:].reshape(nx, 8, LANES)) for p in parts]

    def send_half(par, h, layer, tan_half, source):
        rows = {dy: mix_leading(*load_row(source, h, (my_y + dy) % ny), tan_half, nx) for dy in dy_order}

        def leave(wave, dy):
            y = (my_y + dy) % ny
            store_row(send.at[par], h, y, rows[dy])
            for dx in dx_order:
                for dc in (1, 0):
                    if dy or dx or dc:
                        _, x, dest = peer(dy, dx, dc)
                        pltpu.make_async_remote_copy(
                            src_ref=send.at[par, h, dest], dst_ref=recv.at[par, h, me],
                            send_sem=send_sem.at[par, h], recv_sem=recv_sem.at[par, h, wave],
                            device_id={"qy": y, "qx": x}, device_id_type=MESH_ID).start()

        leave(0, dy_order[0])
        rest = dy_order[1:]
        rows.update(zip(rest, mix_lanes([rows[dy] for dy in rest], layer)))
        for n, wave in enumerate(waves[1:]):
            for dy in wave:
                leave(n + 1, dy)
        for c in range(2):
            recv[par, h, me, c] = send[par, h, me, c]

    def wait_sends(par, h):
        view = send.at[par, h, pl.ds(0, nb - 1)]
        pltpu.make_async_copy(view, view, send_sem.at[par, h]).wait()

    sub = lax.broadcasted_iota(jnp.int32, (nx, 8, LANES), 1)

    def receive(par, h, layer, tan_half, target):
        for n, wave in enumerate(waves):
            count = len(wave) * nx - (1 if 0 in wave else 0)
            view = recv.at[par, h, pl.ds(0, count)]
            pltpu.make_async_copy(view, view, recv_sem.at[par, h, n]).wait()
            for dy in wave:
                y = (my_y + ny - dy) % ny
                re, im = load_row(recv.at[par], h, y)
                for dist in (1, 2, 4):
                    re, im = (re + tan_half * sublane_partner(im, sub, dist),
                              im - tan_half * sublane_partner(re, sub, dist))
                re, im = mix_leading(re, im, tan_half, nx)
                if n == 0:
                    re, im = mix_lanes([(re, im)], layer)[0]
                store_row(target, h, y, (re, im))

    def per_half(body):
        lax.fori_loop(0, 2, lambda h, _: (body(h), 0)[1], 0)

    for copy in inputs:
        copy.wait()
    make_lanes()
    make_table(0, cost)
    tan0 = angle[0, 0]

    def first(places):
        flat = jnp.full((8, LANES), amp, jnp.float32)
        blocks = turn([(flat, jnp.zeros_like(flat)) for _ in places], 0, places)
        store(kept.at[num_layers], places, blocks)
        store(work, places, mix_all(blocks, tan0))

    for_columns((0, 1), first)
    for place in range(acc.shape[0]):
        acc[place] = jnp.zeros((8, LANES), jnp.float32)

    pl.semaphore_wait(barrier, nb - 1)

    for dy, dx, dc in offsets:
        y, x, dest = peer(dy, dx, dc)
        pltpu.make_async_remote_copy(
            src_ref=cost.at[dest], dst_ref=cost_b.at[me], send_sem=cost_send, recv_sem=cost_recv,
            device_id={"qy": y, "qx": x}, device_id_type=MESH_ID).start()
    for h in range(2):
        cost_b[me, h] = cost[me, h]
    per_half(lambda h: send_half(0, h, 0, tan0, work))
    view = cost_b.at[pl.ds(0, nb - 1)]
    pltpu.make_async_copy(view, view, cost_recv).wait()
    make_table(1, cost_b)

    before_at, lam_pre, lam, side_at, sums_at = (num_layers, 2 * num_layers, 2 * num_layers + 1,
                                                 2 * num_layers + 2, 2 * num_layers + 4)
    root = jnp.float32(1.0 / amp)
    zero = jnp.zeros((8, LANES), jnp.float32)
    pairs = num_layers // 2

    def plan(step):
        back = step // num_layers
        done = step + back * (2 * num_layers - 1 - 2 * step)
        return back, done, done + 1 - back, (done + 1 - 2 * back + num_layers) % num_layers

    def middle(step):
        back, done, turned, following = plan(step)
        tan_half, scale, tan_next = angle[done, 0], angle[done, 1], angle[following, 0]
        first_at = done + back * (lam_pre - done)
        second_at = before_at + turned + back * (lam - before_at - turned)

        def body(places):
            blocks = scaled(mix_all(load(work, places), tan_half), scale)
            store(kept.at[first_at], places, blocks)
            blocks = turn(blocks, turned, places)
            store(kept.at[second_at], places, blocks)
            store(work, places, mix_all(blocks, tan_next))

        return body

    def turn_point(places):
        tan_half, scale = angle[last, 0], angle[last, 1]
        blocks = scaled(mix_all(load(work, places), tan_half), scale)
        store(kept.at[last], places, blocks)
        conj = []
        energy = acc[0]
        for (h, j), (re, im) in zip(places, blocks):
            c = cost[j, h]
            conj.append((c * re, -(c * im)))
            energy += c * (re * re + im * im)
        acc[0] = energy
        store(kept.at[lam], places, conj)
        store(work, places, mix_all(conj, tan_half))

    def im_dot(conj, right):
        return conj[0] * right[1] + conj[1] * right[0]

    def sums_of(re, im, size):
        total_re, total_im, stride = swapped(re, 1), swapped(im, 1), 2
        while stride < size:
            total_re, total_im, stride = total_re + swapped(re, stride), total_im + swapped(im, stride), 2 * stride
        return total_re, total_im

    def high_sums(at):
        def body(x, _):
            for h in range(2):
                places = column(x, (h,))
                sums = partner_sums(load(kept.at[at], places))
                store(qbuf, places, [(a + c, b + d) for (a, b), (c, d) in zip(sums, load(qbuf, places))])
            return 0

        lax.fori_loop(0, nx, body, 0)

    def low_sums(at):
        def low(n, _):
            h, y = n // ny, n % ny
            re, im = load_row(kept.at[at], h, y)
            store_row(qbuf, h, y, sums_of(re, im, nx))
            return 0

        lax.fori_loop(0, 2 * ny, low, 0)

    def full_sums(at):
        def inner(y, _):
            rows = [load_row(kept.at[at], h, y) for h in range(2)]
            x = jnp.concatenate([jnp.concatenate([re.reshape(nx * 8, LANES), im.reshape(nx * 8, LANES)], axis=1)
                                 for re, im in rows], axis=0)
            lanes = matmul(x, lane_sum[...])
            for h in range(2):
                sre, sim = sums_of(*rows[h], nx)
                (re, im), (ore, oim) = rows[h], rows[1 - h]
                for dist in (1, 2, 4):
                    sre += sublane_partner(re, sub, dist)
                    sim += sublane_partner(im, sub, dist)
                mine = lanes[h * nx * 8:(h + 1) * nx * 8]
                store_row(qbuf, h, y, (sre + ore + mine[:, :LANES].reshape(nx, 8, LANES),
                                       sim + oim + mine[:, LANES:].reshape(nx, 8, LANES)))
            return 0

        lax.fori_loop(0, ny, inner, 0)
        high_sums(at)

    def prepare(layer):
        low_sums(layer)
        high_sums(layer)

        def body(j, total):
            for h in range(2):
                total += im_dot((kept[lam, h, j, 0], kept[lam, h, j, 1]), (qbuf[h, j, 0], qbuf[h, j, 1]))
            return total

        acc[1 + num_layers + layer] = lax.fori_loop(0, nb, body, zero)
        full_sums(before_at + layer)

    def collect(layer, source):
        at = before_at + layer

        def body(j, sums):
            gamma_sum, beta_sum = sums
            for h in range(2):
                left = (kept[lam_pre, h, j, 0], kept[lam_pre, h, j, 1])
                gamma_sum += source[j, h] * im_dot(left, (kept[at, h, j, 0], kept[at, h, j, 1]))
                beta_sum += im_dot(left, (qbuf[h, j, 0], qbuf[h, j, 1]))
            return gamma_sum, beta_sum

        gamma_sum, beta_sum = lax.fori_loop(0, nb, body, (zero, zero))
        acc[1 + layer] = 2.0 * gamma_sum
        acc[1 + num_layers + layer] += beta_sum

    def side_source(k):
        @pl.when(k == 0)
        def _():
            def body(places):
                blocks = [(cost[j, h] * re, cost[j, h] * im)
                          for (h, j), (re, im) in zip(places, load(kept.at[before_at], places))]
                store(side, places, mix_all(blocks, tan0))

            for_columns((0, 1), body)

        @pl.when(k == 2)
        def _():
            low_sums(before_at)
            high_sums(before_at)
            for_columns((0, 1), lambda places: store(side, places, mix_all(load(qbuf, places), tan0)))

    def side_arrival(n):
        per_half(lambda h: receive(2 + n, h, 0, tan0, side))

        def body(places):
            for h in range(2):
                mine = places[h::2]
                store(kept.at[side_at + n], mine, scaled(mix_all(load(side, mine), tan0), angle[0, 1]))

        for_columns((0, 1), body)

    def side_sums():
        full_sums(0)

        def body(j, _):
            for h in range(2):
                for c in range(2):
                    kept[sums_at, h, j, c] = qbuf[h, j, c] + kept[side_at + 1, h, j, c]
            return 0

        lax.fori_loop(0, nb, body, 0)

    def last_sums(h):
        def body(x, sums):
            gamma1, beta1, gamma0, beta0 = sums
            places = column(x, (h,))
            blocks = scaled(mix_all(load(work, places), angle[1, 0]), angle[1, 1])
            for (h_, j), left, right, q in zip(places, blocks, load(kept.at[before_at + 1], places), load(qbuf, places)):
                gamma1 += cost_b[j, h_] * im_dot(left, right)
                beta1 += im_dot(left, q)
            blocks = turn(blocks, 1, places)
            for left, right, q in zip(blocks, load(kept.at[side_at], places), load(kept.at[sums_at], places)):
                gamma0 += im_dot(left, right)
                beta0 += im_dot(left, q)
            return gamma1, beta1, gamma0, beta0

        gamma1, beta1, gamma0, beta0 = lax.fori_loop(0, nx, body, (zero,) * 4)
        acc[1] += 2.0 * gamma0
        acc[2] += 2.0 * gamma1
        acc[1 + num_layers] += beta0
        acc[2 + num_layers] += beta1

    def two_gaps(k, _):
        step = 2 * k
        _, done, _, following = plan(step)
        tan_half, tan_next = angle[done, 0], angle[following, 0]

        def half(h):
            receive(0, h, done, tan_half, work)
            for_columns((h,), middle(step))

            @pl.when(k > 0)
            def _():
                wait_sends(1, h)

            send_half(1, h, following, tan_next, work)

        per_half(half)

        side_source(k)

        @pl.when(k < 4)
        def _():
            send_half(2 + k // 2, k % 2, 0, tan0, side)

        @pl.when(k < pairs - 1)
        def _():
            make_table(step + 2, cost)

        @pl.when(k >= pairs)
        def _():
            collect(done, cost_b)
            prepare(following)

        step = 2 * k + 1
        _, done, _, following = plan(step)
        tan_half = angle[done, 0]
        per_half(lambda h: receive(1, h, done, tan_half, work))

        @pl.when(k % pairs < pairs - 1)
        def _():
            for_columns((0, 1), middle(step))

        @pl.when(k == pairs - 1)
        def _():
            for_columns((0, 1), turn_point)

        into = following - (k // (pairs - 1)) * (1 - k // pairs) * (following - last)
        tan_next = angle[into, 0]

        def half_joint(h):
            wait_sends(0, h)
            send_half(0, h, into, tan_next, work)

        per_half(half_joint)

        @pl.when(k < pairs - 1)
        def _():
            make_table(step + 2, cost_b)

        @pl.when(k == pairs - 1)
        def _():
            def write(j, _):
                for h in range(2):
                    for c in range(2):
                        final[c, j, h] = root * kept[last, h, j, c]
                return 0

            lax.fori_loop(0, nb, write, 0)

        @pl.when(k >= pairs)
        def _():
            collect(done, cost)

        @pl.when((k == 4) | (k == 5))
        def _():
            side_arrival(k - 4)

        @pl.when(k == 2 * pairs - 2)
        def _():
            side_sums()

        @pl.when(k >= pairs - 1)
        def _():
            prepare(2 * num_layers - 3 - 2 * k)

        return 0

    lax.fori_loop(0, 2 * pairs - 1, two_gaps, 0)

    def last_half(h):
        receive(0, h, 1, angle[1, 0], work)
        last_sums(h)

    per_half(last_half)

    lane = lax.broadcasted_iota(jnp.int32, (1, LANES), 1)
    row = jnp.zeros((1, LANES), jnp.float32)
    for place in range(acc.shape[0]):
        value = jnp.sum(jnp.sum(acc[place], axis=0, keepdims=True), axis=1, keepdims=True)
        row = jnp.where(lane == place, value, row)
    part[...] = row
    for dy, dx, dc in offsets:
        y, x, dest = peer(dy, dx, dc)
        pltpu.make_async_remote_copy(
            src_ref=part, dst_ref=gath.at[me], send_sem=sum_send, recv_sem=sum_recv,
            device_id={"qy": y, "qx": x}, device_id_type=MESH_ID).start()
    gath[me] = row
    for par in range(4):
        for h in range(2):
            wait_sends(par, h)
    view = cost_b.at[pl.ds(0, nb - 1)]
    pltpu.make_async_copy(view, view, cost_send).wait()
    view = gath.at[pl.ds(0, nb - 1)]
    pltpu.make_async_copy(view, view, sum_recv).wait()
    total = gath[0]
    for j in range(1, nb):
        total += gath[j]
    totals[...] = total
    view = gath.at[pl.ds(0, nb - 1)]
    pltpu.make_async_copy(view, view, sum_send).wait()


def solution(mesh):
    ny, nx = mesh.shape["qy"], mesh.shape["qx"]
    nb = ny * nx

    def local_run(cost_local, gamma_angles, beta_angles):
        chunk = cost_local.shape[0]
        num_layers = gamma_angles.shape[0]
        assert chunk == nb * 16 * LANES and num_layers % 2 == 0 and num_layers >= 8
        num_qubits = int(math.log2(chunk * nb))
        amp = (chunk * nb) ** -0.5
        vmem, smem, dma = pltpu.VMEM, pltpu.SMEM, pltpu.SemaphoreType.DMA
        f32 = jnp.float32
        state = (2, nb, 2, 8, LANES)
        final, totals = pl.pallas_call(
            functools.partial(kernel, ny, nx, num_layers, num_qubits, amp),
            out_shape=(jax.ShapeDtypeStruct((2, nb, 2, 8, LANES), f32), jax.ShapeDtypeStruct((1, LANES), f32)),
            in_specs=[pl.BlockSpec(memory_space=pltpu.MemorySpace.HBM)] * 3,
            out_specs=(pl.BlockSpec(memory_space=vmem), pl.BlockSpec(memory_space=vmem)),
            scratch_shapes=[
                vmem((nb, 2, 8, LANES), f32),
                smem((num_layers,), f32),
                smem((num_layers,), f32),
                vmem((nb, 2, 8, LANES), f32),
                vmem((num_layers, 2, 2, nb, 8, LANES), f32),
                vmem((2 * num_layers + 5,) + state, f32),
                vmem((4,) + state, f32),
                vmem((4,) + state, f32),
                vmem(state, f32),
                vmem(state, f32),
                vmem(state, f32),
                vmem((num_layers, 2, 8, LANES), f32),
                vmem((num_layers, 2 * LANES, 2 * LANES), f32),
                vmem((2 * LANES, 2 * LANES), f32),
                vmem((1 + 2 * num_layers, 8, LANES), f32),
                vmem((1, LANES), f32),
                vmem((nb, 1, LANES), f32),
                dma((3,)),
                dma((4, 2)),
                dma((4, 2, 1 + ny // 2)),
                dma,
                dma,
                dma,
                dma,
            ],
            compiler_params=pltpu.CompilerParams(
                collective_id=0, has_side_effects=True, vmem_limit_bytes=48 * 1024 * 1024),
            name="qaoa",
        )(cost_local.reshape(nb, 2, 8, LANES), gamma_angles, beta_angles)
        energy = totals[0, :1]
        grad = totals[0, 1:1 + 2 * num_layers]
        return energy, grad, final.reshape(2, chunk)

    state_spec = P(("inst", "qy", "qx"))
    return jax.shard_map(
        local_run, mesh=mesh, in_specs=(state_spec, P(), P()),
        out_specs=(P("inst"), P("inst"), P(None, ("inst", "qy", "qx"))), check_vma=False)
```

```python
import functools
import math

import jax
import jax.numpy as jnp
from jax import lax
from jax.experimental import pallas as pl
from jax.experimental.pallas import tpu as pltpu
from jax.sharding import PartitionSpec as P

LANES = 128
MESH_ID = pl.DeviceIdType.MESH


def mix_pair(blocks, tan_half, stride):
    out = list(blocks)
    for low in range(len(blocks)):
        if low & stride:
            continue
        high = low | stride
        (re0, im0), (re1, im1) = blocks[low], blocks[high]
        out[low] = (re0 + tan_half * im1, im0 - tan_half * re1)
        out[high] = (re1 + tan_half * im0, im1 - tan_half * re0)
    return out


def mix_all(blocks, tan_half):
    stride = 1
    while stride < len(blocks):
        blocks = mix_pair(blocks, tan_half, stride)
        stride *= 2
    return blocks


def partner_sums(blocks):
    out = []
    for place in range(len(blocks)):
        stride, re, im = 1, None, None
        while stride < len(blocks):
            pre, pim = blocks[place ^ stride]
            re, im = (pre, pim) if re is None else (re + pre, im + pim)
            stride *= 2
        out.append((re, im))
    return out


def sublane_partner(x, ids, dist):
    return jnp.take_along_axis(x, ids ^ dist, axis=1, mode="promise_in_bounds")


def swapped(x, stride):
    pairs = x.reshape((x.shape[0] // (2 * stride), 2, stride) + x.shape[1:])
    return jnp.concatenate([pairs[:, 1:], pairs[:, :1]], axis=1).reshape(x.shape)


def mix_leading(re, im, tan_half, size):
    stride = 1
    while stride < size:
        re, im = re + tan_half * swapped(im, stride), im - tan_half * swapped(re, stride)
        stride *= 2
    return re, im


def matmul(x, w):
    return jnp.dot(x, w, precision=lax.Precision.HIGHEST, preferred_element_type=jnp.float32)


def kernel(ny, nx, num_layers, num_qubits, amp, cost_in, gamma_in, beta_in, final, totals,
           cost, gamma, beta, cost_b, tabs, kept, recv, send, work, side, qbuf, angle, lane_mix, lane_sum, acc, part, gath,
           load_sem, send_sem, recv_sem, cost_send, cost_recv, sum_send, sum_recv):
    nb = ny * nx
    chips = nx // 2
    last = num_layers - 1
    my_y = lax.axis_index("qy")
    my_x = lax.axis_index("qx")
    my_chip, my_core = my_x // 2, my_x % 2
    me = my_y * nx + my_x

    def peer(dy, dx, dc):
        y = (my_y + dy) % ny
        x = ((my_chip + dx) % chips) * 2 + (my_core + dc) % 2
        return y, x, y * nx + x

    dy_order = sorted(range(ny), key=lambda d: -min(d, ny - d))
    dx_order = sorted(range(chips), key=lambda d: -min(d, chips - d))
    offsets = [(dy, dx, dc) for dy in dy_order for dx in dx_order for dc in (1, 0) if dy or dx or dc]

    inputs = [pltpu.make_async_copy(src, dst, load_sem.at[n])
              for n, (src, dst) in enumerate([(gamma_in, gamma), (beta_in, beta), (cost_in, cost)])]
    for copy in inputs:
        copy.start()
    barrier = pltpu.get_barrier_semaphore()
    for dy, dx, dc in offsets:
        y, x, _ = peer(dy, dx, dc)
        pl.semaphore_signal(barrier, inc=1, device_id={"qy": y, "qx": x}, device_id_type=MESH_ID)

    def make_angle(layer):
        half = jnp.full((8, LANES), 0.5 * beta[layer], jnp.float32)
        cos_half, sin_half = jnp.cos(half), jnp.sin(half)
        scale, power, left = None, cos_half, num_qubits - 7
        while left:
            if left % 2:
                scale = power if scale is None else scale * power
            power, left = power * power, left // 2
        angle[layer, 0] = sin_half / cos_half
        angle[layer, 1] = scale
        return cos_half[:1], sin_half[:1]

    def make_lanes(layers):
        flips = lax.broadcasted_iota(jnp.int32, (LANES, LANES), 0) ^ lax.broadcasted_iota(jnp.int32, (LANES, LANES), 1)
        weight = sum((flips >> bit) & 1 for bit in range(7))
        for layer in layers:
            c, s = make_angle(layer)
            coefs = []
            for k in range(8):
                coef = None
                for factor in [c] * (7 - k) + [s] * k:
                    coef = factor if coef is None else coef * factor
                coefs.append(coef if (k // 2) % 2 == 0 else -coef)
            even, odd = jnp.zeros((LANES, LANES), jnp.float32), jnp.zeros((LANES, LANES), jnp.float32)
            for k in range(8):
                if k % 2 == 0:
                    even = jnp.where(weight == k, coefs[k], even)
                else:
                    odd = jnp.where(weight == k, coefs[k], odd)
            lane_mix[layer, :LANES, :LANES] = even
            lane_mix[layer, LANES:, LANES:] = even
            lane_mix[layer, LANES:, :LANES] = odd
            lane_mix[layer, :LANES, LANES:] = -odd
        if 0 not in layers:
            ones = jnp.where(weight == 1, 1.0, 0.0).astype(jnp.float32)
            lane_sum[:LANES, :LANES] = ones
            lane_sum[LANES:, LANES:] = ones
            lane_sum[:LANES, LANES:] = jnp.zeros_like(ones)
            lane_sum[LANES:, :LANES] = jnp.zeros_like(ones)

    def make_table(layer, source):
        g = gamma[layer]

        def body(j, _):
            for h in range(2):
                theta = g * source[j, h]
                tabs[layer, 0, h, j] = jnp.cos(theta)
                tabs[layer, 1, h, j] = jnp.sin(theta)
            return 0

        lax.fori_loop(0, nb, body, 0)

    def load(ref, places):
        return [(ref[h, j, 0], ref[h, j, 1]) for h, j in places]

    def store(ref, places, blocks):
        for (h, j), (re, im) in zip(places, blocks):
            ref[h, j, 0] = re
            ref[h, j, 1] = im

    def turn(blocks, layer, places):
        out = []
        for (re, im), (h, j) in zip(blocks, places):
            c, s = tabs[layer, 0, h, j], tabs[layer, 1, h, j]
            out.append((c * re + s * im, c * im - s * re))
        return out

    def scaled(blocks, scale):
        return [(scale * re, scale * im) for re, im in blocks]

    def column(x, halves):
        return [(h, y * nx + x) for y in range(ny) for h in halves]

    def for_columns(halves, body):
        lax.fori_loop(0, nx, lambda x, _: (body(column(x, halves)), 0)[1], 0, unroll=2)

    def load_row(ref, h, y):
        return ref[h, pl.ds(y * nx, nx), 0], ref[h, pl.ds(y * nx, nx), 1]

    def store_row(ref, h, y, row):
        for c in range(2):
            ref[h, pl.ds(y * nx, nx), c] = row[c]

    waves = [dy_order[:1]] + [dy_order[i:i + 2] for i in range(1, ny, 2)]

    def mix_lanes(rows, layer):
        x = jnp.concatenate([jnp.concatenate([re.reshape(nx * 8, LANES), im.reshape(nx * 8, LANES)], axis=1)
                             for re, im in rows], axis=0)
        x = matmul(x, lane_mix[layer])
        parts = [x[n * nx * 8:(n + 1) * nx * 8] for n in range(len(rows))]
        return [(p[:, :LANES].reshape(nx, 8, LANES), p[:, LANES:].reshape(nx, 8, LANES)) for p in parts]

    def send_half(par, h, layer, tan_half, source):
        rows = {dy: mix_leading(*load_row(source, h, (my_y + dy) % ny), tan_half, nx) for dy in dy_order}

        def leave(wave, dy):
            y = (my_y + dy) % ny
            store_row(send.at[par], h, y, rows[dy])
            for dx in dx_order:
                for dc in (1, 0):
                    if dy or dx or dc:
                        _, x, dest = peer(dy, dx, dc)
                        pltpu.make_async_remote_copy(
                            src_ref=send.at[par, h, dest], dst_ref=recv.at[par, h, me],
                            send_sem=send_sem.at[par, h], recv_sem=recv_sem.at[par, h, wave],
                            device_id={"qy": y, "qx": x}, device_id_type=MESH_ID).start()

        leave(0, dy_order[0])
        rest = dy_order[1:]
        rows.update(zip(rest, mix_lanes([rows[dy] for dy in rest], layer)))
        for n, wave in enumerate(waves[1:]):
            for dy in wave:
                leave(n + 1, dy)
        for c in range(2):
            recv[par, h, me, c] = send[par, h, me, c]

    def wait_sends(par, h):
        view = send.at[par, h, pl.ds(0, nb - 1)]
        pltpu.make_async_copy(view, view, send_sem.at[par, h]).wait()

    sub = lax.broadcasted_iota(jnp.int32, (nx, 8, LANES), 1)

    def receive(par, h, layer, tan_half, target):
        for n, wave in enumerate(waves):
            count = len(wave) * nx - (1 if 0 in wave else 0)
            view = recv.at[par, h, pl.ds(0, count)]
            pltpu.make_async_copy(view, view, recv_sem.at[par, h, n]).wait()
            for dy in wave:
                y = (my_y + ny - dy) % ny
                re, im = load_row(recv.at[par], h, y)
                for dist in (1, 2, 4):
                    re, im = (re + tan_half * sublane_partner(im, sub, dist),
                              im - tan_half * sublane_partner(re, sub, dist))
                re, im = mix_leading(re, im, tan_half, nx)
                if n == 0:
                    re, im = mix_lanes([(re, im)], layer)[0]
                store_row(target, h, y, (re, im))

    def per_half(body):
        lax.fori_loop(0, 2, lambda h, _: (body(h), 0)[1], 0)

    for copy in inputs:
        copy.wait()
    make_lanes([0])
    make_table(0, cost)
    tan0 = angle[0, 0]

    def first(places):
        flat = jnp.full((8, LANES), amp, jnp.float32)
        blocks = turn([(flat, jnp.zeros_like(flat)) for _ in places], 0, places)
        store(kept.at[num_layers], places, blocks)
        store(work, places, mix_all(blocks, tan0))

    for_columns((0, 1), first)
    for place in range(acc.shape[0]):
        acc[place] = jnp.zeros((8, LANES), jnp.float32)

    pl.semaphore_wait(barrier, nb - 1)

    for dy, dx, dc in offsets:
        y, x, dest = peer(dy, dx, dc)
        pltpu.make_async_remote_copy(
            src_ref=cost.at[dest], dst_ref=cost_b.at[me], send_sem=cost_send, recv_sem=cost_recv,
            device_id={"qy": y, "qx": x}, device_id_type=MESH_ID).start()
    for h in range(2):
        cost_b[me, h] = cost[me, h]
    per_half(lambda h: send_half(0, h, 0, tan0, work))
    make_lanes(range(1, num_layers))
    view = cost_b.at[pl.ds(0, nb - 1)]
    pltpu.make_async_copy(view, view, cost_recv).wait()
    make_table(1, cost_b)

    before_at, lam_pre, lam, side_at, sums_at = (num_layers, 2 * num_layers, 2 * num_layers + 1,
                                                 2 * num_layers + 2, 2 * num_layers + 4)
    root = jnp.float32(1.0 / amp)
    zero = jnp.zeros((8, LANES), jnp.float32)
    pairs = num_layers // 2

    def plan(step):
        back = step // num_layers
        done = step + back * (2 * num_layers - 1 - 2 * step)
        return back, done, done + 1 - back, (done + 1 - 2 * back + num_layers) % num_layers

    def middle(step):
        back, done, turned, following = plan(step)
        tan_half, scale, tan_next = angle[done, 0], angle[done, 1], angle[following, 0]
        first_at = done + back * (lam_pre - done)
        second_at = before_at + turned + back * (lam - before_at - turned)

        def body(places):
            blocks = scaled(mix_all(load(work, places), tan_half), scale)
            store(kept.at[first_at], places, blocks)
            blocks = turn(blocks, turned, places)
            store(kept.at[second_at], places, blocks)
            store(work, places, mix_all(blocks, tan_next))

        return body

    def turn_point(places):
        tan_half, scale = angle[last, 0], angle[last, 1]
        blocks = scaled(mix_all(load(work, places), tan_half), scale)
        store(kept.at[last], places, blocks)
        conj = []
        energy = acc[0]
        for (h, j), (re, im) in zip(places, blocks):
            c = cost[j, h]
            conj.append((c * re, -(c * im)))
            energy += c * (re * re + im * im)
        acc[0] = energy
        store(kept.at[lam], places, conj)
        store(work, places, mix_all(conj, tan_half))

    def im_dot(conj, right):
        return conj[0] * right[1] + conj[1] * right[0]

    def sums_of(re, im, size):
        total_re, total_im, stride = swapped(re, 1), swapped(im, 1), 2
        while stride < size:
            total_re, total_im, stride = total_re + swapped(re, stride), total_im + swapped(im, stride), 2 * stride
        return total_re, total_im

    def high_sums(at):
        def body(x, _):
            for h in range(2):
                places = column(x, (h,))
                sums = partner_sums(load(kept.at[at], places))
                store(qbuf, places, [(a + c, b + d) for (a, b), (c, d) in zip(sums, load(qbuf, places))])
            return 0

        lax.fori_loop(0, nx, body, 0)

    def low_sums(at):
        def low(n, _):
            h, y = n // ny, n % ny
            re, im = load_row(kept.at[at], h, y)
            store_row(qbuf, h, y, sums_of(re, im, nx))
            return 0

        lax.fori_loop(0, 2 * ny, low, 0)

    def full_sums(at):
        def inner(y, _):
            rows = [load_row(kept.at[at], h, y) for h in range(2)]
            x = jnp.concatenate([jnp.concatenate([re.reshape(nx * 8, LANES), im.reshape(nx * 8, LANES)], axis=1)
                                 for re, im in rows], axis=0)
            lanes = matmul(x, lane_sum[...])
            for h in range(2):
                sre, sim = sums_of(*rows[h], nx)
                (re, im), (ore, oim) = rows[h], rows[1 - h]
                for dist in (1, 2, 4):
                    sre += sublane_partner(re, sub, dist)
                    sim += sublane_partner(im, sub, dist)
                mine = lanes[h * nx * 8:(h + 1) * nx * 8]
                store_row(qbuf, h, y, (sre + ore + mine[:, :LANES].reshape(nx, 8, LANES),
                                       sim + oim + mine[:, LANES:].reshape(nx, 8, LANES)))
            return 0

        lax.fori_loop(0, ny, inner, 0)
        high_sums(at)

    def prepare(layer):
        low_sums(layer)
        high_sums(layer)

        def body(j, total):
            for h in range(2):
                total += im_dot((kept[lam, h, j, 0], kept[lam, h, j, 1]), (qbuf[h, j, 0], qbuf[h, j, 1]))
            return total

        acc[1 + num_layers + layer] = lax.fori_loop(0, nb, body, zero)
        full_sums(before_at + layer)

    def collect(layer, source):
        at = before_at + layer

        def body(j, sums):
            gamma_sum, beta_sum = sums
            for h in range(2):
                left = (kept[lam_pre, h, j, 0], kept[lam_pre, h, j, 1])
                gamma_sum += source[j, h] * im_dot(left, (kept[at, h, j, 0], kept[at, h, j, 1]))
                beta_sum += im_dot(left, (qbuf[h, j, 0], qbuf[h, j, 1]))
            return gamma_sum, beta_sum

        gamma_sum, beta_sum = lax.fori_loop(0, nb, body, (zero, zero))
        acc[1 + layer] = 2.0 * gamma_sum
        acc[1 + num_layers + layer] += beta_sum

    def side_source(k):
        @pl.when(k == 0)
        def _():
            def body(places):
                blocks = [(cost[j, h] * re, cost[j, h] * im)
                          for (h, j), (re, im) in zip(places, load(kept.at[before_at], places))]
                store(side, places, mix_all(blocks, tan0))

            for_columns((0, 1), body)

        @pl.when(k == 2)
        def _():
            low_sums(before_at)
            high_sums(before_at)
            for_columns((0, 1), lambda places: store(side, places, mix_all(load(qbuf, places), tan0)))

    def side_arrival(n):
        per_half(lambda h: receive(2 + n, h, 0, tan0, side))

        def body(places):
            for h in range(2):
                mine = places[h::2]
                store(kept.at[side_at + n], mine, scaled(mix_all(load(side, mine), tan0), angle[0, 1]))

        for_columns((0, 1), body)

    def side_sums():
        full_sums(0)

        def body(j, _):
            for h in range(2):
                for c in range(2):
                    kept[sums_at, h, j, c] = qbuf[h, j, c] + kept[side_at + 1, h, j, c]
            return 0

        lax.fori_loop(0, nb, body, 0)

    def last_sums(h):
        def body(x, sums):
            gamma1, beta1, gamma0, beta0 = sums
            places = column(x, (h,))
            blocks = scaled(mix_all(load(work, places), angle[1, 0]), angle[1, 1])
            for (h_, j), left, right, q in zip(places, blocks, load(kept.at[before_at + 1], places), load(qbuf, places)):
                gamma1 += cost_b[j, h_] * im_dot(left, right)
                beta1 += im_dot(left, q)
            blocks = turn(blocks, 1, places)
            for left, right, q in zip(blocks, load(kept.at[side_at], places), load(kept.at[sums_at], places)):
                gamma0 += im_dot(left, right)
                beta0 += im_dot(left, q)
            return gamma1, beta1, gamma0, beta0

        gamma1, beta1, gamma0, beta0 = lax.fori_loop(0, nx, body, (zero,) * 4)
        acc[1] += 2.0 * gamma0
        acc[2] += 2.0 * gamma1
        acc[1 + num_layers] += beta0
        acc[2 + num_layers] += beta1

    def two_gaps(k, _):
        step = 2 * k
        _, done, _, following = plan(step)
        tan_half, tan_next = angle[done, 0], angle[following, 0]

        def half(h):
            receive(0, h, done, tan_half, work)
            for_columns((h,), middle(step))

            @pl.when(k > 0)
            def _():
                wait_sends(1, h)

            send_half(1, h, following, tan_next, work)

        per_half(half)

        side_source(k)

        @pl.when(k < pairs - 1)
        def _():
            make_table(step + 2, cost)

        @pl.when(k >= pairs)
        def _():
            collect(done, cost_b)
            prepare(following)

        @pl.when((k < 3) | (k == 4))
        def _():
            piece = k - k // 4
            send_half(2 + piece // 2, piece % 2, 0, tan0, side)

        step = 2 * k + 1
        _, done, _, following = plan(step)
        tan_half = angle[done, 0]
        per_half(lambda h: receive(1, h, done, tan_half, work))

        @pl.when(k % pairs < pairs - 1)
        def _():
            for_columns((0, 1), middle(step))

        @pl.when(k == pairs - 1)
        def _():
            for_columns((0, 1), turn_point)

        into = following - (k // (pairs - 1)) * (1 - k // pairs) * (following - last)
        tan_next = angle[into, 0]

        def half_joint(h):
            wait_sends(0, h)
            send_half(0, h, into, tan_next, work)

        per_half(half_joint)

        @pl.when(k < pairs - 1)
        def _():
            make_table(step + 2, cost_b)

        @pl.when(k == pairs - 1)
        def _():
            def write(j, _):
                for h in range(2):
                    for c in range(2):
                        final[c, j, h] = root * kept[last, h, j, c]
                return 0

            lax.fori_loop(0, nb, write, 0)

        @pl.when(k >= pairs)
        def _():
            collect(done, cost)

        @pl.when((k == 4) | (k == 5))
        def _():
            side_arrival(k - 4)

        @pl.when(k == 2 * pairs - 2)
        def _():
            side_sums()

        @pl.when(k >= pairs - 1)
        def _():
            prepare(2 * num_layers - 3 - 2 * k)

        return 0

    lax.fori_loop(0, 2 * pairs - 1, two_gaps, 0)

    def last_half(h):
        receive(0, h, 1, angle[1, 0], work)
        last_sums(h)

    per_half(last_half)

    lane = lax.broadcasted_iota(jnp.int32, (1, LANES), 1)
    row = jnp.zeros((1, LANES), jnp.float32)
    for place in range(acc.shape[0]):
        value = jnp.sum(jnp.sum(acc[place], axis=0, keepdims=True), axis=1, keepdims=True)
        row = jnp.where(lane == place, value, row)
    part[...] = row
    for dy, dx, dc in offsets:
        y, x, dest = peer(dy, dx, dc)
        pltpu.make_async_remote_copy(
            src_ref=part, dst_ref=gath.at[me], send_sem=sum_send, recv_sem=sum_recv,
            device_id={"qy": y, "qx": x}, device_id_type=MESH_ID).start()
    gath[me] = row
    for par in range(4):
        for h in range(2):
            wait_sends(par, h)
    view = cost_b.at[pl.ds(0, nb - 1)]
    pltpu.make_async_copy(view, view, cost_send).wait()
    view = gath.at[pl.ds(0, nb - 1)]
    pltpu.make_async_copy(view, view, sum_recv).wait()
    total = gath[0]
    for j in range(1, nb):
        total += gath[j]
    totals[...] = total
    view = gath.at[pl.ds(0, nb - 1)]
    pltpu.make_async_copy(view, view, sum_send).wait()


def solution(mesh):
    ny, nx = mesh.shape["qy"], mesh.shape["qx"]
    nb = ny * nx

    def local_run(cost_local, gamma_angles, beta_angles):
        chunk = cost_local.shape[0]
        num_layers = gamma_angles.shape[0]
        assert chunk == nb * 16 * LANES and num_layers % 2 == 0 and num_layers >= 8
        num_qubits = int(math.log2(chunk * nb))
        amp = (chunk * nb) ** -0.5
        vmem, smem, dma = pltpu.VMEM, pltpu.SMEM, pltpu.SemaphoreType.DMA
        f32 = jnp.float32
        state = (2, nb, 2, 8, LANES)
        final, totals = pl.pallas_call(
            functools.partial(kernel, ny, nx, num_layers, num_qubits, amp),
            out_shape=(jax.ShapeDtypeStruct((2, nb, 2, 8, LANES), f32), jax.ShapeDtypeStruct((1, LANES), f32)),
            in_specs=[pl.BlockSpec(memory_space=pltpu.MemorySpace.HBM)] * 3,
            out_specs=(pl.BlockSpec(memory_space=vmem), pl.BlockSpec(memory_space=vmem)),
            scratch_shapes=[
                vmem((nb, 2, 8, LANES), f32),
                smem((num_layers,), f32),
                smem((num_layers,), f32),
                vmem((nb, 2, 8, LANES), f32),
                vmem((num_layers, 2, 2, nb, 8, LANES), f32),
                vmem((2 * num_layers + 5,) + state, f32),
                vmem((4,) + state, f32),
                vmem((4,) + state, f32),
                vmem(state, f32),
                vmem(state, f32),
                vmem(state, f32),
                vmem((num_layers, 2, 8, LANES), f32),
                vmem((num_layers, 2 * LANES, 2 * LANES), f32),
                vmem((2 * LANES, 2 * LANES), f32),
                vmem((1 + 2 * num_layers, 8, LANES), f32),
                vmem((1, LANES), f32),
                vmem((nb, 1, LANES), f32),
                dma((3,)),
                dma((4, 2)),
                dma((4, 2, 1 + ny // 2)),
                dma,
                dma,
                dma,
                dma,
            ],
            compiler_params=pltpu.CompilerParams(
                collective_id=0, has_side_effects=True, vmem_limit_bytes=48 * 1024 * 1024),
            name="qaoa",
        )(cost_local.reshape(nb, 2, 8, LANES), gamma_angles, beta_angles)
        energy = totals[0, :1]
        grad = totals[0, 1:1 + 2 * num_layers]
        return energy, grad, final.reshape(2, chunk)

    state_spec = P(("inst", "qy", "qx"))
    return jax.shard_map(
        local_run, mesh=mesh, in_specs=(state_spec, P(), P()),
        out_specs=(P("inst"), P("inst"), P(None, ("inst", "qy", "qx"))), check_vma=False)
```

```python
import functools
import math

import jax
import jax.numpy as jnp
from jax import lax
from jax.experimental import pallas as pl
from jax.experimental.pallas import tpu as pltpu
from jax.sharding import PartitionSpec as P

LANES = 128
MESH_ID = pl.DeviceIdType.MESH


def mix_pair(blocks, tan_half, stride):
    out = list(blocks)
    for low in range(len(blocks)):
        if low & stride:
            continue
        high = low | stride
        (re0, im0), (re1, im1) = blocks[low], blocks[high]
        out[low] = (re0 + tan_half * im1, im0 - tan_half * re1)
        out[high] = (re1 + tan_half * im0, im1 - tan_half * re0)
    return out


def mix_all(blocks, tan_half):
    stride = 1
    while stride < len(blocks):
        blocks = mix_pair(blocks, tan_half, stride)
        stride *= 2
    return blocks


def partner_sums(blocks):
    out = []
    for place in range(len(blocks)):
        stride, re, im = 1, None, None
        while stride < len(blocks):
            pre, pim = blocks[place ^ stride]
            re, im = (pre, pim) if re is None else (re + pre, im + pim)
            stride *= 2
        out.append((re, im))
    return out


def sublane_partner(x, ids, dist):
    return jnp.take_along_axis(x, ids ^ dist, axis=1, mode="promise_in_bounds")


def swapped(x, stride):
    pairs = x.reshape((x.shape[0] // (2 * stride), 2, stride) + x.shape[1:])
    return jnp.concatenate([pairs[:, 1:], pairs[:, :1]], axis=1).reshape(x.shape)


def mix_leading(re, im, tan_half, size):
    stride = 1
    while stride < size:
        re, im = re + tan_half * swapped(im, stride), im - tan_half * swapped(re, stride)
        stride *= 2
    return re, im


def matmul(x, w):
    return jnp.dot(x, w, precision=lax.Precision.HIGHEST, preferred_element_type=jnp.float32)


def kernel(ny, nx, num_layers, num_qubits, amp, cost_in, gamma_in, beta_in, final, totals,
           cost, gamma, beta, cost_b, tabs, kept, recv, send, work, side, qbuf, angle, lane_mix, lane_sum, acc, part, gath,
           load_sem, send_sem, recv_sem, cost_send, cost_recv, sum_send, sum_recv):
    nb = ny * nx
    chips = nx // 2
    last = num_layers - 1
    my_y = lax.axis_index("qy")
    my_x = lax.axis_index("qx")
    my_chip, my_core = my_x // 2, my_x % 2
    me = my_y * nx + my_x

    def peer(dy, dx, dc):
        y = (my_y + dy) % ny
        x = ((my_chip + dx) % chips) * 2 + (my_core + dc) % 2
        return y, x, y * nx + x

    dy_order = sorted(range(ny), key=lambda d: -min(d, ny - d))
    dx_order = sorted(range(chips), key=lambda d: -min(d, chips - d))
    offsets = [(dy, dx, dc) for dy in dy_order for dx in dx_order for dc in (1, 0) if dy or dx or dc]

    inputs = [pltpu.make_async_copy(src, dst, load_sem.at[n])
              for n, (src, dst) in enumerate([(gamma_in, gamma), (beta_in, beta), (cost_in, cost)])]
    for copy in inputs:
        copy.start()
    barrier = pltpu.get_barrier_semaphore()
    for dy, dx, dc in offsets:
        y, x, _ = peer(dy, dx, dc)
        pl.semaphore_signal(barrier, inc=1, device_id={"qy": y, "qx": x}, device_id_type=MESH_ID)

    def make_angle(layer):
        half = jnp.full((8, LANES), 0.5 * beta[layer], jnp.float32)
        cos_half, sin_half = jnp.cos(half), jnp.sin(half)
        scale, power, left = None, cos_half, num_qubits - 7
        while left:
            if left % 2:
                scale = power if scale is None else scale * power
            power, left = power * power, left // 2
        angle[layer, 0] = sin_half / cos_half
        angle[layer, 1] = scale
        return cos_half[:1], sin_half[:1]

    def make_lanes(layers):
        flips = lax.broadcasted_iota(jnp.int32, (LANES, LANES), 0) ^ lax.broadcasted_iota(jnp.int32, (LANES, LANES), 1)
        weight = sum((flips >> bit) & 1 for bit in range(7))
        for layer in layers:
            c, s = make_angle(layer)
            coefs = []
            for k in range(8):
                coef = None
                for factor in [c] * (7 - k) + [s] * k:
                    coef = factor if coef is None else coef * factor
                coefs.append(coef if (k // 2) % 2 == 0 else -coef)
            even, odd = jnp.zeros((LANES, LANES), jnp.float32), jnp.zeros((LANES, LANES), jnp.float32)
            for k in range(8):
                if k % 2 == 0:
                    even = jnp.where(weight == k, coefs[k], even)
                else:
                    odd = jnp.where(weight == k, coefs[k], odd)
            lane_mix[layer, :LANES, :LANES] = even
            lane_mix[layer, LANES:, LANES:] = even
            lane_mix[layer, LANES:, :LANES] = odd
            lane_mix[layer, :LANES, LANES:] = -odd
        if 0 not in layers:
            ones = jnp.where(weight == 1, 1.0, 0.0).astype(jnp.float32)
            lane_sum[:LANES, :LANES] = ones
            lane_sum[LANES:, LANES:] = ones
            lane_sum[:LANES, LANES:] = jnp.zeros_like(ones)
            lane_sum[LANES:, :LANES] = jnp.zeros_like(ones)

    def make_table(layer, source):
        g = gamma[layer]

        def body(j, _):
            for h in range(2):
                theta = g * source[j, h]
                tabs[layer, 0, h, j] = jnp.cos(theta)
                tabs[layer, 1, h, j] = jnp.sin(theta)
            return 0

        lax.fori_loop(0, nb, body, 0)

    def load(ref, places):
        return [(ref[h, j, 0], ref[h, j, 1]) for h, j in places]

    def store(ref, places, blocks):
        for (h, j), (re, im) in zip(places, blocks):
            ref[h, j, 0] = re
            ref[h, j, 1] = im

    def turn(blocks, layer, places):
        out = []
        for (re, im), (h, j) in zip(blocks, places):
            c, s = tabs[layer, 0, h, j], tabs[layer, 1, h, j]
            out.append((c * re + s * im, c * im - s * re))
        return out

    def scaled(blocks, scale):
        return [(scale * re, scale * im) for re, im in blocks]

    def column(x, halves):
        return [(h, y * nx + x) for y in range(ny) for h in halves]

    def for_columns(halves, body):
        lax.fori_loop(0, nx, lambda x, _: (body(column(x, halves)), 0)[1], 0, unroll=2)

    def load_row(ref, h, y):
        return ref[h, pl.ds(y * nx, nx), 0], ref[h, pl.ds(y * nx, nx), 1]

    def store_row(ref, h, y, row):
        for c in range(2):
            ref[h, pl.ds(y * nx, nx), c] = row[c]

    waves = [dy_order[:1]] + [dy_order[i:i + 2] for i in range(1, ny, 2)]

    def mix_lanes(rows, layer):
        x = jnp.concatenate([jnp.concatenate([re.reshape(nx * 8, LANES), im.reshape(nx * 8, LANES)], axis=1)
                             for re, im in rows], axis=0)
        x = matmul(x, lane_mix[layer])
        parts = [x[n * nx * 8:(n + 1) * nx * 8] for n in range(len(rows))]
        return [(p[:, :LANES].reshape(nx, 8, LANES), p[:, LANES:].reshape(nx, 8, LANES)) for p in parts]

    def lanes_late(even, h):
        return [] if h else waves[:1] if even else waves

    def send_half(par, h, layer, tan_half, source, late):
        rows = {dy: mix_leading(*load_row(source, h, (my_y + dy) % ny), tan_half, nx) for dy in dy_order}

        def leave(wave, dy):
            y = (my_y + dy) % ny
            store_row(send.at[par], h, y, rows[dy])
            for dx in dx_order:
                for dc in (1, 0):
                    if dy or dx or dc:
                        _, x, dest = peer(dy, dx, dc)
                        pltpu.make_async_remote_copy(
                            src_ref=send.at[par, h, dest], dst_ref=recv.at[par, h, me],
                            send_sem=send_sem.at[par, h], recv_sem=recv_sem.at[par, h, wave],
                            device_id={"qy": y, "qx": x}, device_id_type=MESH_ID).start()

        for group in (waves[:1], waves[1:]):
            early = [dy for wave in group if wave not in late for dy in wave]
            if early:
                rows.update(zip(early, mix_lanes([rows[dy] for dy in early], layer)))
            for wave in group:
                for dy in wave:
                    leave(waves.index(wave), dy)
        for c in range(2):
            recv[par, h, me, c] = send[par, h, me, c]

    def wait_sends(par, h):
        view = send.at[par, h, pl.ds(0, nb - 1)]
        pltpu.make_async_copy(view, view, send_sem.at[par, h]).wait()

    sub = lax.broadcasted_iota(jnp.int32, (nx, 8, LANES), 1)

    def receive(par, h, layer, tan_half, target, late):
        late_rows = []
        for n, wave in enumerate(waves):
            count = len(wave) * nx - (1 if 0 in wave else 0)
            view = recv.at[par, h, pl.ds(0, count)]
            pltpu.make_async_copy(view, view, recv_sem.at[par, h, n]).wait()
            for dy in wave:
                y = (my_y + ny - dy) % ny
                re, im = load_row(recv.at[par], h, y)
                for dist in (1, 2, 4):
                    re, im = (re + tan_half * sublane_partner(im, sub, dist),
                              im - tan_half * sublane_partner(re, sub, dist))
                re, im = mix_leading(re, im, tan_half, nx)
                if wave in late:
                    late_rows.append((y, (re, im)))
                else:
                    store_row(target, h, y, (re, im))
        if late_rows:
            for (y, _), row in zip(late_rows, mix_lanes([row for _, row in late_rows], layer)):
                store_row(target, h, y, row)

    def per_half(body):
        lax.fori_loop(0, 2, lambda h, _: (body(h), 0)[1], 0)

    for copy in inputs:
        copy.wait()
    make_lanes([0])
    make_table(0, cost)
    tan0 = angle[0, 0]

    def first(places):
        flat = jnp.full((8, LANES), amp, jnp.float32)
        blocks = turn([(flat, jnp.zeros_like(flat)) for _ in places], 0, places)
        store(kept.at[num_layers], places, blocks)
        store(work, places, mix_all(blocks, tan0))

    for_columns((0, 1), first)
    for place in range(acc.shape[0]):
        acc[place] = jnp.zeros((8, LANES), jnp.float32)

    pl.semaphore_wait(barrier, nb - 1)

    for dy, dx, dc in offsets:
        y, x, dest = peer(dy, dx, dc)
        pltpu.make_async_remote_copy(
            src_ref=cost.at[dest], dst_ref=cost_b.at[me], send_sem=cost_send, recv_sem=cost_recv,
            device_id={"qy": y, "qx": x}, device_id_type=MESH_ID).start()
    for h in range(2):
        cost_b[me, h] = cost[me, h]
    for h in range(2):
        send_half(0, h, 0, tan0, work, lanes_late(True, h))
    make_lanes(range(1, num_layers))
    view = cost_b.at[pl.ds(0, nb - 1)]
    pltpu.make_async_copy(view, view, cost_recv).wait()
    make_table(1, cost_b)

    before_at, lam_pre, lam, side_at, sums_at = (num_layers, 2 * num_layers, 2 * num_layers + 1,
                                                 2 * num_layers + 2, 2 * num_layers + 4)
    root = jnp.float32(1.0 / amp)
    zero = jnp.zeros((8, LANES), jnp.float32)
    pairs = num_layers // 2

    def plan(step):
        back = step // num_layers
        done = step + back * (2 * num_layers - 1 - 2 * step)
        return back, done, done + 1 - back, (done + 1 - 2 * back + num_layers) % num_layers

    def middle(step):
        back, done, turned, following = plan(step)
        tan_half, scale, tan_next = angle[done, 0], angle[done, 1], angle[following, 0]
        first_at = done + back * (lam_pre - done)
        second_at = before_at + turned + back * (lam - before_at - turned)

        def body(places):
            blocks = scaled(mix_all(load(work, places), tan_half), scale)
            store(kept.at[first_at], places, blocks)
            blocks = turn(blocks, turned, places)
            store(kept.at[second_at], places, blocks)
            store(work, places, mix_all(blocks, tan_next))

        return body

    def turn_point(places):
        tan_half, scale = angle[last, 0], angle[last, 1]
        blocks = scaled(mix_all(load(work, places), tan_half), scale)
        store(kept.at[last], places, blocks)
        conj = []
        energy = acc[0]
        for (h, j), (re, im) in zip(places, blocks):
            c = cost[j, h]
            conj.append((c * re, -(c * im)))
            energy += c * (re * re + im * im)
        acc[0] = energy
        store(kept.at[lam], places, conj)
        store(work, places, mix_all(conj, tan_half))

    def im_dot(conj, right):
        return conj[0] * right[1] + conj[1] * right[0]

    def sums_of(re, im, size):
        total_re, total_im, stride = swapped(re, 1), swapped(im, 1), 2
        while stride < size:
            total_re, total_im, stride = total_re + swapped(re, stride), total_im + swapped(im, stride), 2 * stride
        return total_re, total_im

    def high_sums(at):
        def body(x, _):
            for h in range(2):
                places = column(x, (h,))
                sums = partner_sums(load(kept.at[at], places))
                store(qbuf, places, [(a + c, b + d) for (a, b), (c, d) in zip(sums, load(qbuf, places))])
            return 0

        lax.fori_loop(0, nx, body, 0)

    def low_sums(at):
        def low(n, _):
            h, y = n // ny, n % ny
            re, im = load_row(kept.at[at], h, y)
            store_row(qbuf, h, y, sums_of(re, im, nx))
            return 0

        lax.fori_loop(0, 2 * ny, low, 0)

    def full_sums(at):
        def inner(y, _):
            rows = [load_row(kept.at[at], h, y) for h in range(2)]
            x = jnp.concatenate([jnp.concatenate([re.reshape(nx * 8, LANES), im.reshape(nx * 8, LANES)], axis=1)
                                 for re, im in rows], axis=0)
            lanes = matmul(x, lane_sum[...])
            for h in range(2):
                sre, sim = sums_of(*rows[h], nx)
                (re, im), (ore, oim) = rows[h], rows[1 - h]
                for dist in (1, 2, 4):
                    sre += sublane_partner(re, sub, dist)
                    sim += sublane_partner(im, sub, dist)
                mine = lanes[h * nx * 8:(h + 1) * nx * 8]
                store_row(qbuf, h, y, (sre + ore + mine[:, :LANES].reshape(nx, 8, LANES),
                                       sim + oim + mine[:, LANES:].reshape(nx, 8, LANES)))
            return 0

        lax.fori_loop(0, ny, inner, 0)
        high_sums(at)

    def prepare(layer):
        low_sums(layer)
        high_sums(layer)

        def body(j, total):
            for h in range(2):
                total += im_dot((kept[lam, h, j, 0], kept[lam, h, j, 1]), (qbuf[h, j, 0], qbuf[h, j, 1]))
            return total

        acc[1 + num_layers + layer] = lax.fori_loop(0, nb, body, zero)
        full_sums(before_at + layer)

    def collect(layer, source):
        at = before_at + layer

        def body(j, sums):
            gamma_sum, beta_sum = sums
            for h in range(2):
                left = (kept[lam_pre, h, j, 0], kept[lam_pre, h, j, 1])
                gamma_sum += source[j, h] * im_dot(left, (kept[at, h, j, 0], kept[at, h, j, 1]))
                beta_sum += im_dot(left, (qbuf[h, j, 0], qbuf[h, j, 1]))
            return gamma_sum, beta_sum

        gamma_sum, beta_sum = lax.fori_loop(0, nb, body, (zero, zero))
        acc[1 + layer] = 2.0 * gamma_sum
        acc[1 + num_layers + layer] += beta_sum

    def side_source(k):
        @pl.when(k == 0)
        def _():
            def body(places):
                blocks = [(cost[j, h] * re, cost[j, h] * im)
                          for (h, j), (re, im) in zip(places, load(kept.at[before_at], places))]
                store(side, places, mix_all(blocks, tan0))

            for_columns((0, 1), body)

        @pl.when(k == 2)
        def _():
            low_sums(before_at)
            high_sums(before_at)
            for_columns((0, 1), lambda places: store(side, places, mix_all(load(qbuf, places), tan0)))

    def side_arrival(n):
        per_half(lambda h: receive(2 + n, h, 0, tan0, side, []))

        def body(places):
            for h in range(2):
                mine = places[h::2]
                store(kept.at[side_at + n], mine, scaled(mix_all(load(side, mine), tan0), angle[0, 1]))

        for_columns((0, 1), body)

    def side_sums():
        full_sums(0)

        def body(j, _):
            for h in range(2):
                for c in range(2):
                    kept[sums_at, h, j, c] = qbuf[h, j, c] + kept[side_at + 1, h, j, c]
            return 0

        lax.fori_loop(0, nb, body, 0)

    def last_sums(h):
        def body(x, sums):
            gamma1, beta1, gamma0, beta0 = sums
            places = column(x, (h,))
            blocks = scaled(mix_all(load(work, places), angle[1, 0]), angle[1, 1])
            for (h_, j), left, right, q in zip(places, blocks, load(kept.at[before_at + 1], places), load(qbuf, places)):
                gamma1 += cost_b[j, h_] * im_dot(left, right)
                beta1 += im_dot(left, q)
            blocks = turn(blocks, 1, places)
            for left, right, q in zip(blocks, load(kept.at[side_at], places), load(kept.at[sums_at], places)):
                gamma0 += im_dot(left, right)
                beta0 += im_dot(left, q)
            return gamma1, beta1, gamma0, beta0

        gamma1, beta1, gamma0, beta0 = lax.fori_loop(0, nx, body, (zero,) * 4)
        acc[1] += 2.0 * gamma0
        acc[2] += 2.0 * gamma1
        acc[1 + num_layers] += beta0
        acc[2 + num_layers] += beta1

    def two_gaps(k, _):
        step = 2 * k
        _, done, _, following = plan(step)
        tan_half, tan_next = angle[done, 0], angle[following, 0]

        def half(h):
            receive(0, h, done, tan_half, work, lanes_late(True, h))
            for_columns((h,), middle(step))

            @pl.when(k > 0)
            def _():
                wait_sends(1, h)

            send_half(1, h, following, tan_next, work, lanes_late(False, h))

        for h in range(2):
            half(h)

        side_source(k)

        @pl.when(k < pairs - 1)
        def _():
            make_table(step + 2, cost)

        @pl.when(k >= pairs)
        def _():
            collect(done, cost_b)
            prepare(following)

        @pl.when((k < 3) | (k == 4))
        def _():
            piece = k - k // 4
            send_half(2 + piece // 2, piece % 2, 0, tan0, side, [])

        step = 2 * k + 1
        _, done, _, following = plan(step)
        tan_half = angle[done, 0]
        for h in range(2):
            receive(1, h, done, tan_half, work, lanes_late(False, h))

        @pl.when(k % pairs < pairs - 1)
        def _():
            for_columns((0, 1), middle(step))

        @pl.when(k == pairs - 1)
        def _():
            for_columns((0, 1), turn_point)

        into = following - (k // (pairs - 1)) * (1 - k // pairs) * (following - last)
        tan_next = angle[into, 0]

        def half_joint(h):
            wait_sends(0, h)
            send_half(0, h, into, tan_next, work, lanes_late(True, h))

        for h in range(2):
            half_joint(h)

        @pl.when(k < pairs - 1)
        def _():
            make_table(step + 2, cost_b)

        @pl.when(k == pairs - 1)
        def _():
            def write(j, _):
                for h in range(2):
                    for c in range(2):
                        final[c, j, h] = root * kept[last, h, j, c]
                return 0

            lax.fori_loop(0, nb, write, 0)

        @pl.when(k >= pairs)
        def _():
            collect(done, cost)

        @pl.when((k == 4) | (k == 5))
        def _():
            side_arrival(k - 4)

        @pl.when(k == 2 * pairs - 2)
        def _():
            side_sums()

        @pl.when(k >= pairs - 1)
        def _():
            prepare(2 * num_layers - 3 - 2 * k)

        return 0

    lax.fori_loop(0, 2 * pairs - 1, two_gaps, 0)

    def last_half(h):
        receive(0, h, 1, angle[1, 0], work, lanes_late(True, h))
        last_sums(h)

    for h in range(2):
        last_half(h)

    lane = lax.broadcasted_iota(jnp.int32, (1, LANES), 1)
    row = jnp.zeros((1, LANES), jnp.float32)
    for place in range(acc.shape[0]):
        value = jnp.sum(jnp.sum(acc[place], axis=0, keepdims=True), axis=1, keepdims=True)
        row = jnp.where(lane == place, value, row)
    part[...] = row
    for dy, dx, dc in offsets:
        y, x, dest = peer(dy, dx, dc)
        pltpu.make_async_remote_copy(
            src_ref=part, dst_ref=gath.at[me], send_sem=sum_send, recv_sem=sum_recv,
            device_id={"qy": y, "qx": x}, device_id_type=MESH_ID).start()
    gath[me] = row
    for par in range(4):
        for h in range(2):
            wait_sends(par, h)
    view = cost_b.at[pl.ds(0, nb - 1)]
    pltpu.make_async_copy(view, view, cost_send).wait()
    view = gath.at[pl.ds(0, nb - 1)]
    pltpu.make_async_copy(view, view, sum_recv).wait()
    total = gath[0]
    for j in range(1, nb):
        total += gath[j]
    totals[...] = total
    view = gath.at[pl.ds(0, nb - 1)]
    pltpu.make_async_copy(view, view, sum_send).wait()


def solution(mesh):
    ny, nx = mesh.shape["qy"], mesh.shape["qx"]
    nb = ny * nx

    def local_run(cost_local, gamma_angles, beta_angles):
        chunk = cost_local.shape[0]
        num_layers = gamma_angles.shape[0]
        assert chunk == nb * 16 * LANES and num_layers % 2 == 0 and num_layers >= 8
        num_qubits = int(math.log2(chunk * nb))
        amp = (chunk * nb) ** -0.5
        vmem, smem, dma = pltpu.VMEM, pltpu.SMEM, pltpu.SemaphoreType.DMA
        f32 = jnp.float32
        state = (2, nb, 2, 8, LANES)
        final, totals = pl.pallas_call(
            functools.partial(kernel, ny, nx, num_layers, num_qubits, amp),
            out_shape=(jax.ShapeDtypeStruct((2, nb, 2, 8, LANES), f32), jax.ShapeDtypeStruct((1, LANES), f32)),
            in_specs=[pl.BlockSpec(memory_space=pltpu.MemorySpace.HBM)] * 3,
            out_specs=(pl.BlockSpec(memory_space=vmem), pl.BlockSpec(memory_space=vmem)),
            scratch_shapes=[
                vmem((nb, 2, 8, LANES), f32),
                smem((num_layers,), f32),
                smem((num_layers,), f32),
                vmem((nb, 2, 8, LANES), f32),
                vmem((num_layers, 2, 2, nb, 8, LANES), f32),
                vmem((2 * num_layers + 5,) + state, f32),
                vmem((4,) + state, f32),
                vmem((4,) + state, f32),
                vmem(state, f32),
                vmem(state, f32),
                vmem(state, f32),
                vmem((num_layers, 2, 8, LANES), f32),
                vmem((num_layers, 2 * LANES, 2 * LANES), f32),
                vmem((2 * LANES, 2 * LANES), f32),
                vmem((1 + 2 * num_layers, 8, LANES), f32),
                vmem((1, LANES), f32),
                vmem((nb, 1, LANES), f32),
                dma((3,)),
                dma((4, 2)),
                dma((4, 2, 1 + ny // 2)),
                dma,
                dma,
                dma,
                dma,
            ],
            compiler_params=pltpu.CompilerParams(
                collective_id=0, has_side_effects=True, vmem_limit_bytes=48 * 1024 * 1024),
            name="qaoa",
        )(cost_local.reshape(nb, 2, 8, LANES), gamma_angles, beta_angles)
        energy = totals[0, :1]
        grad = totals[0, 1:1 + 2 * num_layers]
        return energy, grad, final.reshape(2, chunk)

    state_spec = P(("inst", "qy", "qx"))
    return jax.shard_map(
        local_run, mesh=mesh, in_specs=(state_spec, P(), P()),
        out_specs=(P("inst"), P("inst"), P(None, ("inst", "qy", "qx"))), check_vma=False)
```

```python
import functools
import math

import jax
import jax.numpy as jnp
from jax import lax
from jax.experimental import pallas as pl
from jax.experimental.pallas import tpu as pltpu
from jax.sharding import PartitionSpec as P

LANES = 128
MESH_ID = pl.DeviceIdType.MESH


def mix_pair(blocks, tan_half, stride):
    out = list(blocks)
    for low in range(len(blocks)):
        if low & stride:
            continue
        high = low | stride
        (re0, im0), (re1, im1) = blocks[low], blocks[high]
        out[low] = (re0 + tan_half * im1, im0 - tan_half * re1)
        out[high] = (re1 + tan_half * im0, im1 - tan_half * re0)
    return out


def mix_all(blocks, tan_half):
    stride = 1
    while stride < len(blocks):
        blocks = mix_pair(blocks, tan_half, stride)
        stride *= 2
    return blocks


def partner_sums(blocks):
    out = []
    for place in range(len(blocks)):
        stride, re, im = 1, None, None
        while stride < len(blocks):
            pre, pim = blocks[place ^ stride]
            re, im = (pre, pim) if re is None else (re + pre, im + pim)
            stride *= 2
        out.append((re, im))
    return out


def sublane_partner(x, ids, dist):
    return jnp.take_along_axis(x, ids ^ dist, axis=1, mode="promise_in_bounds")


def swapped(x, stride):
    pairs = x.reshape((x.shape[0] // (2 * stride), 2, stride) + x.shape[1:])
    return jnp.concatenate([pairs[:, 1:], pairs[:, :1]], axis=1).reshape(x.shape)


def mix_leading(re, im, tan_half, size):
    stride = 1
    while stride < size:
        re, im = re + tan_half * swapped(im, stride), im - tan_half * swapped(re, stride)
        stride *= 2
    return re, im


def matmul(x, w):
    return jnp.dot(x, w, precision=lax.Precision.HIGHEST, preferred_element_type=jnp.float32)


def kernel(ny, nx, num_layers, num_qubits, amp, cost_in, gamma_in, beta_in, final, totals,
           cost, gamma, beta, cost_b, tabs, kept, recv, send, work, side, qbuf, angle, lane_mix, lane_sum, acc, part, gath,
           load_sem, send_sem, recv_sem, cost_send, cost_recv, sum_send, sum_recv):
    nb = ny * nx
    chips = nx // 2
    last = num_layers - 1
    my_y = lax.axis_index("qy")
    my_x = lax.axis_index("qx")
    my_chip, my_core = my_x // 2, my_x % 2
    me = my_y * nx + my_x

    def peer(dy, dx, dc):
        y = (my_y + dy) % ny
        x = ((my_chip + dx) % chips) * 2 + (my_core + dc) % 2
        return y, x, y * nx + x

    dy_order = sorted(range(ny), key=lambda d: -min(d, ny - d))
    dx_order = sorted(range(chips), key=lambda d: -min(d, chips - d))
    offsets = [(dy, dx, dc) for dy in dy_order for dx in dx_order for dc in (1, 0) if dy or dx or dc]

    inputs = [pltpu.make_async_copy(src, dst, load_sem.at[n])
              for n, (src, dst) in enumerate([(gamma_in, gamma), (beta_in, beta), (cost_in, cost)])]
    for copy in inputs:
        copy.start()
    barrier = pltpu.get_barrier_semaphore()
    for dy, dx, dc in offsets:
        y, x, _ = peer(dy, dx, dc)
        pl.semaphore_signal(barrier, inc=1, device_id={"qy": y, "qx": x}, device_id_type=MESH_ID)

    def make_angle(layer):
        half = jnp.full((8, LANES), 0.5 * beta[layer], jnp.float32)
        cos_half, sin_half = jnp.cos(half), jnp.sin(half)
        scale, power, left = None, cos_half, num_qubits - 7
        while left:
            if left % 2:
                scale = power if scale is None else scale * power
            power, left = power * power, left // 2
        angle[layer] = sin_half / cos_half
        return cos_half[:1], sin_half[:1], scale[:1]

    def make_lanes(layers):
        flips = lax.broadcasted_iota(jnp.int32, (LANES, LANES), 0) ^ lax.broadcasted_iota(jnp.int32, (LANES, LANES), 1)
        weight = sum((flips >> bit) & 1 for bit in range(7))
        for layer in layers:
            c, s, scale = make_angle(layer)
            coefs = []
            for k in range(8):
                coef = scale
                for factor in [c] * (7 - k) + [s] * k:
                    coef = coef * factor
                coefs.append(coef if (k // 2) % 2 == 0 else -coef)
            even, odd = jnp.zeros((LANES, LANES), jnp.float32), jnp.zeros((LANES, LANES), jnp.float32)
            for k in range(8):
                if k % 2 == 0:
                    even = jnp.where(weight == k, coefs[k], even)
                else:
                    odd = jnp.where(weight == k, coefs[k], odd)
            lane_mix[layer, :LANES, :LANES] = even
            lane_mix[layer, LANES:, LANES:] = even
            lane_mix[layer, LANES:, :LANES] = odd
            lane_mix[layer, :LANES, LANES:] = -odd
        if 0 not in layers:
            ones = jnp.where(weight == 1, 1.0, 0.0).astype(jnp.float32)
            lane_sum[:LANES, :LANES] = ones
            lane_sum[LANES:, LANES:] = ones
            lane_sum[:LANES, LANES:] = jnp.zeros_like(ones)
            lane_sum[LANES:, :LANES] = jnp.zeros_like(ones)

    def make_table(layer, source):
        g = gamma[layer]

        def body(j, _):
            for h in range(2):
                theta = g * source[j, h]
                tabs[layer, 0, h, j] = jnp.cos(theta)
                tabs[layer, 1, h, j] = jnp.sin(theta)
            return 0

        lax.fori_loop(0, nb, body, 0)

    def load(ref, places):
        return [(ref[h, j, 0], ref[h, j, 1]) for h, j in places]

    def store(ref, places, blocks):
        for (h, j), (re, im) in zip(places, blocks):
            ref[h, j, 0] = re
            ref[h, j, 1] = im

    def turn(blocks, layer, places):
        out = []
        for (re, im), (h, j) in zip(blocks, places):
            c, s = tabs[layer, 0, h, j], tabs[layer, 1, h, j]
            out.append((c * re + s * im, c * im - s * re))
        return out

    def column(x, halves):
        return [(h, y * nx + x) for y in range(ny) for h in halves]

    def for_columns(halves, body):
        lax.fori_loop(0, nx, lambda x, _: (body(column(x, halves)), 0)[1], 0, unroll=2)

    def load_row(ref, h, y):
        return ref[h, pl.ds(y * nx, nx), 0], ref[h, pl.ds(y * nx, nx), 1]

    def store_row(ref, h, y, row):
        for c in range(2):
            ref[h, pl.ds(y * nx, nx), c] = row[c]

    waves = [dy_order[:1]] + [dy_order[i:i + 2] for i in range(1, ny, 2)]

    def mix_lanes(rows, layer):
        x = jnp.concatenate([jnp.concatenate([re.reshape(nx * 8, LANES), im.reshape(nx * 8, LANES)], axis=1)
                             for re, im in rows], axis=0)
        x = matmul(x, lane_mix[layer])
        parts = [x[n * nx * 8:(n + 1) * nx * 8] for n in range(len(rows))]
        return [(p[:, :LANES].reshape(nx, 8, LANES), p[:, LANES:].reshape(nx, 8, LANES)) for p in parts]

    def lanes_late(even, h):
        return [] if h else waves[:1] if even else waves

    def send_half(par, h, layer, tan_half, source, late):
        rows = {}

        def leave(wave, dy):
            y = (my_y + dy) % ny
            store_row(send.at[par], h, y, rows[dy])
            for dx in dx_order:
                for dc in (1, 0):
                    if dy or dx or dc:
                        _, x, dest = peer(dy, dx, dc)
                        pltpu.make_async_remote_copy(
                            src_ref=send.at[par, h, dest], dst_ref=recv.at[par, h, me],
                            send_sem=send_sem.at[par, h], recv_sem=recv_sem.at[par, h, wave],
                            device_id={"qy": y, "qx": x}, device_id_type=MESH_ID).start()

        for group in (waves[:1], waves[1:]) if late else (waves,):
            for dy in [dy for wave in group for dy in wave]:
                rows[dy] = mix_leading(*load_row(source, h, (my_y + dy) % ny), tan_half, nx)
            early = [dy for wave in group if wave not in late for dy in wave]
            if early:
                rows.update(zip(early, mix_lanes([rows[dy] for dy in early], layer)))
            for wave in group:
                for dy in wave:
                    leave(waves.index(wave), dy)
        for c in range(2):
            recv[par, h, me, c] = send[par, h, me, c]

    def wait_sends(par, h):
        view = send.at[par, h, pl.ds(0, nb - 1)]
        pltpu.make_async_copy(view, view, send_sem.at[par, h]).wait()

    sub = lax.broadcasted_iota(jnp.int32, (nx, 8, LANES), 1)

    def receive(par, h, layer, tan_half, target, late):
        late_rows = []
        for n, wave in enumerate(waves):
            count = len(wave) * nx - (1 if 0 in wave else 0)
            view = recv.at[par, h, pl.ds(0, count)]
            pltpu.make_async_copy(view, view, recv_sem.at[par, h, n]).wait()
            for dy in wave:
                y = (my_y + ny - dy) % ny
                re, im = load_row(recv.at[par], h, y)
                for dist in (1, 2, 4):
                    re, im = (re + tan_half * sublane_partner(im, sub, dist),
                              im - tan_half * sublane_partner(re, sub, dist))
                re, im = mix_leading(re, im, tan_half, nx)
                if wave in late:
                    late_rows.append((y, (re, im)))
                else:
                    store_row(target, h, y, (re, im))
            if late_rows and wave == late[-1]:
                for (y, _), row in zip(late_rows, mix_lanes([row for _, row in late_rows], layer)):
                    store_row(target, h, y, row)

    def per_half(body):
        lax.fori_loop(0, 2, lambda h, _: (body(h), 0)[1], 0)

    for copy in inputs:
        copy.wait()
    make_lanes([0])
    make_table(0, cost)
    tan0 = angle[0]

    def first(places):
        flat = jnp.full((8, LANES), amp, jnp.float32)
        blocks = turn([(flat, jnp.zeros_like(flat)) for _ in places], 0, places)
        store(kept.at[num_layers], places, blocks)
        store(work, places, mix_all(blocks, tan0))

    for_columns((0, 1), first)
    for place in range(acc.shape[0]):
        acc[place] = jnp.zeros((8, LANES), jnp.float32)

    pl.semaphore_wait(barrier, nb - 1)

    for dy, dx, dc in offsets:
        y, x, dest = peer(dy, dx, dc)
        pltpu.make_async_remote_copy(
            src_ref=cost.at[dest], dst_ref=cost_b.at[me], send_sem=cost_send, recv_sem=cost_recv,
            device_id={"qy": y, "qx": x}, device_id_type=MESH_ID).start()
    for h in range(2):
        cost_b[me, h] = cost[me, h]
    for h in range(2):
        send_half(0, h, 0, tan0, work, lanes_late(True, h))
    make_lanes(range(1, num_layers))
    view = cost_b.at[pl.ds(0, nb - 1)]
    pltpu.make_async_copy(view, view, cost_recv).wait()
    make_table(1, cost_b)

    before_at, lam_pre, lam, side_at, sums_at = (num_layers, 2 * num_layers, 2 * num_layers + 1,
                                                 2 * num_layers + 2, 2 * num_layers + 4)
    root = jnp.float32(1.0 / amp)
    zero = jnp.zeros((8, LANES), jnp.float32)
    pairs = num_layers // 2

    def plan(step):
        back = step // num_layers
        done = step + back * (2 * num_layers - 1 - 2 * step)
        return back, done, done + 1 - back, (done + 1 - 2 * back + num_layers) % num_layers

    def middle(step):
        back, done, turned, following = plan(step)
        tan_half, tan_next = angle[done], angle[following]
        first_at = done + back * (lam_pre - done)
        second_at = before_at + turned + back * (lam - before_at - turned)

        def body(places):
            blocks = mix_all(load(work, places), tan_half)
            store(kept.at[first_at], places, blocks)
            blocks = turn(blocks, turned, places)
            store(kept.at[second_at], places, blocks)
            store(work, places, mix_all(blocks, tan_next))

        return body

    def turn_point(places):
        tan_half = angle[last]
        blocks = mix_all(load(work, places), tan_half)
        store(kept.at[last], places, blocks)
        conj = []
        energy = acc[0]
        for (h, j), (re, im) in zip(places, blocks):
            c = cost[j, h]
            conj.append((c * re, -(c * im)))
            energy += c * (re * re + im * im)
        acc[0] = energy
        store(kept.at[lam], places, conj)
        store(work, places, mix_all(conj, tan_half))

    def im_dot(conj, right):
        return conj[0] * right[1] + conj[1] * right[0]

    def sums_of(re, im, size):
        total_re, total_im, stride = swapped(re, 1), swapped(im, 1), 2
        while stride < size:
            total_re, total_im, stride = total_re + swapped(re, stride), total_im + swapped(im, stride), 2 * stride
        return total_re, total_im

    def high_sums(at):
        def body(x, _):
            for h in range(2):
                places = column(x, (h,))
                sums = partner_sums(load(kept.at[at], places))
                store(qbuf, places, [(a + c, b + d) for (a, b), (c, d) in zip(sums, load(qbuf, places))])
            return 0

        lax.fori_loop(0, nx, body, 0)

    def low_sums(at):
        def low(n, _):
            h, y = n // ny, n % ny
            re, im = load_row(kept.at[at], h, y)
            store_row(qbuf, h, y, sums_of(re, im, nx))
            return 0

        lax.fori_loop(0, 2 * ny, low, 0)

    def full_sums(at):
        def inner(y, _):
            rows = [load_row(kept.at[at], h, y) for h in range(2)]
            x = jnp.concatenate([jnp.concatenate([re.reshape(nx * 8, LANES), im.reshape(nx * 8, LANES)], axis=1)
                                 for re, im in rows], axis=0)
            lanes = matmul(x, lane_sum[...])
            for h in range(2):
                sre, sim = sums_of(*rows[h], nx)
                (re, im), (ore, oim) = rows[h], rows[1 - h]
                for dist in (1, 2, 4):
                    sre += sublane_partner(re, sub, dist)
                    sim += sublane_partner(im, sub, dist)
                mine = lanes[h * nx * 8:(h + 1) * nx * 8]
                store_row(qbuf, h, y, (sre + ore + mine[:, :LANES].reshape(nx, 8, LANES),
                                       sim + oim + mine[:, LANES:].reshape(nx, 8, LANES)))
            return 0

        lax.fori_loop(0, ny, inner, 0)
        high_sums(at)

    def prepare(layer):
        low_sums(layer)
        high_sums(layer)

        def body(j, total):
            for h in range(2):
                total += im_dot((kept[lam, h, j, 0], kept[lam, h, j, 1]), (qbuf[h, j, 0], qbuf[h, j, 1]))
            return total

        acc[1 + num_layers + layer] = lax.fori_loop(0, nb, body, zero)
        full_sums(before_at + layer)

    def collect(layer, source):
        at = before_at + layer

        def body(j, sums):
            gamma_sum, beta_sum = sums
            for h in range(2):
                left = (kept[lam_pre, h, j, 0], kept[lam_pre, h, j, 1])
                gamma_sum += source[j, h] * im_dot(left, (kept[at, h, j, 0], kept[at, h, j, 1]))
                beta_sum += im_dot(left, (qbuf[h, j, 0], qbuf[h, j, 1]))
            return gamma_sum, beta_sum

        gamma_sum, beta_sum = lax.fori_loop(0, nb, body, (zero, zero))
        acc[1 + layer] = 2.0 * gamma_sum
        acc[1 + num_layers + layer] += beta_sum

    def side_source(k):
        @pl.when(k == 0)
        def _():
            def body(places):
                blocks = [(cost[j, h] * re, cost[j, h] * im)
                          for (h, j), (re, im) in zip(places, load(kept.at[before_at], places))]
                store(side, places, mix_all(blocks, tan0))

            for_columns((0, 1), body)

        @pl.when(k == 2)
        def _():
            low_sums(before_at)
            high_sums(before_at)
            for_columns((0, 1), lambda places: store(side, places, mix_all(load(qbuf, places), tan0)))

    def side_arrival(n):
        per_half(lambda h: receive(2 + n, h, 0, tan0, side, []))

        def body(places):
            for h in range(2):
                mine = places[h::2]
                store(kept.at[side_at + n], mine, mix_all(load(side, mine), tan0))

        for_columns((0, 1), body)

    def side_sums():
        full_sums(0)

        def body(j, _):
            for h in range(2):
                for c in range(2):
                    kept[sums_at, h, j, c] = qbuf[h, j, c] + kept[side_at + 1, h, j, c]
            return 0

        lax.fori_loop(0, nb, body, 0)

    def last_sums(h):
        def body(x, sums):
            gamma1, beta1, gamma0, beta0 = sums
            places = column(x, (h,))
            blocks = mix_all(load(work, places), angle[1])
            for (h_, j), left, right, q in zip(places, blocks, load(kept.at[before_at + 1], places), load(qbuf, places)):
                gamma1 += cost_b[j, h_] * im_dot(left, right)
                beta1 += im_dot(left, q)
            blocks = turn(blocks, 1, places)
            for left, right, q in zip(blocks, load(kept.at[side_at], places), load(kept.at[sums_at], places)):
                gamma0 += im_dot(left, right)
                beta0 += im_dot(left, q)
            return gamma1, beta1, gamma0, beta0

        gamma1, beta1, gamma0, beta0 = lax.fori_loop(0, nx, body, (zero,) * 4)
        acc[1] += 2.0 * gamma0
        acc[2] += 2.0 * gamma1
        acc[1 + num_layers] += beta0
        acc[2 + num_layers] += beta1

    def two_gaps(k, _):
        step = 2 * k
        _, done, _, following = plan(step)
        tan_half, tan_next = angle[done], angle[following]

        def half(h):
            receive(0, h, done, tan_half, work, lanes_late(True, h))
            for_columns((h,), middle(step))

            @pl.when(k > 0)
            def _():
                wait_sends(1, h)

            send_half(1, h, following, tan_next, work, lanes_late(False, h))

        for h in range(2):
            half(h)

        side_source(k)

        @pl.when(k < pairs - 1)
        def _():
            make_table(step + 2, cost)

        @pl.when(k >= pairs)
        def _():
            collect(done, cost_b)
            prepare(following)

        @pl.when((k < 3) | (k == 4))
        def _():
            piece = k - k // 4
            send_half(2 + piece // 2, piece % 2, 0, tan0, side, [])

        step = 2 * k + 1
        _, done, _, following = plan(step)
        tan_half = angle[done]
        for h in range(2):
            receive(1, h, done, tan_half, work, lanes_late(False, h))

        @pl.when(k % pairs < pairs - 1)
        def _():
            for_columns((0, 1), middle(step))

        @pl.when(k == pairs - 1)
        def _():
            for_columns((0, 1), turn_point)

        into = following - (k // (pairs - 1)) * (1 - k // pairs) * (following - last)
        tan_next = angle[into]

        def half_joint(h):
            wait_sends(0, h)
            send_half(0, h, into, tan_next, work, lanes_late(True, h))

        for h in range(2):
            half_joint(h)

        @pl.when(k < pairs - 1)
        def _():
            make_table(step + 2, cost_b)

        @pl.when(k == pairs - 1)
        def _():
            def write(j, _):
                for h in range(2):
                    for c in range(2):
                        final[c, j, h] = root * kept[last, h, j, c]
                return 0

            lax.fori_loop(0, nb, write, 0)

        @pl.when(k >= pairs)
        def _():
            collect(done, cost)

        @pl.when((k == 4) | (k == 5))
        def _():
            side_arrival(k - 4)

        @pl.when(k == 2 * pairs - 2)
        def _():
            side_sums()

        @pl.when(k >= pairs - 1)
        def _():
            prepare(2 * num_layers - 3 - 2 * k)

        return 0

    lax.fori_loop(0, 2 * pairs - 1, two_gaps, 0)

    def last_half(h):
        receive(0, h, 1, angle[1], work, lanes_late(True, h))
        last_sums(h)

    for h in range(2):
        last_half(h)

    lane = lax.broadcasted_iota(jnp.int32, (1, LANES), 1)
    row = jnp.zeros((1, LANES), jnp.float32)
    for place in range(acc.shape[0]):
        value = jnp.sum(jnp.sum(acc[place], axis=0, keepdims=True), axis=1, keepdims=True)
        row = jnp.where(lane == place, value, row)
    part[...] = row
    for dy, dx, dc in offsets:
        y, x, dest = peer(dy, dx, dc)
        pltpu.make_async_remote_copy(
            src_ref=part, dst_ref=gath.at[me], send_sem=sum_send, recv_sem=sum_recv,
            device_id={"qy": y, "qx": x}, device_id_type=MESH_ID).start()
    gath[me] = row
    for par in range(4):
        for h in range(2):
            wait_sends(par, h)
    view = cost_b.at[pl.ds(0, nb - 1)]
    pltpu.make_async_copy(view, view, cost_send).wait()
    view = gath.at[pl.ds(0, nb - 1)]
    pltpu.make_async_copy(view, view, sum_recv).wait()
    total = gath[0]
    for j in range(1, nb):
        total += gath[j]
    totals[...] = total
    view = gath.at[pl.ds(0, nb - 1)]
    pltpu.make_async_copy(view, view, sum_send).wait()


def solution(mesh):
    ny, nx = mesh.shape["qy"], mesh.shape["qx"]
    nb = ny * nx

    def local_run(cost_local, gamma_angles, beta_angles):
        chunk = cost_local.shape[0]
        num_layers = gamma_angles.shape[0]
        assert chunk == nb * 16 * LANES and num_layers % 2 == 0 and num_layers >= 8
        num_qubits = int(math.log2(chunk * nb))
        amp = (chunk * nb) ** -0.5
        vmem, smem, dma = pltpu.VMEM, pltpu.SMEM, pltpu.SemaphoreType.DMA
        f32 = jnp.float32
        state = (2, nb, 2, 8, LANES)
        final, totals = pl.pallas_call(
            functools.partial(kernel, ny, nx, num_layers, num_qubits, amp),
            out_shape=(jax.ShapeDtypeStruct((2, nb, 2, 8, LANES), f32), jax.ShapeDtypeStruct((1, LANES), f32)),
            in_specs=[pl.BlockSpec(memory_space=pltpu.MemorySpace.HBM)] * 3,
            out_specs=(pl.BlockSpec(memory_space=vmem), pl.BlockSpec(memory_space=vmem)),
            scratch_shapes=[
                vmem((nb, 2, 8, LANES), f32),
                smem((num_layers,), f32),
                smem((num_layers,), f32),
                vmem((nb, 2, 8, LANES), f32),
                vmem((num_layers, 2, 2, nb, 8, LANES), f32),
                vmem((2 * num_layers + 5,) + state, f32),
                vmem((4,) + state, f32),
                vmem((4,) + state, f32),
                vmem(state, f32),
                vmem(state, f32),
                vmem(state, f32),
                vmem((num_layers, 8, LANES), f32),
                vmem((num_layers, 2 * LANES, 2 * LANES), f32),
                vmem((2 * LANES, 2 * LANES), f32),
                vmem((1 + 2 * num_layers, 8, LANES), f32),
                vmem((1, LANES), f32),
                vmem((nb, 1, LANES), f32),
                dma((3,)),
                dma((4, 2)),
                dma((4, 2, 1 + ny // 2)),
                dma,
                dma,
                dma,
                dma,
            ],
            compiler_params=pltpu.CompilerParams(
                collective_id=0, has_side_effects=True, vmem_limit_bytes=48 * 1024 * 1024),
            name="qaoa",
        )(cost_local.reshape(nb, 2, 8, LANES), gamma_angles, beta_angles)
        energy = totals[0, :1]
        grad = totals[0, 1:1 + 2 * num_layers]
        return energy, grad, final.reshape(2, chunk)

    state_spec = P(("inst", "qy", "qx"))
    return jax.shard_map(
        local_run, mesh=mesh, in_specs=(state_spec, P(), P()),
        out_specs=(P("inst"), P("inst"), P(None, ("inst", "qy", "qx"))), check_vma=False)
```

```python
import functools
import math

import jax
import jax.numpy as jnp
from jax import lax
from jax.experimental import pallas as pl
from jax.experimental.pallas import tpu as pltpu
from jax.sharding import PartitionSpec as P

LANES = 128
MESH_ID = pl.DeviceIdType.MESH


def mix_pair(blocks, tan_half, stride):
    out = list(blocks)
    for low in range(len(blocks)):
        if low & stride:
            continue
        high = low | stride
        (re0, im0), (re1, im1) = blocks[low], blocks[high]
        out[low] = (re0 + tan_half * im1, im0 - tan_half * re1)
        out[high] = (re1 + tan_half * im0, im1 - tan_half * re0)
    return out


def mix_all(blocks, tan_half):
    stride = 1
    while stride < len(blocks):
        blocks = mix_pair(blocks, tan_half, stride)
        stride *= 2
    return blocks


def partner_sums(blocks):
    out = []
    for place in range(len(blocks)):
        stride, re, im = 1, None, None
        while stride < len(blocks):
            pre, pim = blocks[place ^ stride]
            re, im = (pre, pim) if re is None else (re + pre, im + pim)
            stride *= 2
        out.append((re, im))
    return out


def sublane_partner(x, ids, dist):
    return jnp.take_along_axis(x, ids ^ dist, axis=1, mode="promise_in_bounds")


def swapped(x, stride):
    pairs = x.reshape((x.shape[0] // (2 * stride), 2, stride) + x.shape[1:])
    return jnp.concatenate([pairs[:, 1:], pairs[:, :1]], axis=1).reshape(x.shape)


def mix_leading(re, im, tan_half, size):
    stride = 1
    while stride < size:
        re, im = re + tan_half * swapped(im, stride), im - tan_half * swapped(re, stride)
        stride *= 2
    return re, im


def matmul(x, w):
    return jnp.dot(x, w, precision=lax.Precision.HIGHEST, preferred_element_type=jnp.float32)


def kernel(ny, nx, num_layers, num_qubits, amp, cost_in, gamma_in, beta_in, final, totals,
           cost, gamma, beta, cost_b, tabs, kept, recv, send, work, side, qbuf, angle, lane_mix, lane_sum, acc, part, gath,
           load_sem, send_sem, recv_sem, cost_send, cost_recv, sum_send, sum_recv):
    nb = ny * nx
    chips = nx // 2
    last = num_layers - 1
    my_y = lax.axis_index("qy")
    my_x = lax.axis_index("qx")
    my_chip, my_core = my_x // 2, my_x % 2
    me = my_y * nx + my_x

    def peer(dy, dx, dc):
        y = (my_y + dy) % ny
        x = ((my_chip + dx) % chips) * 2 + (my_core + dc) % 2
        return y, x, y * nx + x

    dy_order = sorted(range(ny), key=lambda d: -min(d, ny - d))
    dx_order = sorted(range(chips), key=lambda d: -min(d, chips - d))
    offsets = [(dy, dx, dc) for dy in dy_order for dx in dx_order for dc in (1, 0) if dy or dx or dc]

    inputs = [pltpu.make_async_copy(src, dst, load_sem.at[n])
              for n, (src, dst) in enumerate([(gamma_in, gamma), (beta_in, beta), (cost_in, cost)])]
    for copy in inputs:
        copy.start()
    barrier = pltpu.get_barrier_semaphore()
    for dy, dx, dc in offsets:
        y, x, _ = peer(dy, dx, dc)
        pl.semaphore_signal(barrier, inc=1, device_id={"qy": y, "qx": x}, device_id_type=MESH_ID)

    def make_angle(layer):
        half = jnp.full((8, LANES), 0.5 * beta[layer], jnp.float32)
        cos_half, sin_half = jnp.cos(half), jnp.sin(half)
        scale, power, left = None, cos_half, num_qubits - 7
        while left:
            if left % 2:
                scale = power if scale is None else scale * power
            power, left = power * power, left // 2
        angle[layer] = sin_half / cos_half
        return cos_half[:1], sin_half[:1], scale[:1]

    def make_lanes(layers):
        flips = lax.broadcasted_iota(jnp.int32, (LANES, LANES), 0) ^ lax.broadcasted_iota(jnp.int32, (LANES, LANES), 1)
        weight = sum((flips >> bit) & 1 for bit in range(7))
        for layer in layers:
            c, s, scale = make_angle(layer)
            coefs = []
            for k in range(8):
                coef = scale
                for factor in [c] * (7 - k) + [s] * k:
                    coef = coef * factor
                coefs.append(coef if (k // 2) % 2 == 0 else -coef)
            even, odd = jnp.zeros((LANES, LANES), jnp.float32), jnp.zeros((LANES, LANES), jnp.float32)
            for k in range(8):
                if k % 2 == 0:
                    even = jnp.where(weight == k, coefs[k], even)
                else:
                    odd = jnp.where(weight == k, coefs[k], odd)
            lane_mix[layer, :LANES, :LANES] = even
            lane_mix[layer, LANES:, LANES:] = even
            lane_mix[layer, LANES:, :LANES] = odd
            lane_mix[layer, :LANES, LANES:] = -odd
        if 0 not in layers:
            ones = jnp.where(weight == 1, 1.0, 0.0).astype(jnp.float32)
            lane_sum[:LANES, :LANES] = ones
            lane_sum[LANES:, LANES:] = ones
            lane_sum[:LANES, LANES:] = jnp.zeros_like(ones)
            lane_sum[LANES:, :LANES] = jnp.zeros_like(ones)

    def make_table(layer, source):
        g = gamma[layer]

        def body(j, _):
            for h in range(2):
                theta = g * source[j, h]
                tabs[layer, 0, h, j] = jnp.cos(theta)
                tabs[layer, 1, h, j] = jnp.sin(theta)
            return 0

        lax.fori_loop(0, nb, body, 0)

    def load(ref, places):
        return [(ref[h, j, 0], ref[h, j, 1]) for h, j in places]

    def store(ref, places, blocks):
        for (h, j), (re, im) in zip(places, blocks):
            ref[h, j, 0] = re
            ref[h, j, 1] = im

    def turn(blocks, layer, places):
        out = []
        for (re, im), (h, j) in zip(blocks, places):
            c, s = tabs[layer, 0, h, j], tabs[layer, 1, h, j]
            out.append((c * re + s * im, c * im - s * re))
        return out

    def column(x, halves):
        return [(h, y * nx + x) for y in range(ny) for h in halves]

    def for_columns(halves, body):
        lax.fori_loop(0, nx, lambda x, _: (body(column(x, halves)), 0)[1], 0, unroll=4)

    def load_row(ref, h, y):
        return ref[h, pl.ds(y * nx, nx), 0], ref[h, pl.ds(y * nx, nx), 1]

    def store_row(ref, h, y, row):
        for c in range(2):
            ref[h, pl.ds(y * nx, nx), c] = row[c]

    waves = [dy_order[:1]] + [dy_order[i:i + 2] for i in range(1, ny, 2)]

    def mix_lanes(rows, layer):
        x = jnp.concatenate([jnp.concatenate([re.reshape(nx * 8, LANES), im.reshape(nx * 8, LANES)], axis=1)
                             for re, im in rows], axis=0)
        x = matmul(x, lane_mix[layer])
        parts = [x[n * nx * 8:(n + 1) * nx * 8] for n in range(len(rows))]
        return [(p[:, :LANES].reshape(nx, 8, LANES), p[:, LANES:].reshape(nx, 8, LANES)) for p in parts]

    def lanes_late(even, h):
        return ([] if h else waves[:1]) if even else (waves[:1] if h else waves)

    def send_half(par, h, layer, tan_half, source, late):
        rows = {}

        def leave(wave, dy):
            y = (my_y + dy) % ny
            store_row(send.at[par], h, y, rows[dy])
            for dx in dx_order:
                for dc in (1, 0):
                    if dy or dx or dc:
                        _, x, dest = peer(dy, dx, dc)
                        pltpu.make_async_remote_copy(
                            src_ref=send.at[par, h, dest], dst_ref=recv.at[par, h, me],
                            send_sem=send_sem.at[par, h], recv_sem=recv_sem.at[par, h, wave],
                            device_id={"qy": y, "qx": x}, device_id_type=MESH_ID).start()

        for group in (waves[:1], waves[1:]) if late else (waves,):
            for dy in [dy for wave in group for dy in wave]:
                rows[dy] = mix_leading(*load_row(source, h, (my_y + dy) % ny), tan_half, nx)
            early = [dy for wave in group if wave not in late for dy in wave]
            if early:
                rows.update(zip(early, mix_lanes([rows[dy] for dy in early], layer)))
            for wave in group:
                for dy in wave:
                    leave(waves.index(wave), dy)
        for c in range(2):
            recv[par, h, me, c] = send[par, h, me, c]

    def wait_sends(par, h):
        view = send.at[par, h, pl.ds(0, nb - 1)]
        pltpu.make_async_copy(view, view, send_sem.at[par, h]).wait()

    sub = lax.broadcasted_iota(jnp.int32, (nx, 8, LANES), 1)

    def receive(par, h, layer, tan_half, target, late):
        late_rows = []
        for n, wave in enumerate(waves):
            count = len(wave) * nx - (1 if 0 in wave else 0)
            view = recv.at[par, h, pl.ds(0, count)]
            pltpu.make_async_copy(view, view, recv_sem.at[par, h, n]).wait()
            for dy in wave:
                y = (my_y + ny - dy) % ny
                re, im = load_row(recv.at[par], h, y)
                for dist in (1, 2, 4):
                    re, im = (re + tan_half * sublane_partner(im, sub, dist),
                              im - tan_half * sublane_partner(re, sub, dist))
                re, im = mix_leading(re, im, tan_half, nx)
                if wave in late:
                    late_rows.append((y, (re, im)))
                else:
                    store_row(target, h, y, (re, im))
            if late_rows and wave == late[-1]:
                for (y, _), row in zip(late_rows, mix_lanes([row for _, row in late_rows], layer)):
                    store_row(target, h, y, row)

    def per_half(body):
        lax.fori_loop(0, 2, lambda h, _: (body(h), 0)[1], 0)

    for copy in inputs:
        copy.wait()
    make_lanes([0])
    make_table(0, cost)
    tan0 = angle[0]

    def first(places):
        flat = jnp.full((8, LANES), amp, jnp.float32)
        blocks = turn([(flat, jnp.zeros_like(flat)) for _ in places], 0, places)
        store(kept.at[num_layers], places, blocks)
        store(work, places, mix_all(blocks, tan0))

    for_columns((0, 1), first)
    for place in range(acc.shape[0]):
        acc[place] = jnp.zeros((8, LANES), jnp.float32)

    pl.semaphore_wait(barrier, nb - 1)

    for dy, dx, dc in offsets:
        y, x, dest = peer(dy, dx, dc)
        pltpu.make_async_remote_copy(
            src_ref=cost.at[dest], dst_ref=cost_b.at[me], send_sem=cost_send, recv_sem=cost_recv,
            device_id={"qy": y, "qx": x}, device_id_type=MESH_ID).start()
    for h in range(2):
        cost_b[me, h] = cost[me, h]
    for h in range(2):
        send_half(0, h, 0, tan0, work, lanes_late(True, h))
    make_lanes(range(1, num_layers))
    view = cost_b.at[pl.ds(0, nb - 1)]
    pltpu.make_async_copy(view, view, cost_recv).wait()
    make_table(1, cost_b)

    before_at, lam_pre, lam, side_at, sums_at = (num_layers, 2 * num_layers, 2 * num_layers + 1,
                                                 2 * num_layers + 2, 2 * num_layers + 4)
    root = jnp.float32(1.0 / amp)
    zero = jnp.zeros((8, LANES), jnp.float32)
    pairs = num_layers // 2

    def plan(step):
        back = step // num_layers
        done = step + back * (2 * num_layers - 1 - 2 * step)
        return back, done, done + 1 - back, (done + 1 - 2 * back + num_layers) % num_layers

    def middle(step):
        back, done, turned, following = plan(step)
        tan_half, tan_next = angle[done], angle[following]
        first_at = done + back * (lam_pre - done)
        second_at = before_at + turned + back * (lam - before_at - turned)

        def body(places):
            blocks = mix_all(load(work, places), tan_half)
            store(kept.at[first_at], places, blocks)
            blocks = turn(blocks, turned, places)
            store(kept.at[second_at], places, blocks)
            store(work, places, mix_all(blocks, tan_next))

        return body

    def turn_point(places):
        tan_half = angle[last]
        blocks = mix_all(load(work, places), tan_half)
        store(kept.at[last], places, blocks)
        conj = []
        energy = acc[0]
        for (h, j), (re, im) in zip(places, blocks):
            c = cost[j, h]
            conj.append((c * re, -(c * im)))
            energy += c * (re * re + im * im)
        acc[0] = energy
        store(kept.at[lam], places, conj)
        store(work, places, mix_all(conj, tan_half))

    def im_dot(conj, right):
        return conj[0] * right[1] + conj[1] * right[0]

    def sums_of(re, im, size):
        total_re, total_im, stride = swapped(re, 1), swapped(im, 1), 2
        while stride < size:
            total_re, total_im, stride = total_re + swapped(re, stride), total_im + swapped(im, stride), 2 * stride
        return total_re, total_im

    def high_sums(at):
        def body(x, _):
            for h in range(2):
                places = column(x, (h,))
                sums = partner_sums(load(kept.at[at], places))
                store(qbuf, places, [(a + c, b + d) for (a, b), (c, d) in zip(sums, load(qbuf, places))])
            return 0

        lax.fori_loop(0, nx, body, 0)

    def low_sums(at):
        def low(n, _):
            h, y = n // ny, n % ny
            re, im = load_row(kept.at[at], h, y)
            store_row(qbuf, h, y, sums_of(re, im, nx))
            return 0

        lax.fori_loop(0, 2 * ny, low, 0)

    def full_sums(at):
        def inner(y, _):
            rows = [load_row(kept.at[at], h, y) for h in range(2)]
            x = jnp.concatenate([jnp.concatenate([re.reshape(nx * 8, LANES), im.reshape(nx * 8, LANES)], axis=1)
                                 for re, im in rows], axis=0)
            lanes = matmul(x, lane_sum[...])
            for h in range(2):
                sre, sim = sums_of(*rows[h], nx)
                (re, im), (ore, oim) = rows[h], rows[1 - h]
                for dist in (1, 2, 4):
                    sre += sublane_partner(re, sub, dist)
                    sim += sublane_partner(im, sub, dist)
                mine = lanes[h * nx * 8:(h + 1) * nx * 8]
                store_row(qbuf, h, y, (sre + ore + mine[:, :LANES].reshape(nx, 8, LANES),
                                       sim + oim + mine[:, LANES:].reshape(nx, 8, LANES)))
            return 0

        lax.fori_loop(0, ny, inner, 0)
        high_sums(at)

    def prepare(layer):
        low_sums(layer)
        high_sums(layer)

        def body(j, total):
            for h in range(2):
                total += im_dot((kept[lam, h, j, 0], kept[lam, h, j, 1]), (qbuf[h, j, 0], qbuf[h, j, 1]))
            return total

        acc[1 + num_layers + layer] = lax.fori_loop(0, nb, body, zero)
        full_sums(before_at + layer)

    def collect(layer, source):
        at = before_at + layer

        def body(j, sums):
            gamma_sum, beta_sum = sums
            for h in range(2):
                left = (kept[lam_pre, h, j, 0], kept[lam_pre, h, j, 1])
                gamma_sum += source[j, h] * im_dot(left, (kept[at, h, j, 0], kept[at, h, j, 1]))
                beta_sum += im_dot(left, (qbuf[h, j, 0], qbuf[h, j, 1]))
            return gamma_sum, beta_sum

        gamma_sum, beta_sum = lax.fori_loop(0, nb, body, (zero, zero))
        acc[1 + layer] = 2.0 * gamma_sum
        acc[1 + num_layers + layer] += beta_sum

    def side_source(k):
        @pl.when(k == 0)
        def _():
            def body(places):
                blocks = [(cost[j, h] * re, cost[j, h] * im)
                          for (h, j), (re, im) in zip(places, load(kept.at[before_at], places))]
                store(side, places, mix_all(blocks, tan0))

            for_columns((0, 1), body)

        @pl.when(k == 2)
        def _():
            low_sums(before_at)
            high_sums(before_at)
            for_columns((0, 1), lambda places: store(side, places, mix_all(load(qbuf, places), tan0)))

    def side_arrival(n):
        per_half(lambda h: receive(2 + n, h, 0, tan0, side, []))

        def body(places):
            for h in range(2):
                mine = places[h::2]
                store(kept.at[side_at + n], mine, mix_all(load(side, mine), tan0))

        for_columns((0, 1), body)

    def side_sums():
        full_sums(0)

        def body(j, _):
            for h in range(2):
                for c in range(2):
                    kept[sums_at, h, j, c] = qbuf[h, j, c] + kept[side_at + 1, h, j, c]
            return 0

        lax.fori_loop(0, nb, body, 0)

    def last_sums(h):
        def body(x, sums):
            gamma1, beta1, gamma0, beta0 = sums
            places = column(x, (h,))
            blocks = mix_all(load(work, places), angle[1])
            for (h_, j), left, right, q in zip(places, blocks, load(kept.at[before_at + 1], places), load(qbuf, places)):
                gamma1 += cost_b[j, h_] * im_dot(left, right)
                beta1 += im_dot(left, q)
            blocks = turn(blocks, 1, places)
            for left, right, q in zip(blocks, load(kept.at[side_at], places), load(kept.at[sums_at], places)):
                gamma0 += im_dot(left, right)
                beta0 += im_dot(left, q)
            return gamma1, beta1, gamma0, beta0

        gamma1, beta1, gamma0, beta0 = lax.fori_loop(0, nx, body, (zero,) * 4)
        acc[1] += 2.0 * gamma0
        acc[2] += 2.0 * gamma1
        acc[1 + num_layers] += beta0
        acc[2 + num_layers] += beta1

    def two_gaps(k, _):
        step = 2 * k
        _, done, _, following = plan(step)
        tan_half, tan_next = angle[done], angle[following]

        def half(h):
            receive(0, h, done, tan_half, work, lanes_late(True, h))
            for_columns((h,), middle(step))

            @pl.when(k > 0)
            def _():
                wait_sends(1, h)

            send_half(1, h, following, tan_next, work, lanes_late(False, h))

        for h in range(2):
            half(h)

        side_source(k)

        @pl.when(k < pairs - 1)
        def _():
            make_table(step + 2, cost)

        @pl.when(k >= pairs)
        def _():
            collect(done, cost_b)
            prepare(following)

        @pl.when((k < 3) | (k == 4))
        def _():
            piece = k - k // 4
            send_half(2 + piece // 2, piece % 2, 0, tan0, side, [])

        step = 2 * k + 1
        _, done, _, following = plan(step)
        tan_half = angle[done]
        for h in range(2):
            receive(1, h, done, tan_half, work, lanes_late(False, h))

        @pl.when(k % pairs < pairs - 1)
        def _():
            for_columns((0, 1), middle(step))

        @pl.when(k == pairs - 1)
        def _():
            for_columns((0, 1), turn_point)

        into = following - (k // (pairs - 1)) * (1 - k // pairs) * (following - last)
        tan_next = angle[into]

        def half_joint(h):
            wait_sends(0, h)
            send_half(0, h, into, tan_next, work, lanes_late(True, h))

        for h in range(2):
            half_joint(h)

        @pl.when(k < pairs - 1)
        def _():
            make_table(step + 2, cost_b)

        @pl.when(k == pairs - 1)
        def _():
            def write(j, _):
                for h in range(2):
                    for c in range(2):
                        final[c, j, h] = root * kept[last, h, j, c]
                return 0

            lax.fori_loop(0, nb, write, 0)

        @pl.when(k >= pairs)
        def _():
            collect(done, cost)

        @pl.when((k == 4) | (k == 5))
        def _():
            side_arrival(k - 4)

        @pl.when(k == 2 * pairs - 2)
        def _():
            side_sums()

        @pl.when(k >= pairs - 1)
        def _():
            prepare(2 * num_layers - 3 - 2 * k)

        return 0

    lax.fori_loop(0, 2 * pairs - 1, two_gaps, 0)

    def last_half(h):
        receive(0, h, 1, angle[1], work, lanes_late(True, h))
        last_sums(h)

    for h in range(2):
        last_half(h)

    lane = lax.broadcasted_iota(jnp.int32, (1, LANES), 1)
    row = jnp.zeros((1, LANES), jnp.float32)
    for place in range(acc.shape[0]):
        value = jnp.sum(jnp.sum(acc[place], axis=0, keepdims=True), axis=1, keepdims=True)
        row = jnp.where(lane == place, value, row)
    part[...] = row
    for dy, dx, dc in offsets:
        y, x, dest = peer(dy, dx, dc)
        pltpu.make_async_remote_copy(
            src_ref=part, dst_ref=gath.at[me], send_sem=sum_send, recv_sem=sum_recv,
            device_id={"qy": y, "qx": x}, device_id_type=MESH_ID).start()
    gath[me] = row
    for par in range(4):
        for h in range(2):
            wait_sends(par, h)
    view = cost_b.at[pl.ds(0, nb - 1)]
    pltpu.make_async_copy(view, view, cost_send).wait()
    view = gath.at[pl.ds(0, nb - 1)]
    pltpu.make_async_copy(view, view, sum_recv).wait()
    total = gath[0]
    for j in range(1, nb):
        total += gath[j]
    totals[...] = total
    view = gath.at[pl.ds(0, nb - 1)]
    pltpu.make_async_copy(view, view, sum_send).wait()


def solution(mesh):
    ny, nx = mesh.shape["qy"], mesh.shape["qx"]
    nb = ny * nx

    def local_run(cost_local, gamma_angles, beta_angles):
        chunk = cost_local.shape[0]
        num_layers = gamma_angles.shape[0]
        assert chunk == nb * 16 * LANES and num_layers % 2 == 0 and num_layers >= 8
        num_qubits = int(math.log2(chunk * nb))
        amp = (chunk * nb) ** -0.5
        vmem, smem, dma = pltpu.VMEM, pltpu.SMEM, pltpu.SemaphoreType.DMA
        f32 = jnp.float32
        state = (2, nb, 2, 8, LANES)
        final, totals = pl.pallas_call(
            functools.partial(kernel, ny, nx, num_layers, num_qubits, amp),
            out_shape=(jax.ShapeDtypeStruct((2, nb, 2, 8, LANES), f32), jax.ShapeDtypeStruct((1, LANES), f32)),
            in_specs=[pl.BlockSpec(memory_space=pltpu.MemorySpace.HBM)] * 3,
            out_specs=(pl.BlockSpec(memory_space=vmem), pl.BlockSpec(memory_space=vmem)),
            scratch_shapes=[
                vmem((nb, 2, 8, LANES), f32),
                smem((num_layers,), f32),
                smem((num_layers,), f32),
                vmem((nb, 2, 8, LANES), f32),
                vmem((num_layers, 2, 2, nb, 8, LANES), f32),
                vmem((2 * num_layers + 5,) + state, f32),
                vmem((4,) + state, f32),
                vmem((4,) + state, f32),
                vmem(state, f32),
                vmem(state, f32),
                vmem(state, f32),
                vmem((num_layers, 8, LANES), f32),
                vmem((num_layers, 2 * LANES, 2 * LANES), f32),
                vmem((2 * LANES, 2 * LANES), f32),
                vmem((1 + 2 * num_layers, 8, LANES), f32),
                vmem((1, LANES), f32),
                vmem((nb, 1, LANES), f32),
                dma((3,)),
                dma((4, 2)),
                dma((4, 2, 1 + ny // 2)),
                dma,
                dma,
                dma,
                dma,
            ],
            compiler_params=pltpu.CompilerParams(
                collective_id=0, has_side_effects=True, vmem_limit_bytes=48 * 1024 * 1024),
            name="qaoa",
        )(cost_local.reshape(nb, 2, 8, LANES), gamma_angles, beta_angles)
        energy = totals[0, :1]
        grad = totals[0, 1:1 + 2 * num_layers]
        return energy, grad, final.reshape(2, chunk)

    state_spec = P(("inst", "qy", "qx"))
    return jax.shard_map(
        local_run, mesh=mesh, in_specs=(state_spec, P(), P()),
        out_specs=(P("inst"), P("inst"), P(None, ("inst", "qy", "qx"))), check_vma=False)
```

```python
import functools
import math

import jax
import jax.numpy as jnp
from jax import lax
from jax.experimental import pallas as pl
from jax.experimental.pallas import tpu as pltpu
from jax.sharding import PartitionSpec as P

LANES = 128
MESH_ID = pl.DeviceIdType.MESH


def mix_pair(blocks, tan_half, stride):
    out = list(blocks)
    for low in range(len(blocks)):
        if low & stride:
            continue
        high = low | stride
        (re0, im0), (re1, im1) = blocks[low], blocks[high]
        out[low] = (re0 + tan_half * im1, im0 - tan_half * re1)
        out[high] = (re1 + tan_half * im0, im1 - tan_half * re0)
    return out


def mix_all(blocks, tan_half):
    stride = 1
    while stride < len(blocks):
        blocks = mix_pair(blocks, tan_half, stride)
        stride *= 2
    return blocks


def partner_sums(blocks):
    out = []
    for place in range(len(blocks)):
        stride, re, im = 1, None, None
        while stride < len(blocks):
            pre, pim = blocks[place ^ stride]
            re, im = (pre, pim) if re is None else (re + pre, im + pim)
            stride *= 2
        out.append((re, im))
    return out


def sublane_partner(x, ids, dist):
    return jnp.take_along_axis(x, ids ^ dist, axis=1, mode="promise_in_bounds")


def swapped(x, stride):
    pairs = x.reshape((x.shape[0] // (2 * stride), 2, stride) + x.shape[1:])
    return jnp.concatenate([pairs[:, 1:], pairs[:, :1]], axis=1).reshape(x.shape)


def mix_leading(re, im, tan_half, size):
    stride = 1
    while stride < size:
        re, im = re + tan_half * swapped(im, stride), im - tan_half * swapped(re, stride)
        stride *= 2
    return re, im


def matmul(x, w):
    return jnp.dot(x, w, precision=lax.Precision.HIGHEST, preferred_element_type=jnp.float32)


def kernel(ny, nx, num_layers, num_qubits, amp, cost_in, gamma_in, beta_in, final, totals,
           cost, gamma, beta, cost_b, tabs, kept, recv, send, work, side, qbuf, angle, lane_mix, lane_sum, acc, part, gath,
           load_sem, send_sem, recv_sem, cost_send, cost_recv, sum_send, sum_recv):
    nb = ny * nx
    chips = nx // 2
    last = num_layers - 1
    my_y = lax.axis_index("qy")
    my_x = lax.axis_index("qx")
    my_chip, my_core = my_x // 2, my_x % 2
    me = my_y * nx + my_x

    def peer(dy, dx, dc):
        y = (my_y + dy) % ny
        x = ((my_chip + dx) % chips) * 2 + (my_core + dc) % 2
        return y, x, y * nx + x

    dy_order = sorted(range(ny), key=lambda d: -min(d, ny - d))
    dx_order = sorted(range(chips), key=lambda d: -min(d, chips - d))
    offsets = [(dy, dx, dc) for dy in dy_order for dx in dx_order for dc in (1, 0) if dy or dx or dc]

    inputs = [pltpu.make_async_copy(src, dst, load_sem.at[n])
              for n, (src, dst) in enumerate([(gamma_in, gamma), (beta_in, beta), (cost_in, cost)])]
    for copy in inputs:
        copy.start()
    barrier = pltpu.get_barrier_semaphore()
    for dy, dx, dc in offsets:
        y, x, _ = peer(dy, dx, dc)
        pl.semaphore_signal(barrier, inc=1, device_id={"qy": y, "qx": x}, device_id_type=MESH_ID)

    def make_angle(layer):
        half = jnp.full((8, LANES), 0.5 * beta[layer], jnp.float32)
        cos_half, sin_half = jnp.cos(half), jnp.sin(half)
        scale, power, left = None, cos_half, num_qubits - 7
        while left:
            if left % 2:
                scale = power if scale is None else scale * power
            power, left = power * power, left // 2
        angle[layer] = sin_half / cos_half
        return cos_half[:1], sin_half[:1], scale[:1]

    def make_lanes(layers):
        flips = lax.broadcasted_iota(jnp.int32, (LANES, LANES), 0) ^ lax.broadcasted_iota(jnp.int32, (LANES, LANES), 1)
        weight = sum((flips >> bit) & 1 for bit in range(7))
        for layer in layers:
            c, s, scale = make_angle(layer)
            coefs = []
            for k in range(8):
                coef = scale
                for factor in [c] * (7 - k) + [s] * k:
                    coef = coef * factor
                coefs.append(coef if (k // 2) % 2 == 0 else -coef)
            even, odd = jnp.zeros((LANES, LANES), jnp.float32), jnp.zeros((LANES, LANES), jnp.float32)
            for k in range(8):
                if k % 2 == 0:
                    even = jnp.where(weight == k, coefs[k], even)
                else:
                    odd = jnp.where(weight == k, coefs[k], odd)
            lane_mix[layer, :LANES, :LANES] = even
            lane_mix[layer, LANES:, LANES:] = even
            lane_mix[layer, LANES:, :LANES] = odd
            lane_mix[layer, :LANES, LANES:] = -odd
        if 0 not in layers:
            ones = jnp.where(weight == 1, 1.0, 0.0).astype(jnp.float32)
            lane_sum[:LANES, :LANES] = ones
            lane_sum[LANES:, LANES:] = ones
            lane_sum[:LANES, LANES:] = jnp.zeros_like(ones)
            lane_sum[LANES:, :LANES] = jnp.zeros_like(ones)

    def make_table(layer, source):
        g = gamma[layer]

        def body(j, _):
            for h in range(2):
                theta = g * source[j, h]
                tabs[layer, 0, h, j] = jnp.cos(theta)
                tabs[layer, 1, h, j] = jnp.sin(theta)
            return 0

        lax.fori_loop(0, nb, body, 0)

    def load(ref, places):
        return [(ref[h, j, 0], ref[h, j, 1]) for h, j in places]

    def store(ref, places, blocks):
        for (h, j), (re, im) in zip(places, blocks):
            ref[h, j, 0] = re
            ref[h, j, 1] = im

    def turn(blocks, layer, places):
        out = []
        for (re, im), (h, j) in zip(blocks, places):
            c, s = tabs[layer, 0, h, j], tabs[layer, 1, h, j]
            out.append((c * re + s * im, c * im - s * re))
        return out

    def column(x, halves):
        return [(h, y * nx + x) for y in range(ny) for h in halves]

    def for_columns(halves, body):
        lax.fori_loop(0, nx, lambda x, _: (body(column(x, halves)), 0)[1], 0, unroll=4)

    def load_row(ref, h, y):
        return ref[h, pl.ds(y * nx, nx), 0], ref[h, pl.ds(y * nx, nx), 1]

    def store_row(ref, h, y, row):
        for c in range(2):
            ref[h, pl.ds(y * nx, nx), c] = row[c]

    waves = [dy_order[:1]] + [dy_order[i:i + 2] for i in range(1, ny, 2)]

    def mix_lanes(rows, layer):
        x = jnp.concatenate([jnp.concatenate([re.reshape(nx * 8, LANES), im.reshape(nx * 8, LANES)], axis=1)
                             for re, im in rows], axis=0)
        x = matmul(x, lane_mix[layer])
        parts = [x[n * nx * 8:(n + 1) * nx * 8] for n in range(len(rows))]
        return [(p[:, :LANES].reshape(nx, 8, LANES), p[:, LANES:].reshape(nx, 8, LANES)) for p in parts]

    def lanes_late(even, h):
        return ([] if h else waves[:1]) if even else (waves[:1] if h else waves)

    def send_half(par, h, layer, tan_half, source, late):
        rows = {}

        def leave(wave, dy):
            y = (my_y + dy) % ny
            store_row(send.at[par], h, y, rows[dy])
            for dx in dx_order:
                for dc in (1, 0):
                    if dy or dx or dc:
                        _, x, dest = peer(dy, dx, dc)
                        pltpu.make_async_remote_copy(
                            src_ref=send.at[par, h, dest], dst_ref=recv.at[par, h, me],
                            send_sem=send_sem.at[par, h], recv_sem=recv_sem.at[par, h, wave],
                            device_id={"qy": y, "qx": x}, device_id_type=MESH_ID).start()

        for group in (waves[:1], waves[1:]) if late else (waves,):
            for dy in [dy for wave in group for dy in wave]:
                rows[dy] = mix_leading(*load_row(source, h, (my_y + dy) % ny), tan_half, nx)
            early = [dy for wave in group if wave not in late for dy in wave]
            if early:
                rows.update(zip(early, mix_lanes([rows[dy] for dy in early], layer)))
            for wave in group:
                for dy in wave:
                    leave(waves.index(wave), dy)
        for c in range(2):
            recv[par, h, me, c] = send[par, h, me, c]

    def wait_sends(par, h):
        view = send.at[par, h, pl.ds(0, nb - 1)]
        pltpu.make_async_copy(view, view, send_sem.at[par, h]).wait()

    sub = lax.broadcasted_iota(jnp.int32, (nx, 8, LANES), 1)

    def receive(par, h, layer, tan_half, target, late):
        late_rows = []
        for n, wave in enumerate(waves):
            count = len(wave) * nx - (1 if 0 in wave else 0)
            view = recv.at[par, h, pl.ds(0, count)]
            pltpu.make_async_copy(view, view, recv_sem.at[par, h, n]).wait()
            for dy in wave:
                y = (my_y + ny - dy) % ny
                re, im = load_row(recv.at[par], h, y)
                for dist in (1, 2, 4):
                    re, im = (re + tan_half * sublane_partner(im, sub, dist),
                              im - tan_half * sublane_partner(re, sub, dist))
                re, im = mix_leading(re, im, tan_half, nx)
                if wave in late:
                    late_rows.append((y, (re, im)))
                else:
                    store_row(target, h, y, (re, im))
            if late_rows and wave == late[-1]:
                for (y, _), row in zip(late_rows, mix_lanes([row for _, row in late_rows], layer)):
                    store_row(target, h, y, row)

    def per_half(body):
        lax.fori_loop(0, 2, lambda h, _: (body(h), 0)[1], 0)

    for copy in inputs:
        copy.wait()
    make_lanes([0])
    make_table(0, cost)
    tan0 = angle[0]

    def first(places):
        flat = jnp.full((8, LANES), amp, jnp.float32)
        blocks = turn([(flat, jnp.zeros_like(flat)) for _ in places], 0, places)
        store(kept.at[num_layers], places, blocks)
        store(work, places, mix_all(blocks, tan0))

    for_columns((0, 1), first)
    for place in range(acc.shape[0]):
        acc[place] = jnp.zeros((8, LANES), jnp.float32)

    pl.semaphore_wait(barrier, nb - 1)

    for dy, dx, dc in offsets:
        y, x, dest = peer(dy, dx, dc)
        pltpu.make_async_remote_copy(
            src_ref=cost.at[dest], dst_ref=cost_b.at[me], send_sem=cost_send, recv_sem=cost_recv,
            device_id={"qy": y, "qx": x}, device_id_type=MESH_ID).start()
    for h in range(2):
        cost_b[me, h] = cost[me, h]
    for h in range(2):
        send_half(0, h, 0, tan0, work, lanes_late(True, h))
    make_lanes(range(1, num_layers))
    view = cost_b.at[pl.ds(0, nb - 1)]
    pltpu.make_async_copy(view, view, cost_recv).wait()
    make_table(1, cost_b)

    before_at, lam_pre, lam, side_at, sums_at = (num_layers, 2 * num_layers, 2 * num_layers + 1,
                                                 2 * num_layers + 2, 2 * num_layers + 4)
    root = jnp.float32(1.0 / amp)
    zero = jnp.zeros((8, LANES), jnp.float32)
    pairs = num_layers // 2

    def plan(step):
        back = step // num_layers
        done = step + back * (2 * num_layers - 1 - 2 * step)
        return back, done, done + 1 - back, (done + 1 - 2 * back + num_layers) % num_layers

    def middle(step):
        back, done, turned, following = plan(step)
        tan_half, tan_next = angle[done], angle[following]
        first_at = done + back * (lam_pre - done)
        second_at = before_at + turned + back * (lam - before_at - turned)

        def body(places):
            blocks = mix_all(load(work, places), tan_half)
            store(kept.at[first_at], places, blocks)
            blocks = turn(blocks, turned, places)
            store(kept.at[second_at], places, blocks)
            store(work, places, mix_all(blocks, tan_next))

        return body

    def turn_point(places):
        tan_half = angle[last]
        blocks = mix_all(load(work, places), tan_half)
        store(kept.at[last], places, blocks)
        conj = []
        energy = acc[0]
        for (h, j), (re, im) in zip(places, blocks):
            c = cost[j, h]
            conj.append((c * re, -(c * im)))
            energy += c * (re * re + im * im)
        acc[0] = energy
        store(kept.at[lam], places, conj)
        store(work, places, mix_all(conj, tan_half))

    def im_dot(conj, right):
        return conj[0] * right[1] + conj[1] * right[0]

    def sums_of(re, im, size):
        total_re, total_im, stride = swapped(re, 1), swapped(im, 1), 2
        while stride < size:
            total_re, total_im, stride = total_re + swapped(re, stride), total_im + swapped(im, stride), 2 * stride
        return total_re, total_im

    def high_sums(at):
        def body(x, _):
            for h in range(2):
                places = column(x, (h,))
                sums = partner_sums(load(kept.at[at], places))
                store(qbuf, places, [(a + c, b + d) for (a, b), (c, d) in zip(sums, load(qbuf, places))])
            return 0

        lax.fori_loop(0, nx, body, 0)

    def low_sums(at):
        def low(n, _):
            h, y = n // ny, n % ny
            re, im = load_row(kept.at[at], h, y)
            store_row(qbuf, h, y, sums_of(re, im, nx))
            return 0

        lax.fori_loop(0, 2 * ny, low, 0)

    def full_sums(at):
        def inner(y, _):
            rows = [load_row(kept.at[at], h, y) for h in range(2)]
            x = jnp.concatenate([jnp.concatenate([re.reshape(nx * 8, LANES), im.reshape(nx * 8, LANES)], axis=1)
                                 for re, im in rows], axis=0)
            lanes = matmul(x, lane_sum[...])
            for h in range(2):
                sre, sim = sums_of(*rows[h], nx)
                (re, im), (ore, oim) = rows[h], rows[1 - h]
                for dist in (1, 2, 4):
                    sre += sublane_partner(re, sub, dist)
                    sim += sublane_partner(im, sub, dist)
                mine = lanes[h * nx * 8:(h + 1) * nx * 8]
                store_row(qbuf, h, y, (sre + ore + mine[:, :LANES].reshape(nx, 8, LANES),
                                       sim + oim + mine[:, LANES:].reshape(nx, 8, LANES)))
            return 0

        lax.fori_loop(0, ny, inner, 0)
        high_sums(at)

    def prepare(layer):
        low_sums(layer)
        high_sums(layer)

        def body(j, total):
            for h in range(2):
                total += im_dot((kept[lam, h, j, 0], kept[lam, h, j, 1]), (qbuf[h, j, 0], qbuf[h, j, 1]))
            return total

        acc[1 + num_layers + layer] = lax.fori_loop(0, nb, body, zero)
        full_sums(before_at + layer)

    def collect(layer, source):
        at = before_at + layer

        def body(j, sums):
            gamma_sum, beta_sum = sums
            for h in range(2):
                left = (kept[lam_pre, h, j, 0], kept[lam_pre, h, j, 1])
                gamma_sum += source[j, h] * im_dot(left, (kept[at, h, j, 0], kept[at, h, j, 1]))
                beta_sum += im_dot(left, (qbuf[h, j, 0], qbuf[h, j, 1]))
            return gamma_sum, beta_sum

        gamma_sum, beta_sum = lax.fori_loop(0, nb, body, (zero, zero))
        acc[1 + layer] = 2.0 * gamma_sum
        acc[1 + num_layers + layer] += beta_sum

    def side_source(k):
        @pl.when(k == 0)
        def _():
            def body(places):
                blocks = [(cost[j, h] * re, cost[j, h] * im)
                          for (h, j), (re, im) in zip(places, load(kept.at[before_at], places))]
                store(side, places, mix_all(blocks, tan0))

            for_columns((0, 1), body)

        @pl.when(k == 2)
        def _():
            low_sums(before_at)
            high_sums(before_at)
            for_columns((0, 1), lambda places: store(side, places, mix_all(load(qbuf, places), tan0)))

    def side_arrival(n):
        per_half(lambda h: receive(2 + n, h, 0, tan0, side, []))

        def body(places):
            for h in range(2):
                mine = places[h::2]
                store(kept.at[side_at + n], mine, mix_all(load(side, mine), tan0))

        for_columns((0, 1), body)

    def side_sums():
        full_sums(0)

        def body(j, _):
            for h in range(2):
                for c in range(2):
                    kept[sums_at, h, j, c] = qbuf[h, j, c] + kept[side_at + 1, h, j, c]
            return 0

        lax.fori_loop(0, nb, body, 0)

    def last_sums(h):
        def body(x, sums):
            gamma1, beta1, gamma0, beta0 = sums
            places = column(x, (h,))
            blocks = mix_all(load(work, places), angle[1])
            for (h_, j), left, right, q in zip(places, blocks, load(kept.at[before_at + 1], places), load(qbuf, places)):
                gamma1 += cost_b[j, h_] * im_dot(left, right)
                beta1 += im_dot(left, q)
            blocks = turn(blocks, 1, places)
            for left, right, q in zip(blocks, load(kept.at[side_at], places), load(kept.at[sums_at], places)):
                gamma0 += im_dot(left, right)
                beta0 += im_dot(left, q)
            return gamma1, beta1, gamma0, beta0

        gamma1, beta1, gamma0, beta0 = lax.fori_loop(0, nx, body, (zero,) * 4)
        acc[1] += 2.0 * gamma0
        acc[2] += 2.0 * gamma1
        acc[1 + num_layers] += beta0
        acc[2 + num_layers] += beta1

    def two_gaps(k, _):
        step = 2 * k
        _, done, _, following = plan(step)
        tan_half, tan_next = angle[done], angle[following]

        def half(h):
            receive(0, h, done, tan_half, work, lanes_late(True, h))
            for_columns((h,), middle(step))

            @pl.when(k > 0)
            def _():
                wait_sends(1, h)

            send_half(1, h, following, tan_next, work, lanes_late(False, h))

        for h in range(2):
            half(h)

        side_source(k)

        @pl.when(k < pairs - 1)
        def _():
            make_table(step + 2, cost)

        @pl.when(k >= pairs)
        def _():
            collect(done, cost_b)
            prepare(following)

        step = 2 * k + 1
        _, done, _, following = plan(step)
        tan_half = angle[done]
        receive(1, 0, done, tan_half, work, lanes_late(False, 0))

        @pl.when((k < 3) | (k == 4))
        def _():
            piece = k - k // 4
            send_half(2 + piece // 2, piece % 2, 0, tan0, side, [])

        receive(1, 1, done, tan_half, work, lanes_late(False, 1))

        @pl.when(k % pairs < pairs - 1)
        def _():
            for_columns((0, 1), middle(step))

        @pl.when(k == pairs - 1)
        def _():
            for_columns((0, 1), turn_point)

        into = following - (k // (pairs - 1)) * (1 - k // pairs) * (following - last)
        tan_next = angle[into]

        def half_joint(h):
            wait_sends(0, h)
            send_half(0, h, into, tan_next, work, lanes_late(True, h))

        for h in range(2):
            half_joint(h)

        @pl.when(k < pairs - 1)
        def _():
            make_table(step + 2, cost_b)

        @pl.when(k == pairs - 1)
        def _():
            def write(j, _):
                for h in range(2):
                    for c in range(2):
                        final[c, j, h] = root * kept[last, h, j, c]
                return 0

            lax.fori_loop(0, nb, write, 0)

        @pl.when(k >= pairs)
        def _():
            collect(done, cost)

        @pl.when((k == 4) | (k == 5))
        def _():
            side_arrival(k - 4)

        @pl.when(k == 2 * pairs - 2)
        def _():
            side_sums()

        @pl.when(k >= pairs - 1)
        def _():
            prepare(2 * num_layers - 3 - 2 * k)

        return 0

    lax.fori_loop(0, 2 * pairs - 1, two_gaps, 0)

    def last_half(h):
        receive(0, h, 1, angle[1], work, lanes_late(True, h))
        last_sums(h)

    for h in range(2):
        last_half(h)

    lane = lax.broadcasted_iota(jnp.int32, (1, LANES), 1)
    row = jnp.zeros((1, LANES), jnp.float32)
    for place in range(acc.shape[0]):
        value = jnp.sum(jnp.sum(acc[place], axis=0, keepdims=True), axis=1, keepdims=True)
        row = jnp.where(lane == place, value, row)
    part[...] = row
    for dy, dx, dc in offsets:
        y, x, dest = peer(dy, dx, dc)
        pltpu.make_async_remote_copy(
            src_ref=part, dst_ref=gath.at[me], send_sem=sum_send, recv_sem=sum_recv,
            device_id={"qy": y, "qx": x}, device_id_type=MESH_ID).start()
    gath[me] = row
    for par in range(4):
        for h in range(2):
            wait_sends(par, h)
    view = cost_b.at[pl.ds(0, nb - 1)]
    pltpu.make_async_copy(view, view, cost_send).wait()
    view = gath.at[pl.ds(0, nb - 1)]
    pltpu.make_async_copy(view, view, sum_recv).wait()
    total = gath[0]
    for j in range(1, nb):
        total += gath[j]
    totals[...] = total
    view = gath.at[pl.ds(0, nb - 1)]
    pltpu.make_async_copy(view, view, sum_send).wait()


def solution(mesh):
    ny, nx = mesh.shape["qy"], mesh.shape["qx"]
    nb = ny * nx

    def local_run(cost_local, gamma_angles, beta_angles):
        chunk = cost_local.shape[0]
        num_layers = gamma_angles.shape[0]
        assert chunk == nb * 16 * LANES and num_layers % 2 == 0 and num_layers >= 8
        num_qubits = int(math.log2(chunk * nb))
        amp = (chunk * nb) ** -0.5
        vmem, smem, dma = pltpu.VMEM, pltpu.SMEM, pltpu.SemaphoreType.DMA
        f32 = jnp.float32
        state = (2, nb, 2, 8, LANES)
        final, totals = pl.pallas_call(
            functools.partial(kernel, ny, nx, num_layers, num_qubits, amp),
            out_shape=(jax.ShapeDtypeStruct((2, nb, 2, 8, LANES), f32), jax.ShapeDtypeStruct((1, LANES), f32)),
            in_specs=[pl.BlockSpec(memory_space=pltpu.MemorySpace.HBM)] * 3,
            out_specs=(pl.BlockSpec(memory_space=vmem), pl.BlockSpec(memory_space=vmem)),
            scratch_shapes=[
                vmem((nb, 2, 8, LANES), f32),
                smem((num_layers,), f32),
                smem((num_layers,), f32),
                vmem((nb, 2, 8, LANES), f32),
                vmem((num_layers, 2, 2, nb, 8, LANES), f32),
                vmem((2 * num_layers + 5,) + state, f32),
                vmem((4,) + state, f32),
                vmem((4,) + state, f32),
                vmem(state, f32),
                vmem(state, f32),
                vmem(state, f32),
                vmem((num_layers, 8, LANES), f32),
                vmem((num_layers, 2 * LANES, 2 * LANES), f32),
                vmem((2 * LANES, 2 * LANES), f32),
                vmem((1 + 2 * num_layers, 8, LANES), f32),
                vmem((1, LANES), f32),
                vmem((nb, 1, LANES), f32),
                dma((3,)),
                dma((4, 2)),
                dma((4, 2, 1 + ny // 2)),
                dma,
                dma,
                dma,
                dma,
            ],
            compiler_params=pltpu.CompilerParams(
                collective_id=0, has_side_effects=True, vmem_limit_bytes=48 * 1024 * 1024),
            name="qaoa",
        )(cost_local.reshape(nb, 2, 8, LANES), gamma_angles, beta_angles)
        energy = totals[0, :1]
        grad = totals[0, 1:1 + 2 * num_layers]
        return energy, grad, final.reshape(2, chunk)

    state_spec = P(("inst", "qy", "qx"))
    return jax.shard_map(
        local_run, mesh=mesh, in_specs=(state_spec, P(), P()),
        out_specs=(P("inst"), P("inst"), P(None, ("inst", "qy", "qx"))), check_vma=False)
```
